32 devices in a mesh: gx: 8 (over z, x), gy: 4 (over y, core).
Axes of the slice: x: 2, y: 2, z: 4, core: 2. Of those that a mesh axis runs over, the one named last changes fastest.
Arguments:
- basis: float32 [64, 512, 512], P(None, 'gx', 'gy'), may hold values from -6 to 6
- panel: float32 [8, 512, 512], P(None, 'gx', 'gy'), may hold values from -12 to 12
- rate_codes: int32 [4, 512, 512], P(None, 'gx', 'gy'), may hold values from 1 to 16
Outputs:
- first_panel: float32 [8, 512, 512], P(None, 'gx', 'gy')
- second_panel: float32 [8, 512, 512], P(None, 'gx', 'gy')
- first_coef: float32 [72, 8], replicated
- second_coef: float32 [80, 8], replicated
The draws below stay inside these ranges and needn't reach their ends.
All inputs are finite; a program needn't handle non-finite values.
Results may differ from the reference program's by a relative error of at most 0.00014.
Values sent between devices are 32-bit elements; how exact they have to be, the bound alone decides.
A program may use at most 64 MiB of HBM per device.

```python
import jax
import jax.numpy as jnp
from jax import lax

BLOCK = 8
BASIS = 64
NX = 512
NY = 512


def basis_fields(key):
    base_key = jax.random.fold_in(key, 23)
    noise_key, shared_key, weight_key, sign_key = jax.random.split(base_key, 4)
    row_pos = jnp.arange(NX, dtype=jnp.float32) / max(NX - 1, 1)
    shared_sign = 2.0 * jax.random.bernoulli(shared_key, 0.5, (1, NX, NY)).astype(jnp.float32) - 1.0
    col_signs = 2.0 * jax.random.bernoulli(sign_key, 0.5, (BASIS, 1, 1)).astype(jnp.float32) - 1.0
    col_weights = jax.random.uniform(weight_key, (BASIS, 1, 1), jnp.float32, 0.03, 0.07) * col_signs
    noise_part = jnp.clip(jax.random.normal(noise_key, (BASIS, NX, NY), jnp.float32), -4.0, 4.0)
    amplitude = 1.0 + 3.0 * row_pos
    result = noise_part + shared_sign * col_weights * amplitude[None, :, None]
    return jnp.clip(result, -6.0, 6.0).astype(jnp.float32)


def draw_basis(key, part):
    return basis_fields(key)


def draw_panel(key, part):
    base_key = jax.random.fold_in(key, 11)
    first_key = jax.random.fold_in(base_key, 0)
    mix_key = jax.random.fold_in(base_key, 2)
    row_pos = jnp.arange(NX, dtype=jnp.float32)
    row_scale = 1.0 + 2.0 * row_pos / max(NX - 1, 1)
    values = jnp.clip(jax.random.normal(first_key, (BLOCK, NX, NY), jnp.float32), -4.0, 4.0)
    own_part = values * row_scale[None, :, None]
    mixing = jax.random.normal(mix_key, (BLOCK, BASIS), jnp.float32) * 0.15
    basis_part = jnp.einsum('jk,kxy->jxy', mixing, basis_fields(key))
    return jnp.clip(own_part + basis_part, -12.0, 12.0).astype(jnp.float32)


def touch_ends(array, rng, low, high):
    index_at = [jax.random.randint(jax.random.fold_in(rng, axis), (), 0, length) for axis, length in enumerate(array.shape)]
    widest = array.shape.index(max(array.shape))
    neighbour = index_at[:widest] + [(index_at[widest] + 1) % array.shape[widest]] + index_at[widest + 1:]
    return array.at[tuple(index_at)].set(low).at[tuple(neighbour)].set(high)


def setup_inputs(seed: int = 0) -> dict:
    seeds = jax.random.split(jax.random.key(seed), 4)
    basis = draw_basis(jax.random.fold_in(seeds[3], 71), 0)
    panel = draw_panel(jax.random.fold_in(seeds[3], 71), 0)
    rate_codes = touch_ends(jax.random.randint(seeds[2], (4, NX, NY), 1, 17), jax.random.fold_in(seeds[2], 1), 1, 16).astype(jnp.int32)
    return {"basis": basis, "panel": panel, "rate_codes": rate_codes}


HIGH = lax.Precision.HIGHEST

def lattice_apply(field, rate_codes):
    rate_vals = rate_codes.astype(jnp.float32) * 0.125
    padded = jnp.pad(field, ((0, 0), (1, 1), (1, 1)))
    rate_pad = jnp.pad(rate_vals, ((0, 0), (1, 1), (1, 1)))
    inflow = padded[:, :-2, 1:-1] * rate_pad[1, :-2, 1:-1] + padded[:, 2:, 1:-1] * rate_pad[0, 2:, 1:-1] + padded[:, 1:-1, :-2] * rate_pad[3, 1:-1, :-2] + padded[:, 1:-1, 2:] * rate_pad[2, 1:-1, 2:]
    return inflow - jnp.sum(rate_vals, axis=0) * field

def expand_once(basis_flat, panel_flat, site_count):
    proj_coef = jnp.dot(basis_flat, panel_flat.T, precision=HIGH) / site_count
    cleaned = panel_flat - jnp.dot(proj_coef.T, basis_flat, precision=HIGH)
    gram_mat = jnp.dot(cleaned, cleaned.T, precision=HIGH) / site_count
    lower_fac = jnp.linalg.cholesky(gram_mat)
    width_cols = gram_mat.shape[0]
    inverse_fac = lax.linalg.triangular_solve(lower_fac, jnp.eye(width_cols, dtype=jnp.float32), left_side=True, lower=True)
    new_panel = jnp.dot(inverse_fac, cleaned, precision=HIGH)
    return (new_panel, jnp.concatenate([proj_coef, lower_fac.T], axis=0))

def reference(basis, panel, rate_codes):
    site_count = jnp.float32(NX * NY)
    basis_flat = basis.reshape(BASIS, NX * NY)
    image_one = lattice_apply(panel, rate_codes).reshape(BLOCK, NX * NY)
    first_flat, first_coef = expand_once(basis_flat, image_one, site_count)
    first_panel = first_flat.reshape(BLOCK, NX, NY)
    image_two = lattice_apply(first_panel, rate_codes).reshape(BLOCK, NX * NY)
    grown = jnp.concatenate([basis_flat, first_flat], axis=0)
    second_flat, second_coef = expand_once(grown, image_two, site_count)
    return (first_panel, second_flat.reshape(BLOCK, NX, NY), first_coef, second_coef)
```

```python
import functools

import jax
import jax.numpy as jnp
from jax import lax
from jax.experimental import pallas as pl
from jax.experimental.pallas import tpu as pltpu
from jax.sharding import PartitionSpec as P

HIGH = lax.Precision.HIGHEST
MESH = pl.DeviceIdType.MESH
F32 = jnp.float32
BF = jnp.bfloat16
LANES = 128
CHUNKS = 4
DIRECT = 64
BUDDY = 2
PAD = 8


def dot_nn(a, b):
    return jnp.dot(a, b, precision=HIGH, preferred_element_type=F32)


def dot_nt(a, b, precision=HIGH):
    return lax.dot_general(
        a, b, (((1,), (1,)), ((), ())), precision=precision, preferred_element_type=F32
    )


def rows_full(v, at=0):
    parts = [v, jnp.zeros((LANES - at - v.shape[0], LANES), F32)]
    if at:
        parts.insert(0, jnp.zeros((at, LANES), F32))
    return jnp.concatenate(parts, axis=0)


def split(v):
    hi = v.astype(BF).astype(F32)
    return hi, v - hi


def split_rows(v):
    return jnp.concatenate(split(v), axis=0).astype(BF)


def eliminate(a, g0, n):
    sub = lax.broadcasted_iota(jnp.int32, a.shape, 0)
    cols = [jnp.broadcast_to(a[:, g0 + j : g0 + j + 1], a.shape) for j in range(n)]
    pivots = jnp.ones(a.shape, F32)
    for k in range(n):
        pivot = jnp.broadcast_to(cols[k][k : k + 1, :], a.shape)
        pivots = jnp.where(sub == k, pivot, pivots)
        if k == n - 1:
            break
        factor = jnp.where(sub > k, cols[k] * (1.0 / pivot), 0.0)
        for j in range(k + 1, n):
            cols[j] = cols[j] - factor * cols[j][k : k + 1, :]
        a = a - factor * a[k : k + 1, :]
    return a * (1.0 / jnp.sqrt(pivots))


def kernel(
    nx, ny, K, N, R,
    basis_hbm, panel_hbm, rate_hbm,
    first_v, second_v, coefs,
    basis_v, panel_v, rate_v, rates, fext, wf, x_v, u_v, m_v, s_v,
    edge_send, edge_recv, eb_send, eb_recv, my_buf, mx_buf, py_buf, px_buf,
    in_sem, edge_ssem, edge_rsem, eb_ssem, eb_rsem, ready,
    my_s, my_r, mx_s, mx_r, py_s, py_r, px_s, px_r,
):
    ix, iy = lax.axis_index("gx"), lax.axis_index("gy")
    sites = R * LANES
    scale = 1.0 / (sites * nx * ny)
    lane = lax.broadcasted_iota(jnp.int32, (N, LANES), 1)
    sub = lax.broadcasted_iota(jnp.int32, (N, LANES), 0)
    KN = K + N
    Z = K + 2 * N
    RP = R + PAD
    T = R + 16

    step = K // CHUNKS
    panel_in = pltpu.make_async_copy(panel_hbm, panel_v.at[:, pl.ds(0, R)], in_sem.at[0])
    rate_in = pltpu.make_async_copy(rate_hbm, rate_v, in_sem.at[1])
    panel_in.start()
    rate_in.start()
    basis_in = []
    for c in range(CHUNKS):
        part = pl.ds(c * step, step)
        basis_in.append(
            pltpu.make_async_copy(
                basis_hbm.at[part], basis_v.at[part, pl.ds(0, R)], in_sem.at[2 + c]
            )
        )
        basis_in[-1].start()
    basis_rows = basis_v.reshape(K * RP, LANES)
    panel_rows = panel_v.reshape(N * RP, LANES)

    axes = (("gx", ix, nx), ("gy", iy, ny))
    everyone = ("all", ix * ny + iy, nx * ny)
    direct = nx * ny <= DIRECT and nx % BUDDY == 0

    def peer_of(axis, me, n, d):
        other = lax.rem(me + d, n)
        if axis == "all":
            return other, {"gx": lax.div(other, ny), "gy": lax.rem(other, ny)}
        return other, {axis: other}

    barrier = pltpu.get_barrier_semaphore()

    def greet(device):
        pl.semaphore_signal(barrier, inc=1, device_id=device, device_id_type=MESH)

    line = []
    if direct:
        home = lax.div(ix, BUDDY) * BUDDY
        seat = (ix - home) * ny + iy
        group = BUDDY * ny
        for d in range(1, group):
            other = lax.rem(seat + d, group)
            greet({"gx": home + lax.div(other, ny), "gy": lax.rem(other, ny)})
        for d in range(1, nx // BUDDY):
            line.append({"gx": lax.rem(ix + d * BUDDY, nx)})
            greet(line[-1])
        outer = jnp.where(ix == home, ix - 1, ix + 1)
        has_outer = (ix != home) & (ix != home + BUDDY - 1) if BUDDY > 2 else (outer >= 0) & (outer < nx)

        @pl.when(has_outer)
        def _():
            greet({"gx": outer})

        greeted = group - 1 + len(line) + jnp.where(has_outer, 1, 0)
    else:
        greeted = 0
        for axis, me, n in axes:
            for d in range(1, n):
                greet(peer_of(axis, me, n, d)[1])
                greeted += 1

    def row_at(r):
        return pl.ds(r * LANES, LANES)

    def rate_row(d, r):
        return rates[pl.ds(d * T + 8 + r, 1), :]

    panel_in.wait()
    rate_in.wait()
    for d in range(4):
        rates[d * T : d * T + 8, :] = jnp.ones((8, LANES), F32)
        rates[d * T + 8 + R : (d + 1) * T, :] = jnp.ones((8, LANES), F32)
        rates[d * T + 8 : d * T + 8 + R, :] = (
            rate_v[d * R : (d + 1) * R, :].astype(F32) * 0.125
        )
    rates[4 * T + 8 : 4 * T + 8 + R, :] = (
        rates[8 : 8 + R, :]
        + rates[T + 8 : T + 8 + R, :]
        + rates[2 * T + 8 : 2 * T + 8 + R, :]
        + rates[3 * T + 8 : 3 * T + 8 + R, :]
    )

    routes = (
        ("gx", ix - 1, ix > 0, ix < nx - 1),
        ("gx", ix + 1, ix < nx - 1, ix > 0),
        ("gy", iy - 1, iy > 0, iy < ny - 1),
        ("gy", iy + 1, iy < ny - 1, iy > 0),
    )

    def edges(send, recv, ssem, rsem):
        def copy(e):
            return pltpu.make_async_remote_copy(
                src_ref=send.at[e],
                dst_ref=recv.at[e],
                send_sem=ssem.at[e],
                recv_sem=rsem.at[e],
                device_id={routes[e][0]: routes[e][1]},
                device_id_type=MESH,
            )

        def start():
            for e in range(4):
                @pl.when(routes[e][2])
                def _(e=e):
                    copy(e).start()

                @pl.when(jnp.logical_not(routes[e][3]))
                def _(e=e):
                    recv[e] = jnp.zeros(recv.shape[1:], F32)

        def wait():
            for e in range(4):
                @pl.when(routes[e][3])
                def _(e=e):
                    copy(e).wait_recv()

        def drain():
            for e in range(4):
                @pl.when(routes[e][2])
                def _(e=e):
                    copy(e).wait_send()

        return start, wait, drain

    def share(buf, ssem, rsem, axis, me, n):
        def copy(d):
            return pltpu.make_async_remote_copy(
                src_ref=buf.at[me],
                dst_ref=buf.at[me],
                send_sem=ssem.at[d],
                recv_sem=rsem.at[me],
                device_id=peer_of(axis, me, n, d)[1],
                device_id_type=MESH,
            )

        def start(store):
            store(buf.at[me])
            for d in range(1, n):
                copy(d).start()

        def finish():
            for d in range(1, n):
                src, device = peer_of(axis, me, n, d)
                pltpu.make_async_remote_copy(
                    src_ref=buf.at[src],
                    dst_ref=buf.at[src],
                    send_sem=ssem.at[d],
                    recv_sem=rsem.at[src],
                    device_id=device,
                    device_id_type=MESH,
                ).wait_recv()
            parts = [buf[k] for k in range(n)]
            while len(parts) > 1:
                parts = [
                    parts[i] + parts[i + 1] if i + 1 < len(parts) else parts[i]
                    for i in range(0, len(parts), 2)
                ]
            return parts[0]

        def drain():
            for d in range(1, n):
                copy(d).wait_send()

        return start, finish, drain

    half = N // 2

    def pack(v):
        turned = pltpu.roll(v, K, 1)
        tail = pltpu.roll(v, 0, 1, stride=2 * N, stride_axis=0)
        mine = lax.div(lane, 2 * N) == lax.rem(sub + K // (2 * N), N)
        tail = jnp.sum(jnp.where(mine, tail, 0.0), axis=0, keepdims=True)
        low = lax.broadcasted_iota(jnp.int32, (half, LANES), 1) < K
        return jnp.where(low, v[0:half], turned[half:N]), tail

    def unpack(t):
        body = jnp.concatenate([t[0:half], pltpu.roll(t[0:half], K, 1)], axis=0)
        spread = jnp.broadcast_to(t[half : half + 1], (N, LANES))
        tail = spread
        for j in range(1, N):
            tail = jnp.where(sub == j, pltpu.roll(spread, LANES - 2 * N * j, 1), tail)
        return jnp.where(lane < K, body, jnp.where(lane < Z, tail, 0.0))

    drains = []

    def reduction(s, value):
        xgroup = everyone if direct else axes[0]
        xstart, xfinish, xdrain = share(px_buf.at[s], px_s.at[s], px_r.at[s], *xgroup)
        drains.append(xdrain)

        def put(parts):
            def store(ref):
                ref[0:half] = parts[0]
                ref[half : half + 1] = parts[1]

            return store

        parts = pack(value)
        if direct:
            xstart(put(parts))
            return lambda: unpack(xfinish())
        ystart, yfinish, ydrain = share(py_buf.at[s], py_s.at[s], py_r.at[s], *axes[1])
        drains.append(ydrain)
        ystart(put(parts))

        def finish():
            t = yfinish()
            xstart(put((t[0:half], t[half : half + 1])))
            return unpack(xfinish())

        return finish

    e0_start, e0_wait, e0_drain = edges(edge_send, edge_recv, edge_ssem, edge_rsem)
    e1_start, e1_wait, e1_drain = edges(eb_send, eb_recv, eb_ssem, eb_rsem)
    drains += [e0_drain, e1_drain]

    with jax.named_scope("packp"):
        left, right = jnp.zeros((N, LANES), F32), jnp.zeros((N, LANES), F32)
        for r in range(R):
            f = panel_rows[pl.ds(r, N, stride=RP), :]
            fext[:, row_at(r + 1)] = f
            left = jnp.where(lane == r, pltpu.roll(f * rate_row(2, r), r, 1), left)
            right = jnp.where(lane == r, pltpu.roll(f * rate_row(3, r), r + 1, 1), right)
            if r == 0:
                edge_send[0] = f * rate_row(0, 0)
            if r == R - 1:
                edge_send[1] = f * rate_row(1, R - 1)
        edge_send[2] = left
        edge_send[3] = right

    with jax.named_scope("barrier"):
        pl.semaphore_wait(barrier, greeted)
    e0_start()
    for device in line:
        pl.semaphore_signal(ready, inc=1, device_id=device, device_id_type=MESH)

    def rate_col(d, c):
        whole = jnp.concatenate(
            [rates[d * T + 8 : d * T + 8 + R, :], jnp.zeros((LANES - R, LANES), F32)], axis=0
        )
        return whole.T[c : c + 1, :]

    rate_left, rate_right = rate_col(2, 0), rate_col(3, LANES - 1)

    wide = lax.broadcasted_iota(jnp.int32, (step, LANES), 1)
    with jax.named_scope("split"):
        for c in range(CHUNKS):
            basis_in[c].wait()
            mine = slice(c * step, (c + 1) * step)
            below = slice(Z + c * step, Z + (c + 1) * step)

            def body(i, carry, c=c, mine=mine, below=below):
                left, right = carry
                for u in range(8):
                    r = i * 8 + u
                    b = basis_rows[pl.ds(c * step * RP + r, step, stride=RP), :]
                    hi = b.astype(BF)
                    at = pl.ds(pl.multiple_of(r * LANES, LANES), LANES)
                    x_v[mine, at] = hi
                    x_v[below, at] = (b - hi.astype(F32)).astype(BF)
                    left = jnp.where(wide == r, pltpu.roll(b, r, 1), left)
                    right = jnp.where(wide == r, pltpu.roll(b, r + 1, 1), right)
                return left, right

            zero = jnp.zeros((step, LANES), F32)
            left, right = lax.fori_loop(0, R // 8, body, (zero, zero))
            eb_send[2, mine] = left * rate_left
            eb_send[3, mine] = right * rate_right
            eb_send[0, mine] = basis_rows[pl.ds(c * step * RP, step, stride=RP), :] * rate_row(0, 0)
            eb_send[1, mine] = (
                basis_rows[pl.ds(c * step * RP + R - 1, step, stride=RP), :] * rate_row(1, R - 1)
            )

    def stencil(from_right, from_left, finish):
        for r in range(R):
            f = fext[:, row_at(r + 1)]
            above = fext[:, row_at(r)] * rate_row(1, r - 1)
            below = fext[:, row_at(r + 2)] * rate_row(0, r + 1)
            west = jnp.where(
                lane == 0,
                pltpu.roll(from_left, (LANES - r) % LANES, 1),
                pltpu.roll(f * rate_row(3, r), 1, 1),
            )
            east = jnp.where(
                lane == LANES - 1,
                pltpu.roll(from_right, LANES - 1 - r, 1),
                pltpu.roll(f * rate_row(2, r), LANES - 1, 1),
            )
            finish(r, f, above + below + west + east - rate_row(4, r) * f)

    def put_pair(r, upper, lower):
        both = jnp.concatenate([upper, lower], axis=0)
        hi = both.astype(BF)
        low = both - hi.astype(F32)
        x_v[K:Z, row_at(r)] = hi
        x_v[Z + K : 2 * Z, row_at(r)] = low.astype(BF)
        return hi.astype(F32), low

    PIECE = 16

    def products(s):
        total = jnp.zeros((2 * N, Z), F32)
        for i in range(R // PIECE):
            at = pl.ds(i * PIECE * LANES, PIECE * LANES)
            for top in (0, Z):
                total = total + dot_nt(u_v[:, at], x_v[top : top + Z, at], lax.Precision.DEFAULT)
        total = (total[0:N] + total[N : 2 * N]) * scale
        s_v[:, 0:Z] = total
        return s_v[...]

    with jax.named_scope("ewait0"):
        e0_wait()
    with jax.named_scope("lat0"):
        s_v[...] = jnp.zeros_like(s_v)
        fext[:, 0:LANES] = edge_recv[1]
        fext[:, (R + 1) * LANES : (R + 2) * LANES] = edge_recv[0]
        zero = jnp.zeros((N, LANES), F32)
        packed = [zero, zero]

        def finish_first(r, f, w):
            wf[:, row_at(r)] = w
            hi, low = put_pair(r, w, zero)
            u_v[:, row_at(r)] = jnp.concatenate([hi[0:N], low[0:N]], axis=0).astype(BF)
            packed[0] = jnp.where(lane == r, pltpu.roll(w, r, 1), packed[0])
            packed[1] = jnp.where(lane == r, pltpu.roll(w, r + 1, 1), packed[1])
            if r == 0:
                eb_send[0, K:KN] = w * rate_row(0, 0)
            if r == R - 1:
                eb_send[1, K:KN] = w * rate_row(1, R - 1)

        stencil(edge_recv[2], edge_recv[3], finish_first)
        eb_send[2, K:KN] = packed[0] * rate_left
        eb_send[3, K:KN] = packed[1] * rate_right
        value = products(0)
        if direct:
            pl.semaphore_wait(ready, len(line))
        finish0 = reduction(0, value)
    e1_start()

    with jax.named_scope("gram"):
        hh = dot_nt(x_v[0:K, 0:sites], x_v[0:K, 0:sites], lax.Precision.DEFAULT)
        hl = dot_nt(x_v[0:K, 0:sites], x_v[Z : Z + K, 0:sites], lax.Precision.DEFAULT)
        lh = dot_nt(x_v[Z : Z + K, 0:sites], x_v[0:K, 0:sites], lax.Precision.DEFAULT)
        full = (hh + hl + lh) * scale
        mid = K // 2
        my_start, my_finish, my_drain = share(my_buf, my_s, my_r, *axes[1])
        mx_start, mx_finish, mx_drain = share(mx_buf, mx_s, mx_r, *axes[0])
        drains += [my_drain, mx_drain]

        def put_gram(ref):
            ref[...] = jnp.concatenate([full[0:mid], full[mid:K]], axis=1)

        my_start(put_gram)

    with jax.named_scope("ewait1"):
        e1_wait()
    with jax.named_scope("esplit"):
        for e in range(4):
            at = pl.ds(sites + e * LANES, LANES)
            b = eb_recv[e, 0:K]
            hi = b.astype(BF)
            x_v[0:K, at] = hi
            x_v[Z : Z + K, at] = (b - hi.astype(F32)).astype(BF)
            x_v[K:Z, at] = jnp.zeros((2 * N, LANES), BF)
            x_v[Z + K : 2 * Z, at] = jnp.zeros((2 * N, LANES), BF)
            wf[:, at] = eb_recv[e, K:KN]
    with jax.named_scope("myfin"):
        m = my_finish()

        def put_m(ref):
            ref[...] = m

        mx_start(put_m)

    with jax.named_scope("red0"):
        total = finish0()

    def combine(lhs, at):
        both = jnp.dot(lhs, x_v[0:Z, at], preferred_element_type=F32) + jnp.dot(
            lhs, x_v[Z : 2 * Z, at], preferred_element_type=F32
        )
        return both[0:N] + both[N : 2 * N]

    wide8 = 8 * LANES
    pm = jnp.where(lane < K, total, 0.0)
    with jax.named_scope("new0"):
        lhs = split_rows(pm)[:, 0:Z]
        at = pl.ds(sites, 4 * LANES)
        edge = wf[:, at] - combine(lhs, at)
        fext[:, 0:LANES] = edge[:, LANES : 2 * LANES]
        fext[:, (R + 1) * LANES : (R + 2) * LANES] = edge[:, 0:LANES]
        for i in range(R // 8):
            at = pl.ds(i * wide8, wide8)
            fext[:, pl.ds(LANES + i * wide8, wide8)] = wf[:, at] - combine(lhs, at)
    with jax.named_scope("lat1"):
        def finish_second(r, f, u):
            hi, low = put_pair(r, f, u)
            u_v[:, row_at(r)] = jnp.concatenate([hi[N : 2 * N], low[N : 2 * N]], axis=0).astype(BF)

        stencil(edge[:, 2 * LANES : 3 * LANES], edge[:, 3 * LANES : 4 * LANES], finish_second)
        finish1 = reduction(1, products(1))

    with jax.named_scope("mxfin"):
        m = mx_finish()
        gram = rows_full(
            jnp.concatenate(
                [
                    jnp.where(lax.broadcasted_iota(jnp.int32, (mid, LANES), 1) < K, m, 0.0),
                    jnp.where(
                        lax.broadcasted_iota(jnp.int32, (mid, LANES), 1) < K,
                        pltpu.roll(m, LANES - K, 1),
                        0.0,
                    ),
                ],
                axis=0,
            )
        )
    G0 = Z
    with jax.named_scope("fac0"):
        own = pltpu.roll(total, G0 - K, 1)
        rest = 2.0 * pm - dot_nn(pm, gram)
        g = jnp.where((lane >= G0) & (lane < G0 + N), own - dot_nt(rest, rows_full(pm, G0)), 0.0)
        a = jnp.where(lane < K, rest - pm, jnp.where(lane == sub + K, 1.0, g))
        a = eliminate(a, G0, N)
        at_t = rows_full(a).T
        inv = pltpu.roll(a, LANES - K, 1)
        inv = jnp.where(lane < N, inv, 0.0)
        low1 = at_t[G0 : G0 + N]
        coefs[0] = pm + jnp.where((lane >= K) & (lane < KN), pltpu.roll(low1, K, 1), 0.0)
        row = lax.broadcasted_iota(jnp.int32, (LANES, LANES), 0)
        col = lax.broadcasted_iota(jnp.int32, (LANES, LANES), 1)
        inner = jnp.where((row < KN), at_t, 0.0)
        flow = dot_nn(inner, rows_full(jnp.where(lane < KN, a, 0.0)))
        in_b = (row < K) & (col < K)
        in_w = (row >= K) & (row < KN) & (col >= K) & (col < KN)
        eye = jnp.where(row == col, 1.0, 0.0)
        kmat = jnp.where(in_b, 2.0 * eye - gram, jnp.where(in_w, flow, -flow))
        dmat = jnp.where(in_b, eye, jnp.where(in_w, flow, 0.0))
        tmat = jnp.where((row >= K) & (row < KN) & (col < N), at_t, 0.0)
        m_v[0] = kmat
        m_v[1] = dmat
        m_v[2] = tmat
    with jax.named_scope("q1"):
        lhs = split_rows(jnp.where((lane >= K) & (lane < KN), pltpu.roll(inv, K, 1), 0.0))[:, 0:Z]
        for i in range(R // 8):
            q = combine(lhs, pl.ds(i * wide8, wide8))
            for u in range(8):
                first_v[pl.ds(i * 8 + u, N, stride=RP), :] = q[:, u * LANES : (u + 1) * LANES]

    with jax.named_scope("red1"):
        total = finish1()
    with jax.named_scope("fac1"):
        ep = jnp.where(lane < KN, total, 0.0)
        own = pltpu.roll(total, G0 - KN, 1)
        ek = dot_nn(ep, m_v[0])
        ed = dot_nn(ep, m_v[1])
        g = jnp.where((lane >= G0) & (lane < G0 + N), own - dot_nt(ek, rows_full(ep, G0)), 0.0)
        a = jnp.where(lane < KN, ed, jnp.where(lane == sub + KN, 1.0, g))
        a = eliminate(a, G0, N)
        lhs = split_rows(jnp.where(lane < KN, -a, a))[:, 0:Z]
    with jax.named_scope("new1"):
        for i in range(R // 8):
            q = combine(lhs, pl.ds(i * wide8, wide8))
            for u in range(8):
                second_v[pl.ds(i * 8 + u, N, stride=RP), :] = q[:, u * LANES : (u + 1) * LANES]
    with jax.named_scope("coef1"):
        low2 = rows_full(a).T[G0 : G0 + N]
        es = dot_nn(ep, m_v[2])
        stack = jnp.where(lane < K, ep, jnp.where(lane < KN, pltpu.roll(es, K, 1), 0.0))
        stack = jnp.where((lane >= KN) & (lane < Z), pltpu.roll(low2, KN, 1), stack)
        coefs[1] = dot_nn(inv, rows_full(stack))
        for drain in drains:
            drain()


def deliver(
    R, first_v, second_v, coefs, first_hbm, second_hbm, one_hbm, two_hbm, coef_one, coef_two, sem
):
    copies = [
        pltpu.make_async_copy(first_v.at[:, pl.ds(0, R)], first_hbm, sem.at[0]),
        pltpu.make_async_copy(second_v.at[:, pl.ds(0, R)], second_hbm, sem.at[1]),
        pltpu.make_async_copy(coef_one, one_hbm, sem.at[2]),
        pltpu.make_async_copy(coef_two, two_hbm, sem.at[3]),
    ]
    for copy in copies[:2]:
        copy.start()
    coef_one[...] = coefs[0, :, 0 : coef_one.shape[1]]
    coef_two[...] = coefs[1, :, 0 : coef_two.shape[1]]
    for copy in copies[2:]:
        copy.start()
    for copy in copies:
        copy.wait()


def local(nx, ny, basis, panel, rate_codes):
    N, R, C = panel.shape
    K = basis.shape[0]
    assert C == LANES and 2 * K == LANES and N == 8
    vmem = pl.BlockSpec(memory_space=pltpu.VMEM)
    hbm = pl.BlockSpec(memory_space=pl.ANY)
    dma = pltpu.SemaphoreType.DMA
    sites = R * LANES
    group = nx * ny if nx * ny <= DIRECT else nx
    Z = K + 2 * N
    first, second, coefs = pl.pallas_call(
        functools.partial(kernel, nx, ny, K, N, R),
        out_shape=(
            pltpu.VMEM((N * (R + PAD), C), F32),
            pltpu.VMEM((N * (R + PAD), C), F32),
            pltpu.VMEM((2, N, C), F32),
        ),
        in_specs=[pl.BlockSpec(memory_space=pltpu.HBM)] * 3,
        out_specs=(vmem, vmem, vmem),
        scratch_shapes=[
            pltpu.VMEM((K, R + PAD, LANES), F32),
            pltpu.VMEM((N, R + PAD, LANES), F32),
            pltpu.VMEM((4 * R, LANES), jnp.int32),
            pltpu.VMEM((5 * (R + 16), LANES), F32),
            pltpu.VMEM((N, (R + 2) * LANES), F32),
            pltpu.VMEM((N, sites + 4 * LANES), F32),
            pltpu.VMEM((2 * Z, sites + 4 * LANES), BF),
            pltpu.VMEM((2 * N, sites), BF),
            pltpu.VMEM((3, LANES, LANES), F32),
            pltpu.VMEM((N, LANES), F32),
            pltpu.VMEM((4, N, LANES), F32),
            pltpu.VMEM((4, N, LANES), F32),
            pltpu.VMEM((4, K + N, LANES), F32),
            pltpu.VMEM((4, K + N, LANES), F32),
            pltpu.VMEM((ny, K // 2, LANES), F32),
            pltpu.VMEM((nx, K // 2, LANES), F32),
            pltpu.VMEM((2, ny, N // 2 + 1, LANES), F32),
            pltpu.VMEM((2, group, N // 2 + 1, LANES), F32),
            dma((2 + CHUNKS,)),
            dma((4,)),
            dma((4,)),
            dma((4,)),
            dma((4,)),
            pltpu.SemaphoreType.REGULAR,
            dma((ny,)),
            dma((ny,)),
            dma((nx,)),
            dma((nx,)),
            dma((2, ny)),
            dma((2, ny)),
            dma((2, group)),
            dma((2, group)),
        ],
        compiler_params=pltpu.CompilerParams(
            collective_id=0, has_side_effects=True
        ),
    )(basis, panel, rate_codes.reshape(rate_codes.shape[0] * R, C))
    first, second, coef_one, coef_two = pl.pallas_call(
        functools.partial(deliver, R),
        out_shape=(
            jax.ShapeDtypeStruct((N, R, C), F32),
            jax.ShapeDtypeStruct((N, R, C), F32),
            jax.ShapeDtypeStruct((N, K + N), F32),
            jax.ShapeDtypeStruct((N, K + 2 * N), F32),
        ),
        in_specs=[vmem] * 3,
        out_specs=(hbm, hbm, hbm, hbm),
        scratch_shapes=[
            pltpu.VMEM((N, K + N), F32),
            pltpu.VMEM((N, K + 2 * N), F32),
            dma((4,)),
        ],
        compiler_params=pltpu.CompilerParams(vmem_limit_bytes=4 * 2**20),
    )(first.reshape(N, R + PAD, C), second.reshape(N, R + PAD, C), coefs)
    return first, second, coef_one.T, coef_two.T


def solution(mesh):
    spec = P(None, "gx", "gy")
    return jax.shard_map(
        functools.partial(local, mesh.shape["gx"], mesh.shape["gy"]),
        mesh=mesh,
        in_specs=(spec, spec, spec),
        out_specs=(spec, spec, P(), P()),
        check_vma=False,
    )
```

```python
import functools

import jax
import jax.numpy as jnp
from jax import lax
from jax.experimental import pallas as pl
from jax.experimental.pallas import tpu as pltpu
from jax.sharding import PartitionSpec as P

HIGH = lax.Precision.HIGHEST
MESH = pl.DeviceIdType.MESH
F32 = jnp.float32
BF = jnp.bfloat16
LANES = 128
CHUNKS = 4
DIRECT = 64
BUDDY = 2
PAD = 8


def dot_nn(a, b):
    return jnp.dot(a, b, precision=HIGH, preferred_element_type=F32)


def dot_nt(a, b, precision=HIGH):
    return lax.dot_general(
        a, b, (((1,), (1,)), ((), ())), precision=precision, preferred_element_type=F32
    )


def rows_full(v, at=0):
    parts = [v, jnp.zeros((LANES - at - v.shape[0], LANES), F32)]
    if at:
        parts.insert(0, jnp.zeros((at, LANES), F32))
    return jnp.concatenate(parts, axis=0)


def split(v):
    hi = v.astype(BF).astype(F32)
    return hi, v - hi


def split_rows(v):
    return jnp.concatenate(split(v), axis=0).astype(BF)


def eliminate(a, g0, n):
    sub = lax.broadcasted_iota(jnp.int32, a.shape, 0)
    cols = [jnp.broadcast_to(a[:, g0 + j : g0 + j + 1], a.shape) for j in range(n)]
    pivots = jnp.ones(a.shape, F32)
    for k in range(n):
        pivot = jnp.broadcast_to(cols[k][k : k + 1, :], a.shape)
        pivots = jnp.where(sub == k, pivot, pivots)
        if k == n - 1:
            break
        factor = jnp.where(sub > k, cols[k] * (1.0 / pivot), 0.0)
        for j in range(k + 1, n):
            cols[j] = cols[j] - factor * cols[j][k : k + 1, :]
        a = a - factor * a[k : k + 1, :]
    return a * (1.0 / jnp.sqrt(pivots))


def kernel(
    nx, ny, K, N, R,
    basis_hbm, panel_hbm, rate_hbm,
    first_v, second_v, coefs,
    basis_v, panel_v, rate_v, rates, fext, wf, x_v, u_v, m_v, t_v,
    edge_send, edge_recv, eb_send, eb_recv, ew_send, ew_recv, ms_buf, my_buf, mx_buf, mz_buf, py_buf, px_buf,
    in_sem, edge_ssem, edge_rsem, eb_ssem, eb_rsem, ew_ssem, ew_rsem, ready,
    m_s, py_s, px_s,
):
    ix, iy = lax.axis_index("gx"), lax.axis_index("gy")
    sites = R * LANES
    scale = 1.0 / (sites * nx * ny)
    lane = lax.broadcasted_iota(jnp.int32, (N, LANES), 1)
    sub = lax.broadcasted_iota(jnp.int32, (N, LANES), 0)
    KN = K + N
    Z = K + 2 * N
    RP = R + PAD
    T = R + 16

    step = K // CHUNKS
    with jax.named_scope("top"):
        pass
    panel_in = pltpu.make_async_copy(panel_hbm, panel_v.at[:, pl.ds(0, R)], in_sem.at[0])
    rate_in = pltpu.make_async_copy(rate_hbm, rate_v, in_sem.at[1])
    panel_in.start()
    rate_in.start()
    basis_in = []
    for c in range(CHUNKS):
        part = pl.ds(c * step, step)
        basis_in.append(
            pltpu.make_async_copy(
                basis_hbm.at[part], basis_v.at[part, pl.ds(0, R)], in_sem.at[2 + c]
            )
        )
        basis_in[-1].start()
    basis_rows = basis_v.reshape(K * RP, LANES)
    panel_rows = panel_v.reshape(N * RP, LANES)

    axes = (("gx", ix, nx), ("gy", iy, ny))
    everyone = ("all", ix * ny + iy, nx * ny)
    direct = nx * ny <= DIRECT and nx % BUDDY == 0

    def peer_of(axis, me, n, d):
        other = lax.rem(me + d, n)
        if axis == "all":
            return other, {"gx": lax.div(other, ny), "gy": lax.rem(other, ny)}
        return other, {axis: other}

    barrier = pltpu.get_barrier_semaphore()

    def greet(device):
        pl.semaphore_signal(barrier, inc=1, device_id=device, device_id_type=MESH)

    if direct:
        planes = nx // BUDDY
        plane = lax.div(ix, BUDDY)
        home = plane * BUDDY
        group = BUDDY * ny
        seat = (ix - home) * ny + iy
        for d in range(1, group):
            other = lax.rem(seat + d, group)
            greet({"gx": home + lax.div(other, ny), "gy": lax.rem(other, ny)})
        near = [
            (plane > 0, ix - BUDDY),
            (plane < planes - 1, ix + BUDDY),
            ((ix == home) & (ix > 0), ix - 1),
            ((ix == home + BUDDY - 1) & (ix < nx - 1), ix + 1),
        ]
        greeted = group - 1
        for there, device in near:
            greeted = greeted + jnp.where(there, 1, 0)

            @pl.when(there)
            def _(device=device):
                greet({"gx": device})

    else:
        greeted = 0
        for axis, me, n in axes:
            for d in range(1, n):
                greet(peer_of(axis, me, n, d)[1])
                greeted += 1

    def row_at(r):
        return pl.ds(r * LANES, LANES)

    def rate_row(d, r):
        return rates[pl.ds(d * T + 8 + r, 1), :]

    with jax.named_scope("inwait"):
        panel_in.wait()
        rate_in.wait()
    for d in range(4):
        rates[d * T : d * T + 8, :] = jnp.ones((8, LANES), F32)
        rates[d * T + 8 + R : (d + 1) * T, :] = jnp.ones((8, LANES), F32)
        rates[d * T + 8 : d * T + 8 + R, :] = (
            rate_v[d * R : (d + 1) * R, :].astype(F32) * 0.125
        )
    rates[4 * T + 8 : 4 * T + 8 + R, :] = (
        rates[8 : 8 + R, :]
        + rates[T + 8 : T + 8 + R, :]
        + rates[2 * T + 8 : 2 * T + 8 + R, :]
        + rates[3 * T + 8 : 3 * T + 8 + R, :]
    )

    routes = (
        ("gx", ix - 1, ix > 0, ix < nx - 1),
        ("gx", ix + 1, ix < nx - 1, ix > 0),
        ("gy", iy - 1, iy > 0, iy < ny - 1),
        ("gy", iy + 1, iy < ny - 1, iy > 0),
    )

    def edges(send, recv, ssem, rsem):
        def copy(e):
            return pltpu.make_async_remote_copy(
                src_ref=send.at[min(e, 2)],
                dst_ref=recv.at[e],
                send_sem=ssem.at[e],
                recv_sem=rsem.at[e],
                device_id={routes[e][0]: routes[e][1]},
                device_id_type=MESH,
            )

        def start():
            for e in range(4):
                @pl.when(routes[e][2])
                def _(e=e):
                    copy(e).start()

                @pl.when(jnp.logical_not(routes[e][3]))
                def _(e=e):
                    recv[e] = jnp.zeros(recv.shape[1:], F32)

        def wait():
            for e in range(4):
                @pl.when(routes[e][3])
                def _(e=e):
                    copy(e).wait_recv()

        def drain():
            for e in range(4):
                @pl.when(routes[e][2])
                def _(e=e):
                    copy(e).wait_send()

        return start, wait, drain

    def share(buf, sem, axis, me, n, source=None):
        def copy(src, dst, device):
            return pltpu.make_async_remote_copy(
                src_ref=src,
                dst_ref=dst,
                send_sem=sem.at[0],
                recv_sem=sem.at[1],
                device_id=device,
                device_id_type=MESH,
            )

        def start(store):
            store(buf.at[me])
            for d in range(1, n):
                other, device = peer_of(axis, me, n, d)
                copy(buf.at[me] if source is None else source.at[other], buf.at[me], device).start()

        rest = buf.at[pl.ds(0, n - 1)]
        whole = copy(rest, rest, peer_of(axis, me, n, 1)[1])

        def wait():
            whole.wait_recv()

        def finish():
            wait()
            parts = [buf[k] for k in range(n)]
            while len(parts) > 1:
                parts = [
                    parts[i] + parts[i + 1] if i + 1 < len(parts) else parts[i]
                    for i in range(0, len(parts), 2)
                ]
            return parts[0]

        def drain():
            whole.wait_send()

        return start, finish, drain, wait

    half = N // 2

    def pack(v):
        turned = pltpu.roll(v, K, 1)
        tail = pltpu.roll(v, 0, 1, stride=2 * N, stride_axis=0)
        mine = lax.div(lane, 2 * N) == lax.rem(sub + K // (2 * N), N)
        tail = jnp.sum(jnp.where(mine, tail, 0.0), axis=0, keepdims=True)
        low = lax.broadcasted_iota(jnp.int32, (half, LANES), 1) < K
        return jnp.where(low, v[0:half], turned[half:N]), tail

    def unpack(t):
        body = jnp.concatenate([t[0:half], pltpu.roll(t[0:half], K, 1)], axis=0)
        spread = jnp.broadcast_to(t[half : half + 1], (N, LANES))
        tail = spread
        for j in range(1, N):
            tail = jnp.where(sub == j, pltpu.roll(spread, LANES - 2 * N * j, 1), tail)
        return jnp.where(lane < K, body, jnp.where(lane < Z, tail, 0.0))

    drains = []

    def reduction(s, value):
        xgroup = everyone if direct else axes[0]
        xstart, xfinish, xdrain, _ = share(px_buf.at[s], px_s.at[s], *xgroup)
        drains.append(xdrain)

        def put(parts):
            def store(ref):
                ref[0:half] = parts[0]
                ref[half : half + 1] = parts[1]

            return store

        parts = pack(value)
        if direct:
            xstart(put(parts))
            return lambda: unpack(xfinish())
        ystart, yfinish, ydrain, _ = share(py_buf.at[s], py_s.at[s], *axes[1])
        drains.append(ydrain)
        ystart(put(parts))

        def finish():
            t = yfinish()
            xstart(put((t[0:half], t[half : half + 1])))
            return unpack(xfinish())

        return finish

    e0_start, e0_wait, e0_drain = edges(edge_send, edge_recv, edge_ssem, edge_rsem)
    e1_start, e1_wait, e1_drain = edges(eb_send, eb_recv, eb_ssem, eb_rsem)
    e2_start, e2_wait, e2_drain = edges(ew_send, ew_recv, ew_ssem, ew_rsem)
    drains += [e0_drain, e1_drain, e2_drain]

    def slots(shape, r):
        at = lax.broadcasted_iota(jnp.int32, shape, len(shape) - 1)
        return (at == 2 * r) | (at == (2 * r - 1) % LANES)

    def tuck(packed, r, f):
        return jnp.where(slots(f.shape, r), pltpu.roll(f, 2 * r, len(f.shape) - 1), packed)

    with jax.named_scope("packp"):
        lane_of = lax.broadcasted_iota(jnp.int32, (R, LANES), 1)
        sides = jnp.where(lane_of == 0, rates[2 * T + 8 : 2 * T + 8 + R, :], rates[3 * T + 8 : 3 * T + 8 + R, :])
        rate_side = jnp.zeros((N, LANES), F32)
        for i in range(R // 8):
            turned = pltpu.roll(sides[i * 8 : i * 8 + 8], 16 * i, 1, stride=2, stride_axis=0)
            mine = (lane == 2 * (sub + 8 * i)) | (lane == lax.rem(2 * (sub + 8 * i) + LANES - 1, LANES))
            rate_side = rate_side + jnp.where(mine, turned, 0.0)
        rate_side = jnp.sum(rate_side, axis=0, keepdims=True)
        packed = jnp.zeros((N, LANES), F32)
        for r in range(R):
            f = panel_rows[pl.ds(r, N, stride=RP), :]
            fext[:, row_at(r + 1)] = f
            packed = tuck(packed, r, f)
            if r == 0:
                edge_send[0] = f * rate_row(0, 0)
            if r == R - 1:
                edge_send[1] = f * rate_row(1, R - 1)
        edge_send[2] = packed * rate_side

    with jax.named_scope("barrier"):
        pl.semaphore_wait(barrier, greeted)
    e0_start()

    def tell(way):
        device = {"gx": ix + (BUDDY if way == 0 else -BUDDY)}
        pl.semaphore_signal(ready.at[way], inc=1, device_id=device, device_id_type=MESH)

    def pass_on(first, last):
        for i in range(first, min(last, planes - 2) + 1):
            for way in (0, 1):
                @pl.when(plane == (i if way == 0 else planes - 1 - i))
                def _(way=way):
                    pl.semaphore_wait(ready.at[way], 1)
                    tell(way)

    def all_arrived():
        for way in (0, 1):
            last = plane == (planes - 1 if way == 0 else 0)

            @pl.when(last & (planes > 1))
            def _(way=way):
                pl.semaphore_wait(ready.at[way], 1)

    if direct and planes > 1:
        for way in (0, 1):
            @pl.when(plane == (0 if way == 0 else planes - 1))
            def _(way=way):
                tell(way)

    with jax.named_scope("split"):
        for c in range(CHUNKS):
            basis_in[c].wait()
            mine = slice(c * step, (c + 1) * step)
            below = slice(Z + c * step, Z + (c + 1) * step)

            packed = jnp.zeros((step, LANES), F32)
            for r in range(R):
                b = basis_rows[pl.ds(c * step * RP + r, step, stride=RP), :]
                hi = b.astype(BF)
                x_v[mine, row_at(r)] = hi
                x_v[below, row_at(r)] = (b - hi.astype(F32)).astype(BF)
                packed = tuck(packed, r, b)
            eb_send[2, mine] = packed * rate_side
            eb_send[0, mine] = basis_rows[pl.ds(c * step * RP, step, stride=RP), :] * rate_row(0, 0)
            eb_send[1, mine] = (
                basis_rows[pl.ds(c * step * RP + R - 1, step, stride=RP), :] * rate_row(1, R - 1)
            )

    e1_start()
    if direct:
        pass_on(1, 1)

    def stencil(from_right, from_left, finish):
        side = jnp.where(lax.rem(lane, 2) == 1, from_left, pltpu.roll(from_right, LANES - 2, 1))
        for r in range(R):
            beside = pltpu.roll(side, (LANES + 1 - 2 * r) % LANES, 1)
            f = fext[:, row_at(r + 1)]
            above = fext[:, row_at(r)] * rate_row(1, r - 1)
            below = fext[:, row_at(r + 2)] * rate_row(0, r + 1)
            west = jnp.where(
                lane == 0,
                beside,
                pltpu.roll(f * rate_row(3, r), 1, 1),
            )
            east = jnp.where(
                lane == LANES - 1,
                beside,
                pltpu.roll(f * rate_row(2, r), LANES - 1, 1),
            )
            finish(r, f, above + below + west + east - rate_row(4, r) * f)

    def put_pair(r, upper, lower):
        both = jnp.concatenate([upper, lower], axis=0)
        hi = both.astype(BF)
        low = both - hi.astype(F32)
        x_v[K:Z, row_at(r)] = hi
        x_v[Z + K : 2 * Z, row_at(r)] = low.astype(BF)
        return hi.astype(F32), low

    def products():
        halves = []
        for h in range(2):
            at = pl.ds(h * (sites // 2), sites // 2)
            for top in (0, Z):
                halves.append(dot_nt(x_v[top : top + Z, at], u_v[:, at], lax.Precision.DEFAULT))
        t_v[0:Z, 0 : 2 * N] = (halves[0] + halves[1]) * scale + (halves[2] + halves[3]) * scale
        turned = t_v[...].T
        return turned[0:N] + turned[N : 2 * N]

    mid = K // 2
    part = mid // ny
    m1_start, m1_finish, m1_drain, _ = share(my_buf, m_s.at[0], *axes[1], source=ms_buf)
    m2_start, m2_finish, m2_drain, _ = share(mx_buf, m_s.at[1], *axes[0])
    m3_start, _, m3_drain, m3_wait = share(mz_buf, m_s.at[2], *axes[1])
    drains += [m1_drain, m2_drain, m3_drain]

    with jax.named_scope("gram"):
        pieces = []
        for h in range(2):
            at = pl.ds(h * (sites // 2), sites // 2)
            pieces.append(dot_nt(x_v[0:K, at], x_v[0:K, at], lax.Precision.DEFAULT))
            pieces.append(dot_nt(x_v[Z : Z + K, at], x_v[0:K, at], lax.Precision.DEFAULT))
        cross = pieces[1] + pieces[3]
        full = (pieces[0] + pieces[2] + (cross + cross.T)) * scale
        full = jnp.concatenate([full[0:mid], full[mid:K]], axis=1)
        for p in range(ny):
            ms_buf[p] = full[p * part : (p + 1) * part]

        def put_own(ref):
            ref[...] = ms_buf[iy]

        m1_start(put_own)
    if direct:
        pass_on(2, planes)

    with jax.named_scope("ewait0"):
        e0_wait()
    with jax.named_scope("lat0"):
        t_v[...] = jnp.zeros_like(t_v)
        fext[:, 0:LANES] = edge_recv[1]
        fext[:, (R + 1) * LANES : (R + 2) * LANES] = edge_recv[0]
        zero = jnp.zeros((N, LANES), F32)

        def finish_first(r, f, w):
            wf[:, row_at(r)] = w
            hi, low = put_pair(r, w, zero)
            u_v[:, row_at(r)] = jnp.concatenate([hi[0:N], low[0:N]], axis=0).astype(BF)

        with jax.named_scope("sten0"):
            stencil(edge_recv[2], edge_recv[3], finish_first)
        with jax.named_scope("prod0"):
            value = products()
        if direct:
            all_arrived()
        finish0 = reduction(0, value)
    with jax.named_scope("packw"):
        packed = jnp.zeros((N, LANES), F32)
        for r in range(R):
            packed = tuck(packed, r, wf[:, row_at(r)])
        ew_send[0] = wf[:, row_at(0)] * rate_row(0, 0)
        ew_send[1] = wf[:, row_at(R - 1)] * rate_row(1, R - 1)
        ew_send[2] = packed * rate_side
    e2_start()

    with jax.named_scope("ewait1"):
        e1_wait()
    with jax.named_scope("esplit"):
        for e in range(4):
            at = pl.ds(sites + e * LANES, LANES)
            b = eb_recv[e]
            hi = b.astype(BF)
            x_v[0:K, at] = hi
            x_v[Z : Z + K, at] = (b - hi.astype(F32)).astype(BF)
            x_v[K:Z, at] = jnp.zeros((2 * N, LANES), BF)
            x_v[Z + K : 2 * Z, at] = jnp.zeros((2 * N, LANES), BF)

    def forward(ref, value):
        ref[...] = value

    with jax.named_scope("m12"):
        m = m1_finish()
        m2_start(lambda ref: forward(ref, m))
    with jax.named_scope("ewait2"):
        e2_wait()
        for e in range(4):
            wf[:, pl.ds(sites + e * LANES, LANES)] = ew_recv[e]
    with jax.named_scope("m23"):
        m_own = m2_finish()
        m3_start(lambda ref: forward(ref, m_own))

    with jax.named_scope("red0"):
        total = finish0()

    def combine(lhs, at):
        both = jnp.dot(lhs, x_v[0:Z, at], preferred_element_type=F32) + jnp.dot(
            lhs, x_v[Z : 2 * Z, at], preferred_element_type=F32
        )
        return both[0:N] + both[N : 2 * N]

    wide8 = 8 * LANES
    pm = jnp.where(lane < K, total, 0.0)
    with jax.named_scope("new0"):
        lhs = split_rows(pm)[:, 0:Z]
        at = pl.ds(sites, 4 * LANES)
        edge = wf[:, at] - combine(lhs, at)
        fext[:, 0:LANES] = edge[:, LANES : 2 * LANES]
        fext[:, (R + 1) * LANES : (R + 2) * LANES] = edge[:, 0:LANES]
        for i in range(R // 8):
            at = pl.ds(i * wide8, wide8)
            fext[:, pl.ds(LANES + i * wide8, wide8)] = wf[:, at] - combine(lhs, at)
    with jax.named_scope("lat1"):
        def finish_second(r, f, u):
            hi, low = put_pair(r, f, u)
            u_v[:, row_at(r)] = jnp.concatenate([hi[N : 2 * N], low[N : 2 * N]], axis=0).astype(BF)

        with jax.named_scope("sten1"):
            stencil(edge[:, 2 * LANES : 3 * LANES], edge[:, 3 * LANES : 4 * LANES], finish_second)
        with jax.named_scope("prod1"):
            value = products()
        finish1 = reduction(1, value)

    with jax.named_scope("mxfin"):
        m3_wait()
        m = jnp.concatenate([mz_buf[p] for p in range(ny)], axis=0)
        gram = rows_full(
            jnp.concatenate(
                [
                    jnp.where(lax.broadcasted_iota(jnp.int32, (mid, LANES), 1) < K, m, 0.0),
                    jnp.where(
                        lax.broadcasted_iota(jnp.int32, (mid, LANES), 1) < K,
                        pltpu.roll(m, LANES - K, 1),
                        0.0,
                    ),
                ],
                axis=0,
            )
        )
    G0 = Z
    with jax.named_scope("fac0"):
        own = pltpu.roll(total, G0 - K, 1)
        rest = 2.0 * pm - dot_nn(pm, gram)
        g = jnp.where((lane >= G0) & (lane < G0 + N), own - dot_nt(rest, rows_full(pm, G0)), 0.0)
        a = jnp.where(lane < K, rest - pm, jnp.where(lane == sub + K, 1.0, g))
        a = eliminate(a, G0, N)
        at_t = rows_full(a).T
        inv = pltpu.roll(a, LANES - K, 1)
        inv = jnp.where(lane < N, inv, 0.0)
        low1 = at_t[G0 : G0 + N]
        coefs[0] = pm + jnp.where((lane >= K) & (lane < KN), pltpu.roll(low1, K, 1), 0.0)
        row = lax.broadcasted_iota(jnp.int32, (LANES, LANES), 0)
        col = lax.broadcasted_iota(jnp.int32, (LANES, LANES), 1)
        inner = jnp.where((row < KN), at_t, 0.0)
        flow = dot_nn(inner, rows_full(jnp.where(lane < KN, a, 0.0)))
        in_b = (row < K) & (col < K)
        in_w = (row >= K) & (row < KN) & (col >= K) & (col < KN)
        eye = jnp.where(row == col, 1.0, 0.0)
        kmat = jnp.where(in_b, 2.0 * eye - gram, jnp.where(in_w, flow, -flow))
        dmat = jnp.where(in_b, eye, jnp.where(in_w, flow, 0.0))
        tmat = jnp.where((row >= K) & (row < KN) & (col < N), at_t, 0.0)
        m_v[0] = kmat
        m_v[1] = dmat
        m_v[2] = tmat
    with jax.named_scope("q1"):
        lhs = split_rows(inv)[:, 0 : 2 * N]
        for i in range(R // 8):
            at = pl.ds(i * wide8, wide8)
            both = jnp.dot(lhs, x_v[K:Z, at], preferred_element_type=F32) + jnp.dot(
                lhs, x_v[Z + K : 2 * Z, at], preferred_element_type=F32
            )
            q = both[0:N] + both[N : 2 * N]
            for u in range(8):
                first_v[pl.ds(i * 8 + u, N, stride=RP), :] = q[:, u * LANES : (u + 1) * LANES]

    with jax.named_scope("red1"):
        total = finish1()
    with jax.named_scope("fac1"):
        ep = jnp.where(lane < KN, total, 0.0)
        own = pltpu.roll(total, G0 - KN, 1)
        ek = dot_nn(ep, m_v[0])
        ed = dot_nn(ep, m_v[1])
        g = jnp.where((lane >= G0) & (lane < G0 + N), own - dot_nt(ek, rows_full(ep, G0)), 0.0)
        a = jnp.where(lane < KN, ed, jnp.where(lane == sub + KN, 1.0, g))
        a = eliminate(a, G0, N)
        lhs = split_rows(jnp.where(lane < KN, -a, a))[:, 0:Z]
    with jax.named_scope("coef1"):
        low2 = rows_full(a).T[G0 : G0 + N]
        es = dot_nn(ep, m_v[2])
        stack = jnp.where(lane < K, ep, jnp.where(lane < KN, pltpu.roll(es, K, 1), 0.0))
        stack = jnp.where((lane >= KN) & (lane < Z), pltpu.roll(low2, KN, 1), stack)
        coefs[1] = dot_nn(inv, rows_full(stack))
    with jax.named_scope("new1"):
        for i in range(R // 8):
            q = combine(lhs, pl.ds(i * wide8, wide8))
            for u in range(8):
                second_v[pl.ds(i * 8 + u, N, stride=RP), :] = q[:, u * LANES : (u + 1) * LANES]
    with jax.named_scope("drain"):
        for drain in drains:
            drain()


def deliver(
    R, first_v, second_v, coefs, first_hbm, second_hbm, one_hbm, two_hbm, coef_one, coef_two, sem
):
    copies = [
        pltpu.make_async_copy(first_v.at[:, pl.ds(0, R)], first_hbm, sem.at[0]),
        pltpu.make_async_copy(second_v.at[:, pl.ds(0, R)], second_hbm, sem.at[1]),
        pltpu.make_async_copy(coef_one, one_hbm, sem.at[2]),
        pltpu.make_async_copy(coef_two, two_hbm, sem.at[3]),
    ]
    for copy in copies[:2]:
        copy.start()
    coef_one[...] = coefs[0, :, 0 : coef_one.shape[1]]
    coef_two[...] = coefs[1, :, 0 : coef_two.shape[1]]
    for copy in copies[2:]:
        copy.start()
    for copy in copies:
        copy.wait()


def local(nx, ny, basis, panel, rate_codes):
    N, R, C = panel.shape
    K = basis.shape[0]
    assert C == LANES and 2 * K == LANES and N == 8
    vmem = pl.BlockSpec(memory_space=pltpu.VMEM)
    hbm = pl.BlockSpec(memory_space=pl.ANY)
    dma = pltpu.SemaphoreType.DMA
    sites = R * LANES
    group = nx * ny if nx * ny <= DIRECT else nx
    Z = K + 2 * N
    first, second, coefs = pl.pallas_call(
        functools.partial(kernel, nx, ny, K, N, R),
        out_shape=(
            pltpu.VMEM((N * (R + PAD), C), F32),
            pltpu.VMEM((N * (R + PAD), C), F32),
            pltpu.VMEM((2, N, C), F32),
        ),
        in_specs=[pl.BlockSpec(memory_space=pltpu.HBM)] * 3,
        out_specs=(vmem, vmem, vmem),
        scratch_shapes=[
            pltpu.VMEM((K, R + PAD, LANES), F32),
            pltpu.VMEM((N, R + PAD, LANES), F32),
            pltpu.VMEM((4 * R, LANES), jnp.int32),
            pltpu.VMEM((5 * (R + 16), LANES), F32),
            pltpu.VMEM((N, (R + 2) * LANES), F32),
            pltpu.VMEM((N, sites + 4 * LANES), F32),
            pltpu.VMEM((2 * Z, sites + 4 * LANES), BF),
            pltpu.VMEM((2 * N, sites), BF),
            pltpu.VMEM((3, LANES, LANES), F32),
            pltpu.VMEM((LANES, LANES), F32),
            pltpu.VMEM((3, N, LANES), F32),
            pltpu.VMEM((4, N, LANES), F32),
            pltpu.VMEM((3, K, LANES), F32),
            pltpu.VMEM((4, K, LANES), F32),
            pltpu.VMEM((3, N, LANES), F32),
            pltpu.VMEM((4, N, LANES), F32),
            pltpu.VMEM((ny, K // 2 // ny, LANES), F32),
            pltpu.VMEM((ny, K // 2 // ny, LANES), F32),
            pltpu.VMEM((nx, K // 2 // ny, LANES), F32),
            pltpu.VMEM((ny, K // 2 // ny, LANES), F32),
            pltpu.VMEM((2, ny, N // 2 + 1, LANES), F32),
            pltpu.VMEM((2, group, N // 2 + 1, LANES), F32),
            dma((2 + CHUNKS,)),
            dma((4,)),
            dma((4,)),
            dma((4,)),
            dma((4,)),
            dma((4,)),
            dma((4,)),
            pltpu.SemaphoreType.REGULAR((2,)),
            dma((3, 2)),
            dma((2, 2)),
            dma((2, 2)),
        ],
        compiler_params=pltpu.CompilerParams(
            collective_id=0, has_side_effects=True
        ),
    )(basis, panel, rate_codes.reshape(rate_codes.shape[0] * R, C))
    first, second, coef_one, coef_two = pl.pallas_call(
        functools.partial(deliver, R),
        out_shape=(
            jax.ShapeDtypeStruct((N, R, C), F32),
            jax.ShapeDtypeStruct((N, R, C), F32),
            jax.ShapeDtypeStruct((N, K + N), F32),
            jax.ShapeDtypeStruct((N, K + 2 * N), F32),
        ),
        in_specs=[vmem] * 3,
        out_specs=(hbm, hbm, hbm, hbm),
        scratch_shapes=[
            pltpu.VMEM((N, K + N), F32),
            pltpu.VMEM((N, K + 2 * N), F32),
            dma((4,)),
        ],
        compiler_params=pltpu.CompilerParams(vmem_limit_bytes=4 * 2**20),
    )(first.reshape(N, R + PAD, C), second.reshape(N, R + PAD, C), coefs)
    return first, second, coef_one.T, coef_two.T


def solution(mesh):
    spec = P(None, "gx", "gy")
    return jax.shard_map(
        functools.partial(local, mesh.shape["gx"], mesh.shape["gy"]),
        mesh=mesh,
        in_specs=(spec, spec, spec),
        out_specs=(spec, spec, P(), P()),
        check_vma=False,
    )
```

```python
import functools

import jax
import jax.numpy as jnp
from jax import lax
from jax.experimental import pallas as pl
from jax.experimental.pallas import tpu as pltpu
from jax.sharding import PartitionSpec as P

HIGH = lax.Precision.HIGHEST
MESH = pl.DeviceIdType.MESH
F32 = jnp.float32
BF = jnp.bfloat16
LANES = 128
CHUNKS = 4
DIRECT = 64
BUDDY = 2
PAD = 8


def dot_nn(a, b):
    return jnp.dot(a, b, precision=HIGH, preferred_element_type=F32)


def dot_nt(a, b, precision=HIGH):
    return lax.dot_general(
        a, b, (((1,), (1,)), ((), ())), precision=precision, preferred_element_type=F32
    )


def rows_full(v, at=0):
    parts = [v, jnp.zeros((LANES - at - v.shape[0], LANES), F32)]
    if at:
        parts.insert(0, jnp.zeros((at, LANES), F32))
    return jnp.concatenate(parts, axis=0)


def split(v):
    hi = v.astype(BF).astype(F32)
    return hi, v - hi


def split_rows(v):
    return jnp.concatenate(split(v), axis=0).astype(BF)


def eliminate(a, g0, n):
    sub = lax.broadcasted_iota(jnp.int32, a.shape, 0)
    cols = [jnp.broadcast_to(a[:, g0 + j : g0 + j + 1], a.shape) for j in range(n)]
    pivots = jnp.ones(a.shape, F32)
    for k in range(n):
        pivot = jnp.broadcast_to(cols[k][k : k + 1, :], a.shape)
        pivots = jnp.where(sub == k, pivot, pivots)
        if k == n - 1:
            break
        factor = jnp.where(sub > k, cols[k] * (1.0 / pivot), 0.0)
        for j in range(k + 1, n):
            cols[j] = cols[j] - factor * cols[j][k : k + 1, :]
        a = a - factor * a[k : k + 1, :]
    return a * (1.0 / jnp.sqrt(pivots))


def kernel(
    nx, ny, K, N, R,
    basis_hbm, panel_hbm, rate_hbm,
    first_v, second_v, coefs,
    basis_v, panel_v, rate_v, rates, fext, wf, x_v, m_v, t_v, g_v,
    edge_send, edge_recv, eb_send, eb_recv, ew_send, ew_recv, ms_buf, my_buf, mx_buf, mz_buf, py_buf, px_buf,
    in_sem, edge_ssem, edge_rsem, eb_ssem, eb_rsem, ew_ssem, ew_rsem, ready,
    m_s, py_s, px_s,
):
    ix, iy = lax.axis_index("gx"), lax.axis_index("gy")
    sites = R * LANES
    scale = 1.0 / (sites * nx * ny)
    lane = lax.broadcasted_iota(jnp.int32, (N, LANES), 1)
    sub = lax.broadcasted_iota(jnp.int32, (N, LANES), 0)
    KN = K + N
    Z = K + 2 * N
    HI = 2 * N
    LO = HI + Z
    EXT = sites
    EDGE = sites + LANES
    RP = R + PAD
    T = R + 16

    basis_rows = basis_v.reshape(K * RP, LANES)
    panel_rows = panel_v.reshape(N * RP, LANES)

    axes = (("gx", ix, nx), ("gy", iy, ny))
    everyone = ("all", ix * ny + iy, nx * ny)
    direct = nx * ny <= DIRECT and nx % BUDDY == 0

    def peer_of(axis, me, n, d):
        other = lax.rem(me + d, n)
        if axis == "all":
            return other, {"gx": lax.div(other, ny), "gy": lax.rem(other, ny)}
        return other, {axis: other}

    with jax.named_scope("dma0"):
        step = K // CHUNKS
        panel_in = pltpu.make_async_copy(panel_hbm, panel_v.at[:, pl.ds(0, R)], in_sem.at[0])
        rate_in = pltpu.make_async_copy(rate_hbm, rate_v, in_sem.at[1])
        panel_in.start()
        rate_in.start()

    barrier = pltpu.get_barrier_semaphore()

    def greet(device):
        pl.semaphore_signal(barrier, inc=1, device_id=device, device_id_type=MESH)

    if direct:
        planes = nx // BUDDY
        plane = lax.div(ix, BUDDY)
        home = plane * BUDDY
        group = BUDDY * ny
        seat = (ix - home) * ny + iy
        mates = []
        for d in range(1, group):
            other = lax.rem(seat + d, group)
            mates.append({"gx": home + lax.div(other, ny), "gy": lax.rem(other, ny)})
        outer = [
            ((ix == home) & (ix > 0), ix - 1),
            ((ix == home + BUDDY - 1) & (ix < nx - 1), ix + 1),
        ]
        greeted = group - 1 + plane
        for there, device in outer:
            greeted = greeted + jnp.where(there, 1, 0)

            @pl.when(there)
            def _(device=device):
                greet({"gx": device})

        for device in mates:
            greet(device)
        for d in range(1, planes):
            @pl.when(plane + d < planes)
            def _(d=d):
                greet({"gx": ix + d * BUDDY})

    else:
        greeted = 0
        for axis, me, n in axes:
            for d in range(1, n):
                greet(peer_of(axis, me, n, d)[1])
                greeted += 1

    basis_in = []
    for c in range(CHUNKS):
        part = pl.ds(c * step, step)
        basis_in.append(
            pltpu.make_async_copy(
                basis_hbm.at[part], basis_v.at[part, pl.ds(0, R)], in_sem.at[2 + c]
            )
        )
        basis_in[-1].start()
    def row_at(r):
        return pl.ds(r * LANES, LANES)

    def rate_row(d, r):
        return rates[pl.ds(d * T + 8 + r, 1), :]

    with jax.named_scope("inwait"):
        panel_in.wait()
        rate_in.wait()
    for d in range(4):
        rates[d * T : d * T + 8, :] = jnp.ones((8, LANES), F32)
        rates[d * T + 8 + R : (d + 1) * T, :] = jnp.ones((8, LANES), F32)
        rates[d * T + 8 : d * T + 8 + R, :] = (
            rate_v[d * R : (d + 1) * R, :].astype(F32) * 0.125
        )
    rates[4 * T + 8 : 4 * T + 8 + R, :] = (
        rates[8 : 8 + R, :]
        + rates[T + 8 : T + 8 + R, :]
        + rates[2 * T + 8 : 2 * T + 8 + R, :]
        + rates[3 * T + 8 : 3 * T + 8 + R, :]
    )

    routes = (
        ("gx", ix - 1, ix > 0, ix < nx - 1),
        ("gx", ix + 1, ix < nx - 1, ix > 0),
        ("gy", iy - 1, iy > 0, iy < ny - 1),
        ("gy", iy + 1, iy < ny - 1, iy > 0),
    )

    def edges(send, recv, ssem, rsem):
        def copy(e):
            return pltpu.make_async_remote_copy(
                src_ref=send.at[min(e, 2)],
                dst_ref=recv.at[e],
                send_sem=ssem.at[e],
                recv_sem=rsem.at[e],
                device_id={routes[e][0]: routes[e][1]},
                device_id_type=MESH,
            )

        def start():
            for e in range(4):
                @pl.when(routes[e][2])
                def _(e=e):
                    copy(e).start()

                @pl.when(jnp.logical_not(routes[e][3]))
                def _(e=e):
                    recv[e] = jnp.zeros(recv.shape[1:], F32)

        def wait():
            for e in range(4):
                @pl.when(routes[e][3])
                def _(e=e):
                    copy(e).wait_recv()

        def drain():
            for e in range(4):
                @pl.when(routes[e][2])
                def _(e=e):
                    copy(e).wait_send()

        return start, wait, drain

    def share(buf, sem, axis, me, n, source=None):
        def copy(src, dst, device):
            return pltpu.make_async_remote_copy(
                src_ref=src,
                dst_ref=dst,
                send_sem=sem.at[0],
                recv_sem=sem.at[1],
                device_id=device,
                device_id_type=MESH,
            )

        def start(store):
            store(buf.at[me])
            for d in range(1, n):
                other, device = peer_of(axis, me, n, d)
                copy(buf.at[me] if source is None else source.at[other], buf.at[me], device).start()

        rest = buf.at[pl.ds(0, n - 1)]
        whole = copy(rest, rest, peer_of(axis, me, n, 1)[1])

        def wait():
            whole.wait_recv()

        def finish():
            wait()
            parts = [buf[k] for k in range(n)]
            while len(parts) > 1:
                parts = [
                    parts[i] + parts[i + 1] if i + 1 < len(parts) else parts[i]
                    for i in range(0, len(parts), 2)
                ]
            return parts[0]

        def drain():
            whole.wait_send()

        return start, finish, drain, wait

    half = N // 2

    def pack(v):
        turned = pltpu.roll(v, K, 1)
        tail = pltpu.roll(v, 0, 1, stride=2 * N, stride_axis=0)
        mine = lax.div(lane, 2 * N) == lax.rem(sub + K // (2 * N), N)
        tail = jnp.sum(jnp.where(mine, tail, 0.0), axis=0, keepdims=True)
        low = lax.broadcasted_iota(jnp.int32, (half, LANES), 1) < K
        return jnp.where(low, v[0:half], turned[half:N]), tail

    def unpack(t):
        body = jnp.concatenate([t[0:half], pltpu.roll(t[0:half], K, 1)], axis=0)
        spread = jnp.broadcast_to(t[half : half + 1], (N, LANES))
        tail = spread
        for j in range(1, N):
            tail = jnp.where(sub == j, pltpu.roll(spread, LANES - 2 * N * j, 1), tail)
        return jnp.where(lane < K, body, jnp.where(lane < Z, tail, 0.0))

    drains = []

    def reduction(s, value):
        xgroup = everyone if direct else axes[0]
        xstart, xfinish, xdrain, _ = share(px_buf.at[s], px_s.at[s], *xgroup)
        drains.append(xdrain)

        def put(parts):
            def store(ref):
                ref[0:half] = parts[0]
                ref[half : half + 1] = parts[1]

            return store

        parts = pack(value)
        if direct:
            xstart(put(parts))
            return lambda: unpack(xfinish())
        ystart, yfinish, ydrain, _ = share(py_buf.at[s], py_s.at[s], *axes[1])
        drains.append(ydrain)
        ystart(put(parts))

        def finish():
            t = yfinish()
            xstart(put((t[0:half], t[half : half + 1])))
            return unpack(xfinish())

        return finish

    e0_start, e0_wait, e0_drain = edges(edge_send, edge_recv, edge_ssem, edge_rsem)
    e1_start, e1_wait, e1_drain = edges(eb_send, eb_recv, eb_ssem, eb_rsem)
    e2_start, e2_wait, e2_drain = edges(ew_send, ew_recv, ew_ssem, ew_rsem)
    drains += [e0_drain, e1_drain, e2_drain]

    def slots(shape, r):
        at = lax.broadcasted_iota(jnp.int32, shape, len(shape) - 1)
        return (at == 2 * r) | (at == (2 * r - 1) % LANES)

    def tuck(packed, r, f):
        return jnp.where(slots(f.shape, r), pltpu.roll(f, 2 * r, len(f.shape) - 1), packed)

    with jax.named_scope("packp"):
        lane_of = lax.broadcasted_iota(jnp.int32, (R, LANES), 1)
        sides = jnp.where(lane_of == 0, rates[2 * T + 8 : 2 * T + 8 + R, :], rates[3 * T + 8 : 3 * T + 8 + R, :])
        rate_side = jnp.zeros((N, LANES), F32)
        for i in range(R // 8):
            turned = pltpu.roll(sides[i * 8 : i * 8 + 8], 16 * i, 1, stride=2, stride_axis=0)
            mine = (lane == 2 * (sub + 8 * i)) | (lane == lax.rem(2 * (sub + 8 * i) + LANES - 1, LANES))
            rate_side = rate_side + jnp.where(mine, turned, 0.0)
        rate_side = jnp.sum(rate_side, axis=0, keepdims=True)
        packed = jnp.zeros((N, LANES), F32)
        for r in range(R):
            f = panel_rows[pl.ds(r, N, stride=RP), :]
            fext[:, row_at(r + 1)] = f
            packed = tuck(packed, r, f)
            if r == 0:
                edge_send[0] = f * rate_row(0, 0)
            if r == R - 1:
                edge_send[1] = f * rate_row(1, R - 1)
        edge_send[2] = packed * rate_side

    with jax.named_scope("barrier"):
        pl.semaphore_wait(barrier, greeted)
    e0_start()

    if direct:
        for device in mates:
            pl.semaphore_signal(ready.at[0], inc=1, device_id=device, device_id_type=MESH)
        for d in range(1, planes):
            @pl.when(plane >= d)
            def _(d=d):
                device = {"gx": ix - d * BUDDY}
                pl.semaphore_signal(ready.at[1], inc=1, device_id=device, device_id_type=MESH)

    def all_arrived():
        pl.semaphore_wait(ready.at[0], group - 1)

        @pl.when(plane < planes - 1)
        def _():
            pl.semaphore_wait(ready.at[1], planes - 1 - plane)

    with jax.named_scope("split"):
        for c in range(CHUNKS):
            basis_in[c].wait()
            mine = slice(c * step, (c + 1) * step)
            above = slice(HI + c * step, HI + (c + 1) * step)
            below = slice(LO + c * step, LO + (c + 1) * step)

            packed = jnp.zeros((step, LANES), F32)
            for r in range(R):
                b = basis_rows[pl.ds(c * step * RP + r, step, stride=RP), :]
                hi = b.astype(BF)
                x_v[above, row_at(r)] = hi
                x_v[below, row_at(r)] = (b - hi.astype(F32)).astype(BF)
                packed = tuck(packed, r, b)
            hi = packed.astype(BF)
            x_v[above, pl.ds(EXT, LANES)] = hi
            x_v[below, pl.ds(EXT, LANES)] = (packed - hi.astype(F32)).astype(BF)
            eb_send[2, mine] = packed * rate_side
            eb_send[0, mine] = basis_rows[pl.ds(c * step * RP, step, stride=RP), :] * rate_row(0, 0)
            eb_send[1, mine] = (
                basis_rows[pl.ds(c * step * RP + R - 1, step, stride=RP), :] * rate_row(1, R - 1)
            )

    e1_start()

    def sides(from_right, from_left):
        side = jnp.where(lax.rem(lane, 2) == 1, from_left, pltpu.roll(from_right, LANES - 2, 1))
        return lambda r: pltpu.roll(side, (LANES + 1 - 2 * r) % LANES, 1)

    def stencil(beside, finish):
        for r in range(R):
            f = fext[:, row_at(r + 1)]
            above = fext[:, row_at(r)] * rate_row(1, r - 1)
            below = fext[:, row_at(r + 2)] * rate_row(0, r + 1)
            west = pltpu.roll(f * rate_row(3, r), 1, 1)
            east = pltpu.roll(f * rate_row(2, r), LANES - 1, 1)
            other = beside(r)
            west = jnp.where(lane == 0, other, west)
            east = jnp.where(lane == LANES - 1, other, east)
            finish(r, f, above + below + west + east - rate_row(4, r) * f)

    def put_pair(at, upper, lower):
        both = jnp.concatenate([upper, lower], axis=0)
        hi = both.astype(BF)
        low = both - hi.astype(F32)
        x_v[HI + K : LO, at] = hi
        x_v[LO + K : LO + Z, at] = low.astype(BF)
        return hi.astype(F32), low

    def put_rhs(at, hi, low):
        x_v[0:HI, at] = jnp.concatenate([hi, low], axis=0).astype(BF)

    def against(at, width):
        return [
            dot_nt(x_v[top : top + Z, at], x_v[0:width, at], lax.Precision.DEFAULT)
            for top in (HI, LO)
        ]

    def halves(width):
        parts = [against(pl.ds(h * (sites // 2), sites // 2), width) for h in range(2)]
        return [parts[0][i] * scale + parts[1][i] * scale for i in range(2)]

    def turned(total):
        t_v[0:Z, 0:HI] = total
        value = t_v[...].T
        return value[0:N] + value[N:HI]

    mid = K // 2
    part = mid // ny
    m1_start, m1_finish, m1_drain, _ = share(my_buf, m_s.at[0], *axes[1], source=ms_buf)
    m2_start, m2_finish, m2_drain, _ = share(mx_buf, m_s.at[1], *axes[0])
    m3_start, _, m3_drain, m3_wait = share(mz_buf, m_s.at[2], *axes[1])
    drains += [m1_drain, m2_drain, m3_drain]

    zero = jnp.zeros((N, LANES), F32)
    with jax.named_scope("sten0"):
        t_v[...] = jnp.zeros_like(t_v)
        fext[:, 0:LANES] = zero
        fext[:, (R + 1) * LANES : (R + 2) * LANES] = zero
        columns = [zero]

        def finish_first(r, f, w):
            wf[:, row_at(r)] = w
            hi, low = put_pair(row_at(r), w, zero)
            put_rhs(row_at(r), hi[0:N], low[0:N])

        stencil(lambda r: 0.0, finish_first)
    with jax.named_scope("tuck0"):
        for r in range(R):
            columns[0] = tuck(columns[0], r, wf[:, row_at(r)])
    with jax.named_scope("gram"):
        high, low = halves(HI + K)
        first = (high + low)[:, 0:HI]
        g_v[...] = jnp.zeros_like(g_v)
        g_v[0, 0:K, 0 : HI + K] = (high + low)[0:K]
        g_v[1, 0:K, 0 : HI + K] = low[0:K]
        straight = g_v[0]
        flipped = g_v[1].T[HI : HI + K]
        is_low = lax.broadcasted_iota(jnp.int32, (mid, LANES), 1) < K
        full = jnp.where(
            is_low,
            pltpu.roll(straight[0:mid], LANES - HI, 1) + flipped[0:mid],
            pltpu.roll(straight[mid:K], K - HI, 1) + pltpu.roll(flipped[mid:K], K, 1),
        )
        for p in range(ny):
            ms_buf[p] = full[p * part : (p + 1) * part]

        def put_own(ref):
            ref[...] = ms_buf[iy]

        m1_start(put_own)

    with jax.named_scope("ewait0"):
        e0_wait()
    with jax.named_scope("lat0"):
        from_below, from_above, from_right, from_left = [edge_recv[e] for e in range(4)]
        gain = jnp.where(
            lax.rem(lane, 2) == 0, pltpu.roll(from_left, 1, 1), pltpu.roll(from_right, LANES - 1, 1)
        )
        column = columns[0]
        column = jnp.where(slots(zero.shape, 0), column + from_above, column)
        column = jnp.where(
            slots(zero.shape, R - 1), column + pltpu.roll(from_below, 2 * (R - 1), 1), column
        )
        ends = ((0, from_above), (R - 1, from_below))
        for r, extra in ends:
            w = wf[:, row_at(r)]
            put_pair(row_at(r), zero, w + 0.5 * extra)
            put_rhs(row_at(r), *split(extra))
            wf[:, row_at(r)] = w + extra
        put_pair(pl.ds(EXT, LANES), zero, column + 0.5 * gain)
        put_rhs(pl.ds(EXT, LANES), *split(gain))
        last = against(pl.ds(sites - LANES, 2 * LANES), HI)
        top = against(row_at(0), HI)
        value = turned(first + ((last[0] + last[1]) + (top[0] + top[1])) * scale)
        if direct:
            all_arrived()
        finish0 = reduction(0, value)
    with jax.named_scope("packw"):
        beside = sides(from_right, from_left)
        outer = (lane == 0) | (lane == LANES - 1)
        for r in range(R):
            wf[:, row_at(r)] = wf[:, row_at(r)] + jnp.where(outer, beside(r), 0.0)
        ew_send[0] = wf[:, row_at(0)] * rate_row(0, 0)
        ew_send[1] = wf[:, row_at(R - 1)] * rate_row(1, R - 1)
        ew_send[2] = (column + gain) * rate_side
    e2_start()

    with jax.named_scope("ewait1"):
        e1_wait()
    with jax.named_scope("esplit"):
        for e in range(4):
            at = pl.ds(EDGE + e * LANES, LANES)
            b = eb_recv[e]
            hi = b.astype(BF)
            x_v[HI : HI + K, at] = hi
            x_v[LO : LO + K, at] = (b - hi.astype(F32)).astype(BF)
            x_v[HI + K : LO, at] = jnp.zeros((2 * N, LANES), BF)
            x_v[LO + K : LO + Z, at] = jnp.zeros((2 * N, LANES), BF)

    def forward(ref, value):
        ref[...] = value

    with jax.named_scope("m12"):
        m = m1_finish()
        m2_start(lambda ref: forward(ref, m))
    with jax.named_scope("ewait2"):
        e2_wait()
        for e in range(4):
            wf[:, pl.ds(EDGE + e * LANES, LANES)] = ew_recv[e]
    with jax.named_scope("red0"):
        total = finish0()

    def combine(lhs, at):
        both = jnp.dot(lhs, x_v[HI:LO, at], preferred_element_type=F32) + jnp.dot(
            lhs, x_v[LO : LO + Z, at], preferred_element_type=F32
        )
        return both[0:N] + both[N : 2 * N]

    wide8 = 8 * LANES
    pm = jnp.where(lane < K, total, 0.0)
    with jax.named_scope("new0"):
        lhs = split_rows(pm)[:, 0:Z]
        at = pl.ds(EDGE, 4 * LANES)
        edge = wf[:, at] - combine(lhs, at)
        fext[:, 0:LANES] = edge[:, LANES : 2 * LANES]
        fext[:, (R + 1) * LANES : (R + 2) * LANES] = edge[:, 0:LANES]
        for i in range(R // 8):
            at = pl.ds(i * wide8, wide8)
            fext[:, pl.ds(LANES + i * wide8, wide8)] = wf[:, at] - combine(lhs, at)
    with jax.named_scope("lat1"):
        def finish_second(r, f, u):
            hi, low = put_pair(row_at(r), f, u)
            put_rhs(row_at(r), hi[N:HI], low[N:HI])

        with jax.named_scope("sten1"):
            stencil(
                sides(edge[:, 2 * LANES : 3 * LANES], edge[:, 3 * LANES : 4 * LANES]), finish_second
            )
        with jax.named_scope("prod1"):
            high, low = halves(HI)
            value = turned(high + low)
        finish1 = reduction(1, value)

    with jax.named_scope("mxfin"):
        m_own = m2_finish()
        m3_start(lambda ref: forward(ref, m_own))
        m3_wait()
        m = jnp.concatenate([mz_buf[p] for p in range(ny)], axis=0)
        gram = rows_full(
            jnp.concatenate(
                [
                    jnp.where(lax.broadcasted_iota(jnp.int32, (mid, LANES), 1) < K, m, 0.0),
                    jnp.where(
                        lax.broadcasted_iota(jnp.int32, (mid, LANES), 1) < K,
                        pltpu.roll(m, LANES - K, 1),
                        0.0,
                    ),
                ],
                axis=0,
            )
        )
    G0 = Z
    with jax.named_scope("fac0"):
        own = (
            pltpu.roll(total, G0 - K, 1)
            + pltpu.roll(total, G0 - KN, 1)
            + pltpu.roll(rows_full(total).T[KN:Z], G0, 1)
        )
        rest = 2.0 * pm - dot_nn(pm, gram)
        g = jnp.where((lane >= G0) & (lane < G0 + N), own - dot_nt(rest, rows_full(pm, G0)), 0.0)
        a = jnp.where(lane < K, rest - pm, jnp.where(lane == sub + K, 1.0, g))
        a = eliminate(a, G0, N)
        at_t = rows_full(a).T
        inv = pltpu.roll(a, LANES - K, 1)
        inv = jnp.where(lane < N, inv, 0.0)
        low1 = at_t[G0 : G0 + N]
        coefs[0] = pm + jnp.where((lane >= K) & (lane < KN), pltpu.roll(low1, K, 1), 0.0)
        row = lax.broadcasted_iota(jnp.int32, (LANES, LANES), 0)
        col = lax.broadcasted_iota(jnp.int32, (LANES, LANES), 1)
        inner = jnp.where((row < KN), at_t, 0.0)
        flow = dot_nn(inner, rows_full(jnp.where(lane < KN, a, 0.0)))
        in_b = (row < K) & (col < K)
        in_w = (row >= K) & (row < KN) & (col >= K) & (col < KN)
        eye = jnp.where(row == col, 1.0, 0.0)
        kmat = jnp.where(in_b, 2.0 * eye - gram, jnp.where(in_w, flow, -flow))
        dmat = jnp.where(in_b, eye, jnp.where(in_w, flow, 0.0))
        tmat = jnp.where((row >= K) & (row < KN) & (col < N), at_t, 0.0)
        m_v[0] = kmat
        m_v[1] = dmat
        m_v[2] = tmat
    with jax.named_scope("q1"):
        lhs = split_rows(inv)[:, 0 : 2 * N]
        for i in range(R // 8):
            at = pl.ds(i * wide8, wide8)
            both = jnp.dot(lhs, x_v[HI + K : LO, at], preferred_element_type=F32) + jnp.dot(
                lhs, x_v[LO + K : LO + Z, at], preferred_element_type=F32
            )
            q = both[0:N] + both[N : 2 * N]
            for u in range(8):
                first_v[pl.ds(i * 8 + u, N, stride=RP), :] = q[:, u * LANES : (u + 1) * LANES]

    with jax.named_scope("red1"):
        total = finish1()
    with jax.named_scope("fac1"):
        ep = jnp.where(lane < KN, total, 0.0)
        own = pltpu.roll(total, G0 - KN, 1)
        ek = dot_nn(ep, m_v[0])
        ed = dot_nn(ep, m_v[1])
        g = jnp.where((lane >= G0) & (lane < G0 + N), own - dot_nt(ek, rows_full(ep, G0)), 0.0)
        a = jnp.where(lane < KN, ed, jnp.where(lane == sub + KN, 1.0, g))
        a = eliminate(a, G0, N)
        lhs = split_rows(jnp.where(lane < KN, -a, a))[:, 0:Z]
    with jax.named_scope("coef1"):
        low2 = rows_full(a).T[G0 : G0 + N]
        es = dot_nn(ep, m_v[2])
        stack = jnp.where(lane < K, ep, jnp.where(lane < KN, pltpu.roll(es, K, 1), 0.0))
        stack = jnp.where((lane >= KN) & (lane < Z), pltpu.roll(low2, KN, 1), stack)
        coefs[1] = dot_nn(inv, rows_full(stack))
    with jax.named_scope("new1"):
        for i in range(R // 8):
            q = combine(lhs, pl.ds(i * wide8, wide8))
            for u in range(8):
                second_v[pl.ds(i * 8 + u, N, stride=RP), :] = q[:, u * LANES : (u + 1) * LANES]
    with jax.named_scope("drain"):
        for drain in drains:
            drain()


def deliver(
    R, first_v, second_v, coefs, first_hbm, second_hbm, one_hbm, two_hbm, coef_one, coef_two, sem
):
    copies = [
        pltpu.make_async_copy(first_v.at[:, pl.ds(0, R)], first_hbm, sem.at[0]),
        pltpu.make_async_copy(second_v.at[:, pl.ds(0, R)], second_hbm, sem.at[1]),
        pltpu.make_async_copy(coef_one, one_hbm, sem.at[2]),
        pltpu.make_async_copy(coef_two, two_hbm, sem.at[3]),
    ]
    for copy in copies[:2]:
        copy.start()
    coef_one[...] = coefs[0, :, 0 : coef_one.shape[1]]
    coef_two[...] = coefs[1, :, 0 : coef_two.shape[1]]
    for copy in copies[2:]:
        copy.start()
    for copy in copies:
        copy.wait()


def local(nx, ny, basis, panel, rate_codes):
    N, R, C = panel.shape
    K = basis.shape[0]
    assert C == LANES and 2 * K == LANES and N == 8
    vmem = pl.BlockSpec(memory_space=pltpu.VMEM)
    hbm = pl.BlockSpec(memory_space=pl.ANY)
    dma = pltpu.SemaphoreType.DMA
    sites = R * LANES
    group = nx * ny if nx * ny <= DIRECT else nx
    Z = K + 2 * N
    first, second, coefs = pl.pallas_call(
        functools.partial(kernel, nx, ny, K, N, R),
        out_shape=(
            pltpu.VMEM((N * (R + PAD), C), F32),
            pltpu.VMEM((N * (R + PAD), C), F32),
            pltpu.VMEM((2, N, C), F32),
        ),
        in_specs=[pl.BlockSpec(memory_space=pltpu.HBM)] * 3,
        out_specs=(vmem, vmem, vmem),
        scratch_shapes=[
            pltpu.VMEM((K, R + PAD, LANES), F32),
            pltpu.VMEM((N, R + PAD, LANES), F32),
            pltpu.VMEM((4 * R, LANES), jnp.int32),
            pltpu.VMEM((5 * (R + 16), LANES), F32),
            pltpu.VMEM((N, (R + 2) * LANES), F32),
            pltpu.VMEM((N, sites + 5 * LANES), F32),
            pltpu.VMEM((2 * N + 2 * Z, sites + 5 * LANES), BF),
            pltpu.VMEM((3, LANES, LANES), F32),
            pltpu.VMEM((LANES, LANES), F32),
            pltpu.VMEM((2, LANES, LANES), F32),
            pltpu.VMEM((3, N, LANES), F32),
            pltpu.VMEM((4, N, LANES), F32),
            pltpu.VMEM((3, K, LANES), F32),
            pltpu.VMEM((4, K, LANES), F32),
            pltpu.VMEM((3, N, LANES), F32),
            pltpu.VMEM((4, N, LANES), F32),
            pltpu.VMEM((ny, K // 2 // ny, LANES), F32),
            pltpu.VMEM((ny, K // 2 // ny, LANES), F32),
            pltpu.VMEM((nx, K // 2 // ny, LANES), F32),
            pltpu.VMEM((ny, K // 2 // ny, LANES), F32),
            pltpu.VMEM((2, ny, N // 2 + 1, LANES), F32),
            pltpu.VMEM((2, group, N // 2 + 1, LANES), F32),
            dma((2 + CHUNKS,)),
            dma((4,)),
            dma((4,)),
            dma((4,)),
            dma((4,)),
            dma((4,)),
            dma((4,)),
            pltpu.SemaphoreType.REGULAR((2,)),
            dma((3, 2)),
            dma((2, 2)),
            dma((2, 2)),
        ],
        compiler_params=pltpu.CompilerParams(
            collective_id=0, has_side_effects=True
        ),
    )(basis, panel, rate_codes.reshape(rate_codes.shape[0] * R, C))
    first, second, coef_one, coef_two = pl.pallas_call(
        functools.partial(deliver, R),
        out_shape=(
            jax.ShapeDtypeStruct((N, R, C), F32),
            jax.ShapeDtypeStruct((N, R, C), F32),
            jax.ShapeDtypeStruct((N, K + N), F32),
            jax.ShapeDtypeStruct((N, K + 2 * N), F32),
        ),
        in_specs=[vmem] * 3,
        out_specs=(hbm, hbm, hbm, hbm),
        scratch_shapes=[
            pltpu.VMEM((N, K + N), F32),
            pltpu.VMEM((N, K + 2 * N), F32),
            dma((4,)),
        ],
        compiler_params=pltpu.CompilerParams(vmem_limit_bytes=4 * 2**20),
    )(first.reshape(N, R + PAD, C), second.reshape(N, R + PAD, C), coefs)
    return first, second, coef_one.T, coef_two.T


def solution(mesh):
    spec = P(None, "gx", "gy")
    return jax.shard_map(
        functools.partial(local, mesh.shape["gx"], mesh.shape["gy"]),
        mesh=mesh,
        in_specs=(spec, spec, spec),
        out_specs=(spec, spec, P(), P()),
        check_vma=False,
    )
```

```python
import functools

import jax
import jax.numpy as jnp
from jax import lax
from jax.experimental import pallas as pl
from jax.experimental.pallas import tpu as pltpu
from jax.sharding import PartitionSpec as P

HIGH = lax.Precision.HIGHEST
MESH = pl.DeviceIdType.MESH
F32 = jnp.float32
BF = jnp.bfloat16
LANES = 128
CHUNKS = 4
DIRECT = 64
BUDDY = 2
PAD = 8


def dot_nn(a, b):
    return jnp.dot(a, b, precision=HIGH, preferred_element_type=F32)


def dot_nt(a, b, precision=HIGH):
    return lax.dot_general(
        a, b, (((1,), (1,)), ((), ())), precision=precision, preferred_element_type=F32
    )


def rows_full(v, at=0):
    parts = [v, jnp.zeros((LANES - at - v.shape[0], LANES), F32)]
    if at:
        parts.insert(0, jnp.zeros((at, LANES), F32))
    return jnp.concatenate(parts, axis=0)


def split(v):
    hi = v.astype(BF).astype(F32)
    return hi, v - hi


def split_rows(v):
    return jnp.concatenate(split(v), axis=0).astype(BF)


def eliminate(a, g0, n):
    sub = lax.broadcasted_iota(jnp.int32, a.shape, 0)
    cols = [jnp.broadcast_to(a[:, g0 + j : g0 + j + 1], a.shape) for j in range(n)]
    pivots = jnp.ones(a.shape, F32)
    for k in range(n):
        pivot = jnp.broadcast_to(cols[k][k : k + 1, :], a.shape)
        pivots = jnp.where(sub == k, pivot, pivots)
        if k == n - 1:
            break
        factor = jnp.where(sub > k, cols[k] * (1.0 / pivot), 0.0)
        for j in range(k + 1, n):
            cols[j] = cols[j] - factor * cols[j][k : k + 1, :]
        a = a - factor * a[k : k + 1, :]
    return a * (1.0 / jnp.sqrt(pivots))


def kernel(
    nx, ny, K, N, R,
    basis_hbm, panel_hbm, rate_hbm,
    first_v, second_v, coefs,
    basis_v, panel_v, rate_v, rates, fext, wf, x_v, m_v, t_v, g_v,
    edge_send, edge_recv, eb_send, eb_recv, ew_send, ew_recv, ms_buf, my_buf, mx_buf, mz_buf, py_buf, px_buf,
    in_sem, edge_ssem, edge_rsem, eb_ssem, eb_rsem, ew_ssem, ew_rsem, ready,
    m_s, py_s, px_s,
):
    ix, iy = lax.axis_index("gx"), lax.axis_index("gy")
    sites = R * LANES
    scale = 1.0 / (sites * nx * ny)
    lane = lax.broadcasted_iota(jnp.int32, (N, LANES), 1)
    sub = lax.broadcasted_iota(jnp.int32, (N, LANES), 0)
    KN = K + N
    Z = K + 2 * N
    HI = 2 * N
    LO = HI + Z
    EXT = sites
    EDGE = sites + LANES
    RP = R + PAD
    T = R + 16

    basis_rows = basis_v.reshape(K * RP, LANES)
    panel_rows = panel_v.reshape(N * RP, LANES)

    axes = (("gx", ix, nx), ("gy", iy, ny))
    everyone = ("all", ix * ny + iy, nx * ny)
    direct = nx * ny <= DIRECT and nx % BUDDY == 0

    def peer_of(axis, me, n, d):
        other = lax.rem(me + d, n)
        if axis == "all":
            return other, {"gx": lax.div(other, ny), "gy": lax.rem(other, ny)}
        return other, {axis: other}

    with jax.named_scope("dma0"):
        step = K // CHUNKS
        panel_in = pltpu.make_async_copy(panel_hbm, panel_v.at[:, pl.ds(0, R)], in_sem.at[0])
        rate_in = pltpu.make_async_copy(rate_hbm, rate_v, in_sem.at[1])
        panel_in.start()
        rate_in.start()

    barrier = pltpu.get_barrier_semaphore()

    def greet(device):
        pl.semaphore_signal(barrier, inc=1, device_id=device, device_id_type=MESH)

    if direct:
        planes = nx // BUDDY
        plane = lax.div(ix, BUDDY)
        home = plane * BUDDY
        group = BUDDY * ny
        seat = (ix - home) * ny + iy
        mates = []
        for d in range(1, group):
            other = lax.rem(seat + d, group)
            mates.append({"gx": home + lax.div(other, ny), "gy": lax.rem(other, ny)})
        outer = [
            ((ix == home) & (ix > 0), ix - 1),
            ((ix == home + BUDDY - 1) & (ix < nx - 1), ix + 1),
        ]
        far_first = []
        for c in sorted(range(planes), key=lambda c: ((planes - 1 - c) % 2, -c)):
            other = lax.rem(planes + c - plane, planes)
            for k in range(group):
                to = lax.rem(seat + k + group // 2, group)
                far_first.append(
                    (
                        None if planes % 2 == 0 and c % 2 == 1 else other != plane,
                        {"gx": other * BUDDY + lax.div(to, ny), "gy": lax.rem(to, ny)},
                    )
                )
        far_first += [(None, device) for device in mates]
        row_mates = [{"gy": lax.rem(iy + d, ny)} for d in range(1, ny)]
        column_mates = [{"gx": home + lax.rem(ix - home + d, BUDDY)} for d in range(1, BUDDY)]
        greeted = ny - 1 + BUDDY - 1 + BUDDY * plane
        for there, device in outer:
            greeted = greeted + jnp.where(there, 1, 0)

            @pl.when(there)
            def _(device=device):
                greet({"gx": device})

        for device in column_mates + row_mates:
            greet(device)
        for d in range(1, planes):
            @pl.when(plane + d < planes)
            def _(d=d):
                for b in range(BUDDY):
                    greet({"gx": home + d * BUDDY + b})

    else:
        greeted = 0
        for axis, me, n in axes:
            for d in range(1, n):
                greet(peer_of(axis, me, n, d)[1])
                greeted += 1

    basis_in = []
    for c in range(CHUNKS):
        part = pl.ds(c * step, step)
        basis_in.append(
            pltpu.make_async_copy(
                basis_hbm.at[part], basis_v.at[part, pl.ds(0, R)], in_sem.at[2 + c]
            )
        )
        basis_in[-1].start()
    def row_at(r):
        return pl.ds(r * LANES, LANES)

    def rate_row(d, r):
        return rates[pl.ds(d * T + 8 + r, 1), :]

    with jax.named_scope("inwait"):
        panel_in.wait()
        rate_in.wait()
    for d in range(4):
        rates[d * T : d * T + 8, :] = jnp.ones((8, LANES), F32)
        rates[d * T + 8 + R : (d + 1) * T, :] = jnp.ones((8, LANES), F32)
        rates[d * T + 8 : d * T + 8 + R, :] = (
            rate_v[d * R : (d + 1) * R, :].astype(F32) * 0.125
        )
    rates[4 * T + 8 : 4 * T + 8 + R, :] = (
        rates[8 : 8 + R, :]
        + rates[T + 8 : T + 8 + R, :]
        + rates[2 * T + 8 : 2 * T + 8 + R, :]
        + rates[3 * T + 8 : 3 * T + 8 + R, :]
    )

    routes = (
        ("gx", ix - 1, ix > 0, ix < nx - 1),
        ("gx", ix + 1, ix < nx - 1, ix > 0),
        ("gy", iy - 1, iy > 0, iy < ny - 1),
        ("gy", iy + 1, iy < ny - 1, iy > 0),
    )

    def edges(send, recv, ssem, rsem):
        def copy(e):
            return pltpu.make_async_remote_copy(
                src_ref=send.at[min(e, 2)],
                dst_ref=recv.at[e],
                send_sem=ssem.at[e],
                recv_sem=rsem.at[e],
                device_id={routes[e][0]: routes[e][1]},
                device_id_type=MESH,
            )

        def start():
            for e in range(4):
                @pl.when(routes[e][2])
                def _(e=e):
                    copy(e).start()

                @pl.when(jnp.logical_not(routes[e][3]))
                def _(e=e):
                    recv[e] = jnp.zeros(recv.shape[1:], F32)

        def wait():
            for e in range(4):
                @pl.when(routes[e][3])
                def _(e=e):
                    copy(e).wait_recv()

        def drain():
            for e in range(4):
                @pl.when(routes[e][2])
                def _(e=e):
                    copy(e).wait_send()

        return start, wait, drain

    def share(buf, sem, axis, me, n, source=None):
        def copy(src, dst, device):
            return pltpu.make_async_remote_copy(
                src_ref=src,
                dst_ref=dst,
                send_sem=sem.at[0],
                recv_sem=sem.at[1],
                device_id=device,
                device_id_type=MESH,
            )

        def start(store):
            store(buf.at[me])
            if axis == "all":
                for there, device in far_first:
                    if there is None:
                        copy(buf.at[me], buf.at[me], device).start()
                    else:
                        @pl.when(there)
                        def _(device=device):
                            copy(buf.at[me], buf.at[me], device).start()
                return
            for d in range(1, n):
                other, device = peer_of(axis, me, n, d)
                copy(buf.at[me] if source is None else source.at[other], buf.at[me], device).start()

        rest = buf.at[pl.ds(0, n - 1)]
        whole = copy(rest, rest, peer_of(axis, me, n, 1)[1])

        def wait():
            whole.wait_recv()

        def finish():
            wait()
            parts = [buf[k] for k in range(n)]
            while len(parts) > 1:
                parts = [
                    parts[i] + parts[i + 1] if i + 1 < len(parts) else parts[i]
                    for i in range(0, len(parts), 2)
                ]
            return parts[0]

        def drain():
            whole.wait_send()

        return start, finish, drain, wait

    half = N // 2

    def pack(v):
        turned = pltpu.roll(v, K, 1)
        tail = pltpu.roll(v, 0, 1, stride=2 * N, stride_axis=0)
        mine = lax.div(lane, 2 * N) == lax.rem(sub + K // (2 * N), N)
        tail = jnp.sum(jnp.where(mine, tail, 0.0), axis=0, keepdims=True)
        low = lax.broadcasted_iota(jnp.int32, (half, LANES), 1) < K
        return jnp.where(low, v[0:half], turned[half:N]), tail

    def unpack(t):
        body = jnp.concatenate([t[0:half], pltpu.roll(t[0:half], K, 1)], axis=0)
        spread = jnp.broadcast_to(t[half : half + 1], (N, LANES))
        tail = spread
        for j in range(1, N):
            tail = jnp.where(sub == j, pltpu.roll(spread, LANES - 2 * N * j, 1), tail)
        return jnp.where(lane < K, body, jnp.where(lane < Z, tail, 0.0))

    drains = []

    def reduction(s, value):
        xgroup = everyone if direct else axes[0]
        xstart, xfinish, xdrain, _ = share(px_buf.at[s], px_s.at[s], *xgroup)
        drains.append(xdrain)

        def put(parts):
            def store(ref):
                ref[0:half] = parts[0]
                ref[half : half + 1] = parts[1]

            return store

        parts = pack(value)
        if direct:
            xstart(put(parts))
            return lambda: unpack(xfinish())
        ystart, yfinish, ydrain, _ = share(py_buf.at[s], py_s.at[s], *axes[1])
        drains.append(ydrain)
        ystart(put(parts))

        def finish():
            t = yfinish()
            xstart(put((t[0:half], t[half : half + 1])))
            return unpack(xfinish())

        return finish

    e0_start, e0_wait, e0_drain = edges(edge_send, edge_recv, edge_ssem, edge_rsem)
    e1_start, e1_wait, e1_drain = edges(eb_send, eb_recv, eb_ssem, eb_rsem)
    e2_start, e2_wait, e2_drain = edges(ew_send, ew_recv, ew_ssem, ew_rsem)
    drains += [e0_drain, e1_drain, e2_drain]

    def slots(shape, r):
        at = lax.broadcasted_iota(jnp.int32, shape, len(shape) - 1)
        return (at == 2 * r) | (at == (2 * r - 1) % LANES)

    def tuck(packed, r, f):
        return jnp.where(slots(f.shape, r), pltpu.roll(f, 2 * r, len(f.shape) - 1), packed)

    with jax.named_scope("packp"):
        lane_of = lax.broadcasted_iota(jnp.int32, (R, LANES), 1)
        sides = jnp.where(lane_of == 0, rates[2 * T + 8 : 2 * T + 8 + R, :], rates[3 * T + 8 : 3 * T + 8 + R, :])
        rate_side = jnp.zeros((N, LANES), F32)
        for i in range(R // 8):
            turned = pltpu.roll(sides[i * 8 : i * 8 + 8], 16 * i, 1, stride=2, stride_axis=0)
            mine = (lane == 2 * (sub + 8 * i)) | (lane == lax.rem(2 * (sub + 8 * i) + LANES - 1, LANES))
            rate_side = rate_side + jnp.where(mine, turned, 0.0)
        rate_side = jnp.sum(rate_side, axis=0, keepdims=True)
        packed = jnp.zeros((N, LANES), F32)
        for r in range(R):
            f = panel_rows[pl.ds(r, N, stride=RP), :]
            fext[:, row_at(r + 1)] = f
            packed = tuck(packed, r, f)
            if r == 0:
                edge_send[0] = f * rate_row(0, 0)
            if r == R - 1:
                edge_send[1] = f * rate_row(1, R - 1)
        edge_send[2] = packed * rate_side

    with jax.named_scope("barrier"):
        pl.semaphore_wait(barrier, greeted)
    e0_start()

    if direct:
        for device in row_mates:
            pl.semaphore_signal(ready.at[0], inc=1, device_id=device, device_id_type=MESH)
        for d in range(1, planes):
            @pl.when(plane >= d)
            def _(d=d):
                for b in range(BUDDY):
                    device = {"gx": home - d * BUDDY + b}
                    pl.semaphore_signal(ready.at[1], inc=1, device_id=device, device_id_type=MESH)

    def all_arrived():
        pl.semaphore_wait(ready.at[0], ny - 1)

        @pl.when(plane < planes - 1)
        def _():
            pl.semaphore_wait(ready.at[1], BUDDY * (planes - 1 - plane))

    with jax.named_scope("split"):
        for c in range(CHUNKS):
            basis_in[c].wait()
            mine = slice(c * step, (c + 1) * step)
            above = slice(HI + c * step, HI + (c + 1) * step)
            below = slice(LO + c * step, LO + (c + 1) * step)

            packed = jnp.zeros((step, LANES), F32)
            for r in range(R):
                b = basis_rows[pl.ds(c * step * RP + r, step, stride=RP), :]
                hi = b.astype(BF)
                x_v[above, row_at(r)] = hi
                x_v[below, row_at(r)] = (b - hi.astype(F32)).astype(BF)
                packed = tuck(packed, r, b)
            hi = packed.astype(BF)
            x_v[above, pl.ds(EXT, LANES)] = hi
            x_v[below, pl.ds(EXT, LANES)] = (packed - hi.astype(F32)).astype(BF)
            eb_send[2, mine] = packed * rate_side
            eb_send[0, mine] = basis_rows[pl.ds(c * step * RP, step, stride=RP), :] * rate_row(0, 0)
            eb_send[1, mine] = (
                basis_rows[pl.ds(c * step * RP + R - 1, step, stride=RP), :] * rate_row(1, R - 1)
            )

    e1_start()

    def sides(from_right, from_left):
        side = jnp.where(lax.rem(lane, 2) == 1, from_left, pltpu.roll(from_right, LANES - 2, 1))
        return lambda r: pltpu.roll(side, (LANES + 1 - 2 * r) % LANES, 1)

    def stencil(beside, finish):
        for r in range(R):
            f = fext[:, row_at(r + 1)]
            above = fext[:, row_at(r)] * rate_row(1, r - 1)
            below = fext[:, row_at(r + 2)] * rate_row(0, r + 1)
            west = pltpu.roll(f * rate_row(3, r), 1, 1)
            east = pltpu.roll(f * rate_row(2, r), LANES - 1, 1)
            other = beside(r)
            west = jnp.where(lane == 0, other, west)
            east = jnp.where(lane == LANES - 1, other, east)
            finish(r, f, above + below + west + east - rate_row(4, r) * f)

    def put_pair(at, upper, lower):
        both = jnp.concatenate([upper, lower], axis=0)
        hi = both.astype(BF)
        low = both - hi.astype(F32)
        x_v[HI + K : LO, at] = hi
        x_v[LO + K : LO + Z, at] = low.astype(BF)
        return hi.astype(F32), low

    def put_rhs(at, hi, low):
        x_v[0:HI, at] = jnp.concatenate([hi, low], axis=0).astype(BF)

    def against(at, width):
        return [
            dot_nt(x_v[top : top + Z, at], x_v[0:width, at], lax.Precision.DEFAULT)
            for top in (HI, LO)
        ]

    def halves(width):
        parts = [against(pl.ds(h * (sites // 2), sites // 2), width) for h in range(2)]
        return [parts[0][i] * scale + parts[1][i] * scale for i in range(2)]

    def turned(total):
        t_v[0:Z, 0:HI] = total
        value = t_v[...].T
        return value[0:N] + value[N:HI]

    mid = K // 2
    part = mid // ny
    m1_start, m1_finish, m1_drain, _ = share(my_buf, m_s.at[0], *axes[1], source=ms_buf)
    m2_start, m2_finish, m2_drain, _ = share(mx_buf, m_s.at[1], *axes[0])
    m3_start, _, m3_drain, m3_wait = share(mz_buf, m_s.at[2], *axes[1])
    drains += [m1_drain, m2_drain, m3_drain]

    zero = jnp.zeros((N, LANES), F32)
    with jax.named_scope("sten0"):
        t_v[...] = jnp.zeros_like(t_v)
        fext[:, 0:LANES] = zero
        fext[:, (R + 1) * LANES : (R + 2) * LANES] = zero
        columns = [zero]

        def finish_first(r, f, w):
            wf[:, row_at(r)] = w
            hi, low = put_pair(row_at(r), w, zero)
            put_rhs(row_at(r), hi[0:N], low[0:N])

        stencil(lambda r: 0.0, finish_first)
    with jax.named_scope("tuck0"):
        for r in range(R):
            columns[0] = tuck(columns[0], r, wf[:, row_at(r)])
    with jax.named_scope("gram"):
        high, low = halves(HI + K)
        first = (high + low)[:, 0:HI]
        g_v[...] = jnp.zeros_like(g_v)
        g_v[0, 0:K, 0 : HI + K] = (high + low)[0:K]
        g_v[1, 0:K, 0 : HI + K] = low[0:K]
        straight = g_v[0]
        flipped = g_v[1].T[HI : HI + K]
        is_low = lax.broadcasted_iota(jnp.int32, (mid, LANES), 1) < K
        full = jnp.where(
            is_low,
            pltpu.roll(straight[0:mid], LANES - HI, 1) + flipped[0:mid],
            pltpu.roll(straight[mid:K], K - HI, 1) + pltpu.roll(flipped[mid:K], K, 1),
        )
        for p in range(ny):
            ms_buf[p] = full[p * part : (p + 1) * part]

        def put_own(ref):
            ref[...] = ms_buf[iy]

        m1_start(put_own)

    with jax.named_scope("ewait0"):
        e0_wait()
    with jax.named_scope("lat0"):
        from_below, from_above, from_right, from_left = [edge_recv[e] for e in range(4)]
        gain = jnp.where(
            lax.rem(lane, 2) == 0, pltpu.roll(from_left, 1, 1), pltpu.roll(from_right, LANES - 1, 1)
        )
        column = columns[0]
        column = jnp.where(slots(zero.shape, 0), column + from_above, column)
        column = jnp.where(
            slots(zero.shape, R - 1), column + pltpu.roll(from_below, 2 * (R - 1), 1), column
        )
        ends = ((0, from_above), (R - 1, from_below))
        for r, extra in ends:
            w = wf[:, row_at(r)]
            put_pair(row_at(r), zero, w + 0.5 * extra)
            put_rhs(row_at(r), *split(extra))
            wf[:, row_at(r)] = w + extra
        put_pair(pl.ds(EXT, LANES), zero, column + 0.5 * gain)
        put_rhs(pl.ds(EXT, LANES), *split(gain))
        last = against(pl.ds(sites - LANES, 2 * LANES), HI)
        top = against(row_at(0), HI)
        value = turned(first + ((last[0] + last[1]) + (top[0] + top[1])) * scale)
        if direct:
            all_arrived()
        finish0 = reduction(0, value)
    with jax.named_scope("packw"):
        beside = sides(from_right, from_left)
        outer = (lane == 0) | (lane == LANES - 1)
        for r in range(R):
            wf[:, row_at(r)] = wf[:, row_at(r)] + jnp.where(outer, beside(r), 0.0)
        ew_send[0] = wf[:, row_at(0)] * rate_row(0, 0)
        ew_send[1] = wf[:, row_at(R - 1)] * rate_row(1, R - 1)
        ew_send[2] = (column + gain) * rate_side
    e2_start()

    with jax.named_scope("ewait1"):
        e1_wait()
    with jax.named_scope("esplit"):
        for e in range(4):
            at = pl.ds(EDGE + e * LANES, LANES)
            b = eb_recv[e]
            hi = b.astype(BF)
            x_v[HI : HI + K, at] = hi
            x_v[LO : LO + K, at] = (b - hi.astype(F32)).astype(BF)

    def forward(ref, value):
        ref[...] = value

    with jax.named_scope("m12"):
        m = m1_finish()
        m2_start(lambda ref: forward(ref, m))
    with jax.named_scope("ewait2"):
        e2_wait()
        for e in range(4):
            wf[:, pl.ds(EDGE + e * LANES, LANES)] = ew_recv[e]
    with jax.named_scope("red0"):
        total = finish0()

    def combine(lhs, at):
        both = jnp.dot(lhs, x_v[HI:LO, at], preferred_element_type=F32) + jnp.dot(
            lhs, x_v[LO : LO + Z, at], preferred_element_type=F32
        )
        return both[0:N] + both[N : 2 * N]

    wide8 = 8 * LANES
    pm = jnp.where(lane < K, total, 0.0)
    def project(lhs, at):
        both = jnp.dot(lhs, x_v[HI : HI + K, at], preferred_element_type=F32) + jnp.dot(
            lhs, x_v[LO : LO + K, at], preferred_element_type=F32
        )
        return both[0:N] + both[N : 2 * N]

    with jax.named_scope("new0"):
        lhs = split_rows(pm)[:, 0:K]
        at = pl.ds(EDGE, 4 * LANES)
        edge = wf[:, at] - project(lhs, at)
        fext[:, 0:LANES] = edge[:, LANES : 2 * LANES]
        fext[:, (R + 1) * LANES : (R + 2) * LANES] = edge[:, 0:LANES]
        for i in range(R // 8):
            at = pl.ds(i * wide8, wide8)
            fext[:, pl.ds(LANES + i * wide8, wide8)] = wf[:, at] - project(lhs, at)
    with jax.named_scope("lat1"):
        def finish_second(r, f, u):
            hi, low = put_pair(row_at(r), f, u)
            put_rhs(row_at(r), hi[N:HI], low[N:HI])

        with jax.named_scope("sten1"):
            stencil(
                sides(edge[:, 2 * LANES : 3 * LANES], edge[:, 3 * LANES : 4 * LANES]), finish_second
            )
        with jax.named_scope("prod1"):
            high, low = halves(HI)
            value = turned(high + low)
        m_own = m2_finish()
        m3_start(lambda ref: forward(ref, m_own))
        finish1 = reduction(1, value)

    with jax.named_scope("mxfin"):
        m3_wait()
        m = jnp.concatenate([mz_buf[p] for p in range(ny)], axis=0)
        gram = rows_full(
            jnp.concatenate(
                [
                    jnp.where(lax.broadcasted_iota(jnp.int32, (mid, LANES), 1) < K, m, 0.0),
                    jnp.where(
                        lax.broadcasted_iota(jnp.int32, (mid, LANES), 1) < K,
                        pltpu.roll(m, LANES - K, 1),
                        0.0,
                    ),
                ],
                axis=0,
            )
        )
    G0 = Z

    def times(parts, stacked):
        pair = jnp.concatenate(parts, axis=0).astype(BF)
        both = jnp.dot(
            jnp.concatenate([pair, pair], axis=1), stacked, preferred_element_type=F32
        )
        return both[0:N] + both[N : 2 * N]

    def gram_of(value, parts):
        both = sum(
            dot_nt(split_rows(value), rows_full(p, G0).astype(BF), lax.Precision.DEFAULT)
            for p in parts
        )
        return both[0:N] + both[N : 2 * N]

    with jax.named_scope("fac0"):
        own = (
            pltpu.roll(total, G0 - K, 1)
            + pltpu.roll(total, G0 - KN, 1)
            + pltpu.roll(rows_full(total).T[KN:Z], G0, 1)
        )
        pm_parts = split(pm)
        rest = 2.0 * pm - times(pm_parts, jnp.concatenate(split(gram), axis=0).astype(BF))
        g = own - gram_of(rest, pm_parts)
        g = jnp.where((lane >= G0) & (lane < G0 + N), g, 0.0)
        a = jnp.where(lane < K, rest - pm, jnp.where(lane == sub + K, 1.0, g))
        a = eliminate(a, G0, N)
        at_t = rows_full(a).T
        inv = pltpu.roll(a, LANES - K, 1)
        inv = jnp.where(lane < N, inv, 0.0)
        low1 = at_t[G0 : G0 + N]
        coefs[0] = pm + jnp.where((lane >= K) & (lane < KN), pltpu.roll(low1, K, 1), 0.0)
        row = lax.broadcasted_iota(jnp.int32, (LANES, LANES), 0)
        col = lax.broadcasted_iota(jnp.int32, (LANES, LANES), 1)
        inner = jnp.where((row < KN), at_t, 0.0)
        flow = dot_nn(inner, rows_full(jnp.where(lane < KN, a, 0.0)))
        in_b = (row < K) & (col < K)
        in_w = (row >= K) & (row < KN) & (col >= K) & (col < KN)
        eye = jnp.where(row == col, 1.0, 0.0)
        kmat = jnp.where(in_b, 2.0 * eye - gram, jnp.where(in_w, flow, -flow))
        dmat = jnp.where(in_b, eye, jnp.where(in_w, flow, 0.0))
        tmat = jnp.where((row >= K) & (row < KN) & (col < N), at_t, 0.0)
        for i, mat in enumerate((kmat, dmat, tmat)):
            hi, low = split(mat)
            m_v[0:LANES, i * LANES : (i + 1) * LANES] = hi.astype(BF)
            m_v[LANES : 2 * LANES, i * LANES : (i + 1) * LANES] = low.astype(BF)
    with jax.named_scope("q1"):
        lhs = split_rows(inv)[:, 0 : 2 * N]
        for i in range(R // 8):
            at = pl.ds(i * wide8, wide8)
            both = jnp.dot(lhs, x_v[HI + K : LO, at], preferred_element_type=F32) + jnp.dot(
                lhs, x_v[LO + K : LO + Z, at], preferred_element_type=F32
            )
            q = both[0:N] + both[N : 2 * N]
            for u in range(8):
                first_v[pl.ds(i * 8 + u, N, stride=RP), :] = q[:, u * LANES : (u + 1) * LANES]

    with jax.named_scope("red1"):
        total = finish1()
    with jax.named_scope("fac1"):
        ep = jnp.where(lane < KN, total, 0.0)
        own = pltpu.roll(total, G0 - KN, 1)
        ep_parts = split(ep)
        both = times(ep_parts, m_v[:, 0 : 2 * LANES])
        ek, ed = both[:, 0:LANES], both[:, LANES : 2 * LANES]
        g = own - gram_of(ek, ep_parts)
        g = jnp.where((lane >= G0) & (lane < G0 + N), g, 0.0)
        a = jnp.where(lane < KN, ed, jnp.where(lane == sub + KN, 1.0, g))
        a = eliminate(a, G0, N)
        lhs = split_rows(jnp.where(lane < KN, -a, a))[:, 0:Z]
    with jax.named_scope("coef1"):
        low2 = rows_full(a).T[G0 : G0 + N]
        es = times(ep_parts, m_v[:, 2 * LANES : 3 * LANES])
        stack = jnp.where(lane < K, ep, jnp.where(lane < KN, pltpu.roll(es, K, 1), 0.0))
        stack = jnp.where((lane >= KN) & (lane < Z), pltpu.roll(low2, KN, 1), stack)
        coefs[1] = dot_nn(inv, rows_full(stack))
    with jax.named_scope("new1"):
        for i in range(R // 8):
            q = combine(lhs, pl.ds(i * wide8, wide8))
            for u in range(8):
                second_v[pl.ds(i * 8 + u, N, stride=RP), :] = q[:, u * LANES : (u + 1) * LANES]
    with jax.named_scope("drain"):
        for drain in drains:
            drain()


def deliver(
    R, first_v, second_v, coefs, first_hbm, second_hbm, one_hbm, two_hbm, coef_one, coef_two, sem
):
    copies = [
        pltpu.make_async_copy(first_v.at[:, pl.ds(0, R)], first_hbm, sem.at[0]),
        pltpu.make_async_copy(second_v.at[:, pl.ds(0, R)], second_hbm, sem.at[1]),
        pltpu.make_async_copy(coef_one, one_hbm, sem.at[2]),
        pltpu.make_async_copy(coef_two, two_hbm, sem.at[3]),
    ]
    for copy in copies[:2]:
        copy.start()
    coef_one[...] = coefs[0, :, 0 : coef_one.shape[1]]
    coef_two[...] = coefs[1, :, 0 : coef_two.shape[1]]
    for copy in copies[2:]:
        copy.start()
    for copy in copies:
        copy.wait()


def local(nx, ny, basis, panel, rate_codes):
    N, R, C = panel.shape
    K = basis.shape[0]
    assert C == LANES and 2 * K == LANES and N == 8
    vmem = pl.BlockSpec(memory_space=pltpu.VMEM)
    hbm = pl.BlockSpec(memory_space=pl.ANY)
    dma = pltpu.SemaphoreType.DMA
    sites = R * LANES
    group = nx * ny if nx * ny <= DIRECT else nx
    Z = K + 2 * N
    first, second, coefs = pl.pallas_call(
        functools.partial(kernel, nx, ny, K, N, R),
        out_shape=(
            pltpu.VMEM((N * (R + PAD), C), F32),
            pltpu.VMEM((N * (R + PAD), C), F32),
            pltpu.VMEM((2, N, C), F32),
        ),
        in_specs=[pl.BlockSpec(memory_space=pltpu.HBM)] * 3,
        out_specs=(vmem, vmem, vmem),
        scratch_shapes=[
            pltpu.VMEM((K, R + PAD, LANES), F32),
            pltpu.VMEM((N, R + PAD, LANES), F32),
            pltpu.VMEM((4 * R, LANES), jnp.int32),
            pltpu.VMEM((5 * (R + 16), LANES), F32),
            pltpu.VMEM((N, (R + 2) * LANES), F32),
            pltpu.VMEM((N, sites + 5 * LANES), F32),
            pltpu.VMEM((2 * N + 2 * Z, sites + 5 * LANES), BF),
            pltpu.VMEM((2 * LANES, 3 * LANES), BF),
            pltpu.VMEM((LANES, LANES), F32),
            pltpu.VMEM((2, LANES, LANES), F32),
            pltpu.VMEM((3, N, LANES), F32),
            pltpu.VMEM((4, N, LANES), F32),
            pltpu.VMEM((3, K, LANES), F32),
            pltpu.VMEM((4, K, LANES), F32),
            pltpu.VMEM((3, N, LANES), F32),
            pltpu.VMEM((4, N, LANES), F32),
            pltpu.VMEM((ny, K // 2 // ny, LANES), F32),
            pltpu.VMEM((ny, K // 2 // ny, LANES), F32),
            pltpu.VMEM((nx, K // 2 // ny, LANES), F32),
            pltpu.VMEM((ny, K // 2 // ny, LANES), F32),
            pltpu.VMEM((2, ny, N // 2 + 1, LANES), F32),
            pltpu.VMEM((2, group, N // 2 + 1, LANES), F32),
            dma((2 + CHUNKS,)),
            dma((4,)),
            dma((4,)),
            dma((4,)),
            dma((4,)),
            dma((4,)),
            dma((4,)),
            pltpu.SemaphoreType.REGULAR((2,)),
            dma((3, 2)),
            dma((2, 2)),
            dma((2, 2)),
        ],
        compiler_params=pltpu.CompilerParams(
            collective_id=0, has_side_effects=True
        ),
    )(basis, panel, rate_codes.reshape(rate_codes.shape[0] * R, C))
    first, second, coef_one, coef_two = pl.pallas_call(
        functools.partial(deliver, R),
        out_shape=(
            jax.ShapeDtypeStruct((N, R, C), F32),
            jax.ShapeDtypeStruct((N, R, C), F32),
            jax.ShapeDtypeStruct((N, K + N), F32),
            jax.ShapeDtypeStruct((N, K + 2 * N), F32),
        ),
        in_specs=[vmem] * 3,
        out_specs=(hbm, hbm, hbm, hbm),
        scratch_shapes=[
            pltpu.VMEM((N, K + N), F32),
            pltpu.VMEM((N, K + 2 * N), F32),
            dma((4,)),
        ],
        compiler_params=pltpu.CompilerParams(vmem_limit_bytes=4 * 2**20),
    )(first.reshape(N, R + PAD, C), second.reshape(N, R + PAD, C), coefs)
    return first, second, coef_one.T, coef_two.T


def solution(mesh):
    spec = P(None, "gx", "gy")
    return jax.shard_map(
        functools.partial(local, mesh.shape["gx"], mesh.shape["gy"]),
        mesh=mesh,
        in_specs=(spec, spec, spec),
        out_specs=(spec, spec, P(), P()),
        check_vma=False,
    )
```

```python
import functools

import jax
import jax.numpy as jnp
from jax import lax
from jax.experimental import pallas as pl
from jax.experimental.pallas import tpu as pltpu
from jax.sharding import PartitionSpec as P

HIGH = lax.Precision.HIGHEST
MESH = pl.DeviceIdType.MESH
F32 = jnp.float32
BF = jnp.bfloat16
LANES = 128
CHUNKS = 2
DIRECT = 64
BUDDY = 2
PAD = 8


def dot_nn(a, b):
    return jnp.dot(a, b, precision=HIGH, preferred_element_type=F32)


def dot_nt(a, b, precision=HIGH):
    return lax.dot_general(
        a, b, (((1,), (1,)), ((), ())), precision=precision, preferred_element_type=F32
    )


def rows_full(v, at=0):
    parts = [v, jnp.zeros((LANES - at - v.shape[0], LANES), F32)]
    if at:
        parts.insert(0, jnp.zeros((at, LANES), F32))
    return jnp.concatenate(parts, axis=0)


def split(v):
    hi = v.astype(BF).astype(F32)
    return hi, v - hi


def split_rows(v):
    return jnp.concatenate(split(v), axis=0).astype(BF)


def eliminate(a, g0, n):
    sub = lax.broadcasted_iota(jnp.int32, a.shape, 0)
    cols = [jnp.broadcast_to(a[:, g0 + j : g0 + j + 1], a.shape) for j in range(n)]
    pivots = jnp.ones(a.shape, F32)
    for k in range(n):
        pivot = jnp.broadcast_to(cols[k][k : k + 1, :], a.shape)
        pivots = jnp.where(sub == k, pivot, pivots)
        if k == n - 1:
            break
        factor = jnp.where(sub > k, cols[k] * (1.0 / pivot), 0.0)
        for j in range(k + 1, n):
            cols[j] = cols[j] - factor * cols[j][k : k + 1, :]
        a = a - factor * a[k : k + 1, :]
    return a * (1.0 / jnp.sqrt(pivots))


def kernel(
    nx, ny, K, N, R,
    basis_hbm, panel_hbm, rate_hbm,
    first_v, second_v, coefs,
    basis_v, panel_v, rate_v, rates, fext, wf, x_v, m_v, t_v, g_v,
    edge_send, edge_recv, eb_send, eb_recv, ew_send, ew_recv, ms_buf, mm_buf, py_buf, px_buf,
    in_sem, edge_ssem, edge_rsem, eb_ssem, eb_rsem, ew_rsem, ready,
    m_s, py_s, px_s,
):
    ix, iy = lax.axis_index("gx"), lax.axis_index("gy")
    sites = R * LANES
    scale = 1.0 / (sites * nx * ny)
    lane = lax.broadcasted_iota(jnp.int32, (N, LANES), 1)
    sub = lax.broadcasted_iota(jnp.int32, (N, LANES), 0)
    KN = K + N
    Z = K + 2 * N
    HI = 2 * N
    LO = HI + Z
    EXT = sites
    EDGE = sites + LANES
    RP = R + PAD
    T = R + 16

    basis_rows = basis_v.reshape(K * RP, LANES)
    panel_rows = panel_v.reshape(N * RP, LANES)

    axes = (("gx", ix, nx), ("gy", iy, ny))
    everyone = ("all", ix * ny + iy, nx * ny)
    direct = nx * ny <= DIRECT and nx % BUDDY == 0

    def peer_of(axis, me, n, d):
        other = lax.rem(me + d, n)
        if axis == "all":
            return other, {"gx": lax.div(other, ny), "gy": lax.rem(other, ny)}
        return other, {axis: other}

    with jax.named_scope("dma0"):
        step = K // CHUNKS
        panel_in = pltpu.make_async_copy(panel_hbm, panel_v.at[:, pl.ds(0, R)], in_sem.at[0])
        rate_in = pltpu.make_async_copy(rate_hbm, rate_v, in_sem.at[1])
        panel_in.start()
        rate_in.start()

    barrier = pltpu.get_barrier_semaphore()

    def greet(device):
        pl.semaphore_signal(barrier, inc=1, device_id=device, device_id_type=MESH)

    if direct:
        planes = nx // BUDDY
        plane = lax.div(ix, BUDDY)
        home = plane * BUDDY
        group = BUDDY * ny
        seat = (ix - home) * ny + iy
        mates = []
        for d in range(1, group):
            other = lax.rem(seat + d, group)
            mates.append({"gx": home + lax.div(other, ny), "gy": lax.rem(other, ny)})
        outer = [
            ((ix == home) & (ix > 0), ix - 1),
            ((ix == home + BUDDY - 1) & (ix < nx - 1), ix + 1),
        ]
        if planes % 2:
            others = [lax.rem(plane + d, planes) for d in range(1, planes)]
        else:
            others = [lax.rem(planes + c - plane, planes) for c in range(planes - 1, 0, -2)]
            others += [lax.rem(plane + d, planes) for d in range(2, planes, 2)]
        far_first = []
        for other in others:
            for k in range(group):
                to = lax.rem(seat + k + group // 2, group)
                far_first.append({"gx": other * BUDDY + lax.div(to, ny), "gy": lax.rem(to, ny)})
        far_first += mates
        row_mates = [{"gy": lax.rem(iy + d, ny)} for d in range(1, ny)]
        column_mates = [{"gx": home + lax.rem(ix - home + d, BUDDY)} for d in range(1, BUDDY)]
        greeted = ny - 1 + BUDDY - 1 + BUDDY * plane
        for there, device in outer:
            greeted = greeted + jnp.where(there, 1, 0)

            @pl.when(there)
            def _(device=device):
                greet({"gx": device})

        for device in column_mates + row_mates:
            greet(device)
        for d in range(1, planes):
            @pl.when(plane + d < planes)
            def _(d=d):
                for b in range(BUDDY):
                    greet({"gx": home + d * BUDDY + b})

    else:
        greeted = 0
        for axis, me, n in axes:
            for d in range(1, n):
                greet(peer_of(axis, me, n, d)[1])
                greeted += 1

    basis_in = []
    for c in range(CHUNKS):
        part = pl.ds(c * step, step)
        basis_in.append(
            pltpu.make_async_copy(
                basis_hbm.at[part], basis_v.at[part, pl.ds(0, R)], in_sem.at[2 + c]
            )
        )
        basis_in[-1].start()
    def row_at(r):
        return pl.ds(r * LANES, LANES)

    def rate_row(d, r):
        return rates[pl.ds(d * T + 8 + r, 1), :]

    with jax.named_scope("inwait"):
        panel_in.wait()
        rate_in.wait()
    for d in range(4):
        rates[d * T : d * T + 8, :] = jnp.ones((8, LANES), F32)
        rates[d * T + 8 + R : (d + 1) * T, :] = jnp.ones((8, LANES), F32)
        rates[d * T + 8 : d * T + 8 + R, :] = (
            rate_v[d * R : (d + 1) * R, :].astype(F32) * 0.125
        )
    rates[4 * T + 8 : 4 * T + 8 + R, :] = (
        rates[8 : 8 + R, :]
        + rates[T + 8 : T + 8 + R, :]
        + rates[2 * T + 8 : 2 * T + 8 + R, :]
        + rates[3 * T + 8 : 3 * T + 8 + R, :]
    )

    routes = (
        ("gx", ix - 1, ix > 0, ix < nx - 1),
        ("gx", ix + 1, ix < nx - 1, ix > 0),
        ("gy", iy - 1, iy > 0, iy < ny - 1),
        ("gy", iy + 1, iy < ny - 1, iy > 0),
    )

    def edges(send, recv, ssem, rsem):
        def copy(e):
            return pltpu.make_async_remote_copy(
                src_ref=send.at[min(e, 2)],
                dst_ref=recv.at[e],
                send_sem=ssem.at[e],
                recv_sem=rsem.at[e],
                device_id={routes[e][0]: routes[e][1]},
                device_id_type=MESH,
            )

        def start(which=range(4)):
            for e in which:
                @pl.when(routes[e][2])
                def _(e=e):
                    copy(e).start()

                @pl.when(jnp.logical_not(routes[e][3]))
                def _(e=e):
                    recv[e] = jnp.zeros(recv.shape[1:], F32)

        def wait():
            for e in range(4):
                @pl.when(routes[e][3])
                def _(e=e):
                    copy(e).wait_recv()

        def drain():
            for e in range(4):
                @pl.when(routes[e][2])
                def _(e=e):
                    copy(e).wait_send()

        return start, wait, drain

    def share(buf, send_sem, recv_sem, axis, me, n, source=None):
        def copy(src, dst, device):
            return pltpu.make_async_remote_copy(
                src_ref=src,
                dst_ref=dst,
                send_sem=send_sem,
                recv_sem=recv_sem,
                device_id=device,
                device_id_type=MESH,
            )

        def start(store):
            store(buf.at[me])
            if axis == "all":
                for device in far_first:
                    copy(buf.at[me], buf.at[me], device).start()
                return
            for d in range(1, n):
                other, device = peer_of(axis, me, n, d)
                copy(buf.at[me] if source is None else source.at[other], buf.at[me], device).start()

        def all_of(ref):
            return copy(ref, ref, peer_of(axis, me, n, 1)[1])

        def wait():
            all_of(buf.at[pl.ds(0, n - 1)]).wait_recv()

        def finish():
            wait()
            parts = [buf[k] for k in range(n)]
            while len(parts) > 1:
                parts = [
                    parts[i] + parts[i + 1] if i + 1 < len(parts) else parts[i]
                    for i in range(0, len(parts), 2)
                ]
            return parts[0]

        return start, finish, all_of, wait

    half = N // 2

    def pack(v):
        turned = pltpu.roll(v, K, 1)
        tail = pltpu.roll(v, 0, 1, stride=2 * N, stride_axis=0)
        mine = lax.div(lane, 2 * N) == lax.rem(sub + K // (2 * N), N)
        tail = jnp.sum(jnp.where(mine, tail, 0.0), axis=0, keepdims=True)
        low = lax.broadcasted_iota(jnp.int32, (half, LANES), 1) < K
        return jnp.where(low, v[0:half], turned[half:N]), tail

    def unpack(t):
        body = jnp.concatenate([t[0:half], pltpu.roll(t[0:half], K, 1)], axis=0)
        spread = jnp.broadcast_to(t[half : half + 1], (N, LANES))
        tail = spread
        for j in range(1, N):
            tail = jnp.where(sub == j, pltpu.roll(spread, LANES - 2 * N * j, 1), tail)
        return jnp.where(lane < K, body, jnp.where(lane < Z, tail, 0.0))

    drains = []

    def reduction(s, value):
        xgroup = everyone if direct else axes[0]
        xstart, xfinish, all_of, _ = share(px_buf.at[s], px_s.at[2], px_s.at[s], *xgroup)
        if s:
            both = px_buf.at[:, pl.ds(0, xgroup[2] - 1)]
            drains.append(lambda: all_of(both).wait_send())

        def put(parts):
            def store(ref):
                ref[0:half] = parts[0]
                ref[half : half + 1] = parts[1]

            return store

        parts = pack(value)
        if direct:
            xstart(put(parts))
            return lambda: unpack(xfinish())
        ystart, yfinish, y_all_of, _ = share(py_buf.at[s], py_s.at[2], py_s.at[s], *axes[1])
        if s:
            y_both = py_buf.at[:, pl.ds(0, ny - 1)]
            drains.append(lambda: y_all_of(y_both).wait_send())
        ystart(put(parts))

        def finish():
            t = yfinish()
            xstart(put((t[0:half], t[half : half + 1])))
            return unpack(xfinish())

        return finish

    e0_start, e0_wait, e0_drain = edges(edge_send, edge_recv, edge_ssem, edge_rsem)
    e1_start, e1_wait, e1_drain = edges(eb_send, eb_recv, eb_ssem, eb_rsem)
    e2_start, e2_wait, e2_drain = edges(ew_send, ew_recv, edge_ssem, ew_rsem)
    drains += [e1_drain, e2_drain]

    def slots(shape, r):
        at = lax.broadcasted_iota(jnp.int32, shape, len(shape) - 1)
        return (at == 2 * r) | (at == (2 * r - 1) % LANES)

    def tuck(packed, r, f):
        return jnp.where(slots(f.shape, r), pltpu.roll(f, 2 * r, len(f.shape) - 1), packed)

    with jax.named_scope("packp"):
        lane_of = lax.broadcasted_iota(jnp.int32, (R, LANES), 1)
        sides = jnp.where(lane_of == 0, rates[2 * T + 8 : 2 * T + 8 + R, :], rates[3 * T + 8 : 3 * T + 8 + R, :])
        rate_side = jnp.zeros((N, LANES), F32)
        for i in range(R // 8):
            turned = pltpu.roll(sides[i * 8 : i * 8 + 8], 16 * i, 1, stride=2, stride_axis=0)
            mine = (lane == 2 * (sub + 8 * i)) | (lane == lax.rem(2 * (sub + 8 * i) + LANES - 1, LANES))
            rate_side = rate_side + jnp.where(mine, turned, 0.0)
        rate_side = jnp.sum(rate_side, axis=0, keepdims=True)
        edge_send[0] = panel_rows[pl.ds(0, N, stride=RP), :] * rate_row(0, 0)
        edge_send[1] = panel_rows[pl.ds(R - 1, N, stride=RP), :] * rate_row(1, R - 1)
    with jax.named_scope("barrier"):
        pl.semaphore_wait(barrier, greeted)
    e0_start((0, 1))
    packed = jnp.zeros((N, LANES), F32)
    for r in range(R):
        f = panel_rows[pl.ds(r, N, stride=RP), :]
        fext[:, row_at(r + 1)] = f
        packed = tuck(packed, r, f)
    edge_send[2] = packed * rate_side
    e0_start((2, 3))
    if direct:
        for device in row_mates:
            pl.semaphore_signal(ready.at[0], inc=1, device_id=device, device_id_type=MESH)
        for d in range(1, planes):
            @pl.when(plane >= d)
            def _(d=d):
                for b in range(BUDDY):
                    device = {"gx": home - d * BUDDY + b}
                    pl.semaphore_signal(ready.at[1], inc=1, device_id=device, device_id_type=MESH)

    def all_arrived():
        pl.semaphore_wait(ready.at[0], ny - 1)

        @pl.when(plane < planes - 1)
        def _():
            pl.semaphore_wait(ready.at[1], BUDDY * (planes - 1 - plane))

    with jax.named_scope("split"):
        for c in range(CHUNKS):
            basis_in[c].wait()
            mine = slice(c * step, (c + 1) * step)
            above = slice(HI + c * step, HI + (c + 1) * step)
            below = slice(LO + c * step, LO + (c + 1) * step)

            packed = jnp.zeros((step, LANES), F32)
            for r in range(R):
                b = basis_rows[pl.ds(c * step * RP + r, step, stride=RP), :]
                hi = b.astype(BF)
                x_v[above, row_at(r)] = hi
                x_v[below, row_at(r)] = (b - hi.astype(F32)).astype(BF)
                packed = tuck(packed, r, b)
            hi = packed.astype(BF)
            x_v[above, pl.ds(EXT, LANES)] = hi
            x_v[below, pl.ds(EXT, LANES)] = (packed - hi.astype(F32)).astype(BF)
            eb_send[2, mine] = packed * rate_side
            eb_send[0, mine] = basis_rows[pl.ds(c * step * RP, step, stride=RP), :] * rate_row(0, 0)
            eb_send[1, mine] = (
                basis_rows[pl.ds(c * step * RP + R - 1, step, stride=RP), :] * rate_row(1, R - 1)
            )

    e1_start()

    def sides(from_right, from_left):
        side = jnp.where(lax.rem(lane, 2) == 1, from_left, pltpu.roll(from_right, LANES - 2, 1))
        return lambda r: pltpu.roll(side, (LANES + 1 - 2 * r) % LANES, 1)

    def stencil(beside, finish):
        for r in range(R):
            f = fext[:, row_at(r + 1)]
            above = fext[:, row_at(r)] * rate_row(1, r - 1)
            below = fext[:, row_at(r + 2)] * rate_row(0, r + 1)
            west = pltpu.roll(f * rate_row(3, r), 1, 1)
            east = pltpu.roll(f * rate_row(2, r), LANES - 1, 1)
            other = beside(r)
            west = jnp.where(lane == 0, other, west)
            east = jnp.where(lane == LANES - 1, other, east)
            finish(r, f, above + below + west + east - rate_row(4, r) * f)

    def put_pair(at, upper, lower):
        both = jnp.concatenate([upper, lower], axis=0)
        hi = both.astype(BF)
        low = both - hi.astype(F32)
        x_v[HI + K : LO, at] = hi
        x_v[LO + K : LO + Z, at] = low.astype(BF)
        return hi.astype(F32), low

    def put_rhs(at, hi, low):
        x_v[0:HI, at] = jnp.concatenate([hi, low], axis=0).astype(BF)

    def against(at, width):
        return [
            dot_nt(x_v[top : top + Z, at], x_v[0:width, at], lax.Precision.DEFAULT)
            for top in (HI, LO)
        ]

    def halves(width):
        parts = [against(pl.ds(h * (sites // 2), sites // 2), width) for h in range(2)]
        return [parts[0][i] * scale + parts[1][i] * scale for i in range(2)]

    def turned(total):
        t_v[0:Z, 0:HI] = total
        value = t_v[...].T
        return value[0:N] + value[N:HI]

    mid = K // 2
    part = mid // ny
    my_buf, mx_buf, mz_buf = (
        mm_buf.at[pl.ds(at, n)] for at, n in ((0, ny), (ny, nx), (ny + nx, ny))
    )
    m1_start, m1_finish, m_all_of, _ = share(my_buf, m_s.at[3], m_s.at[0], *axes[1], source=ms_buf)
    m2_start, m2_finish, _, _ = share(mx_buf, m_s.at[3], m_s.at[1], *axes[0])
    m3_start, _, _, m3_wait = share(mz_buf, m_s.at[3], m_s.at[2], *axes[1])
    m_sent = mm_buf.at[pl.ds(0, 2 * (ny - 1) + nx - 1)]
    drains.append(lambda: m_all_of(m_sent).wait_send())

    zero = jnp.zeros((N, LANES), F32)
    with jax.named_scope("sten0"):
        t_v[...] = jnp.zeros_like(t_v)
        fext[:, 0:LANES] = zero
        fext[:, (R + 1) * LANES : (R + 2) * LANES] = zero
        columns = [zero]

        def finish_first(r, f, w):
            wf[:, row_at(r)] = w
            hi, low = put_pair(row_at(r), w, zero)
            put_rhs(row_at(r), hi[0:N], low[0:N])

        stencil(lambda r: 0.0, finish_first)
    with jax.named_scope("tuck0"):
        for r in range(R):
            columns[0] = tuck(columns[0], r, wf[:, row_at(r)])
    with jax.named_scope("gram"):
        high, low = halves(HI + K)
        first = (high + low)[:, 0:HI]
        g_v[...] = jnp.zeros_like(g_v)
        g_v[0, 0:K, 0 : HI + K] = (high + low)[0:K]
        g_v[1, 0:K, 0 : HI + K] = low[0:K]
        straight = g_v[0]
        flipped = g_v[1].T[HI : HI + K]
        is_low = lax.broadcasted_iota(jnp.int32, (mid, LANES), 1) < K
        full = jnp.where(
            is_low,
            pltpu.roll(straight[0:mid], LANES - HI, 1) + flipped[0:mid],
            pltpu.roll(straight[mid:K], K - HI, 1) + pltpu.roll(flipped[mid:K], K, 1),
        )
        for p in range(ny):
            ms_buf[p] = full[p * part : (p + 1) * part]

        def put_own(ref):
            ref[...] = ms_buf[iy]

        m1_start(put_own)

    with jax.named_scope("ewait0"):
        e0_wait()
    with jax.named_scope("lat0"):
        from_below, from_above, from_right, from_left = [edge_recv[e] for e in range(4)]
        gain = jnp.where(
            lax.rem(lane, 2) == 0, pltpu.roll(from_left, 1, 1), pltpu.roll(from_right, LANES - 1, 1)
        )
        column = columns[0]
        column = jnp.where(slots(zero.shape, 0), column + from_above, column)
        column = jnp.where(
            slots(zero.shape, R - 1), column + pltpu.roll(from_below, 2 * (R - 1), 1), column
        )
        ends = ((0, from_above), (R - 1, from_below))
        for r, extra in ends:
            w = wf[:, row_at(r)]
            put_pair(row_at(r), zero, w + 0.5 * extra)
            put_rhs(row_at(r), *split(extra))
            wf[:, row_at(r)] = w + extra
        put_pair(pl.ds(EXT, LANES), zero, column + 0.5 * gain)
        put_rhs(pl.ds(EXT, LANES), *split(gain))
        last = against(pl.ds(sites - LANES, 2 * LANES), HI)
        top = against(row_at(0), HI)
        value = turned(first + ((last[0] + last[1]) + (top[0] + top[1])) * scale)
        if direct:
            all_arrived()
        finish0 = reduction(0, value)
    with jax.named_scope("packw"):
        beside = sides(from_right, from_left)
        outer = (lane == 0) | (lane == LANES - 1)
        for r in range(R):
            wf[:, row_at(r)] = wf[:, row_at(r)] + jnp.where(outer, beside(r), 0.0)
        ew_send[0] = wf[:, row_at(0)] * rate_row(0, 0)
        ew_send[1] = wf[:, row_at(R - 1)] * rate_row(1, R - 1)
        ew_send[2] = (column + gain) * rate_side
    e0_drain()
    e2_start()

    with jax.named_scope("ewait1"):
        e1_wait()
    with jax.named_scope("esplit"):
        for e in range(4):
            at = pl.ds(EDGE + e * LANES, LANES)
            b = eb_recv[e]
            hi = b.astype(BF)
            x_v[HI : HI + K, at] = hi
            x_v[LO : LO + K, at] = (b - hi.astype(F32)).astype(BF)

    def forward(ref, value):
        ref[...] = value

    with jax.named_scope("m12"):
        m = m1_finish()
        m2_start(lambda ref: forward(ref, m))
    with jax.named_scope("ewait2"):
        e2_wait()
        for e in range(4):
            wf[:, pl.ds(EDGE + e * LANES, LANES)] = ew_recv[e]
    with jax.named_scope("red0"):
        total = finish0()

    def combine(lhs, at):
        both = jnp.dot(lhs, x_v[HI:LO, at], preferred_element_type=F32) + jnp.dot(
            lhs, x_v[LO : LO + Z, at], preferred_element_type=F32
        )
        return both[0:N] + both[N : 2 * N]

    wide8 = 8 * LANES
    pm = jnp.where(lane < K, total, 0.0)
    def project(lhs, at):
        both = jnp.dot(lhs, x_v[HI : HI + K, at], preferred_element_type=F32) + jnp.dot(
            lhs, x_v[LO : LO + K, at], preferred_element_type=F32
        )
        return both[0:N] + both[N : 2 * N]

    with jax.named_scope("new0"):
        lhs = split_rows(pm)[:, 0:K]
        at = pl.ds(EDGE, 4 * LANES)
        edge = wf[:, at] - project(lhs, at)
        fext[:, 0:LANES] = edge[:, LANES : 2 * LANES]
        fext[:, (R + 1) * LANES : (R + 2) * LANES] = edge[:, 0:LANES]
        for i in range(R // 8):
            at = pl.ds(i * wide8, wide8)
            fext[:, pl.ds(LANES + i * wide8, wide8)] = wf[:, at] - project(lhs, at)
    with jax.named_scope("lat1"):
        def finish_second(r, f, u):
            hi, low = put_pair(row_at(r), f, u)
            put_rhs(row_at(r), hi[N:HI], low[N:HI])

        with jax.named_scope("sten1"):
            stencil(
                sides(edge[:, 2 * LANES : 3 * LANES], edge[:, 3 * LANES : 4 * LANES]), finish_second
            )
        with jax.named_scope("prod1"):
            high, low = halves(HI)
            value = turned(high + low)
        m_own = m2_finish()
        m3_start(lambda ref: forward(ref, m_own))
        finish1 = reduction(1, value)

    with jax.named_scope("mxfin"):
        m3_wait()
        m = jnp.concatenate([mz_buf[p] for p in range(ny)], axis=0)
        gram = rows_full(
            jnp.concatenate(
                [
                    jnp.where(lax.broadcasted_iota(jnp.int32, (mid, LANES), 1) < K, m, 0.0),
                    jnp.where(
                        lax.broadcasted_iota(jnp.int32, (mid, LANES), 1) < K,
                        pltpu.roll(m, LANES - K, 1),
                        0.0,
                    ),
                ],
                axis=0,
            )
        )
    G0 = Z

    def times(parts, stacked):
        pair = jnp.concatenate(parts, axis=0).astype(BF)
        both = jnp.dot(
            jnp.concatenate([pair, pair], axis=1), stacked, preferred_element_type=F32
        )
        return both[0:N] + both[N : 2 * N]

    def gram_of(value, parts):
        both = sum(
            dot_nt(split_rows(value), rows_full(p, G0).astype(BF), lax.Precision.DEFAULT)
            for p in parts
        )
        return both[0:N] + both[N : 2 * N]

    with jax.named_scope("fac0"):
        own = (
            pltpu.roll(total, G0 - K, 1)
            + pltpu.roll(total, G0 - KN, 1)
            + pltpu.roll(rows_full(total).T[KN:Z], G0, 1)
        )
        pm_parts = split(pm)
        rest = 2.0 * pm - times(pm_parts, jnp.concatenate(split(gram), axis=0).astype(BF))
        g = own - gram_of(rest, pm_parts)
        g = jnp.where((lane >= G0) & (lane < G0 + N), g, 0.0)
        a = jnp.where(lane < K, rest - pm, jnp.where(lane == sub + K, 1.0, g))
        a = eliminate(a, G0, N)
        at_t = rows_full(a).T
        inv = pltpu.roll(a, LANES - K, 1)
        inv = jnp.where(lane < N, inv, 0.0)
        low1 = at_t[G0 : G0 + N]
        coefs[0] = pm + jnp.where((lane >= K) & (lane < KN), pltpu.roll(low1, K, 1), 0.0)
        row = lax.broadcasted_iota(jnp.int32, (LANES, LANES), 0)
        col = lax.broadcasted_iota(jnp.int32, (LANES, LANES), 1)
        inner = jnp.where((row < KN), at_t, 0.0)
        flow = dot_nn(inner, rows_full(jnp.where(lane < KN, a, 0.0)))
        in_b = (row < K) & (col < K)
        in_w = (row >= K) & (row < KN) & (col >= K) & (col < KN)
        eye = jnp.where(row == col, 1.0, 0.0)
        kmat = jnp.where(in_b, 2.0 * eye - gram, jnp.where(in_w, flow, -flow))
        dmat = jnp.where(in_b, eye, jnp.where(in_w, flow, 0.0))
        tmat = jnp.where((row >= K) & (row < KN) & (col < N), at_t, 0.0)
        for i, mat in enumerate((kmat, dmat, tmat)):
            hi, low = split(mat)
            m_v[0:LANES, i * LANES : (i + 1) * LANES] = hi.astype(BF)
            m_v[LANES : 2 * LANES, i * LANES : (i + 1) * LANES] = low.astype(BF)
    with jax.named_scope("q1"):
        lhs = split_rows(inv)[:, 0 : 2 * N]
        for i in range(R // 8):
            at = pl.ds(i * wide8, wide8)
            both = jnp.dot(lhs, x_v[HI + K : LO, at], preferred_element_type=F32) + jnp.dot(
                lhs, x_v[LO + K : LO + Z, at], preferred_element_type=F32
            )
            q = both[0:N] + both[N : 2 * N]
            for u in range(8):
                first_v[pl.ds(i * 8 + u, N, stride=RP), :] = q[:, u * LANES : (u + 1) * LANES]

    with jax.named_scope("red1"):
        total = finish1()
    with jax.named_scope("fac1"):
        ep = jnp.where(lane < KN, total, 0.0)
        own = pltpu.roll(total, G0 - KN, 1)
        ep_parts = split(ep)
        both = times(ep_parts, m_v[:, 0 : 2 * LANES])
        ek, ed = both[:, 0:LANES], both[:, LANES : 2 * LANES]
        g = own - gram_of(ek, ep_parts)
        g = jnp.where((lane >= G0) & (lane < G0 + N), g, 0.0)
        a = jnp.where(lane < KN, ed, jnp.where(lane == sub + KN, 1.0, g))
        a = eliminate(a, G0, N)
        lhs = split_rows(jnp.where(lane < KN, -a, a))[:, 0:Z]
    with jax.named_scope("new1"):
        for i in range(R // 8):
            q = combine(lhs, pl.ds(i * wide8, wide8))
            for u in range(8):
                second_v[pl.ds(i * 8 + u, N, stride=RP), :] = q[:, u * LANES : (u + 1) * LANES]
    with jax.named_scope("coef1"):
        low2 = rows_full(a).T[G0 : G0 + N]
        es = times(ep_parts, m_v[:, 2 * LANES : 3 * LANES])
        stack = jnp.where(lane < K, ep, jnp.where(lane < KN, pltpu.roll(es, K, 1), 0.0))
        stack = jnp.where((lane >= KN) & (lane < Z), pltpu.roll(low2, KN, 1), stack)
        coefs[1] = dot_nn(inv, rows_full(stack))
    with jax.named_scope("drain"):
        for drain in drains:
            drain()


def deliver(
    R, first_v, second_v, coefs, first_hbm, second_hbm, one_hbm, two_hbm, coef_one, coef_two, sem
):
    copies = [
        pltpu.make_async_copy(first_v.at[:, pl.ds(0, R)], first_hbm, sem.at[0]),
        pltpu.make_async_copy(second_v.at[:, pl.ds(0, R)], second_hbm, sem.at[1]),
        pltpu.make_async_copy(coef_one, one_hbm, sem.at[2]),
        pltpu.make_async_copy(coef_two, two_hbm, sem.at[3]),
    ]
    for copy in copies[:2]:
        copy.start()
    coef_one[...] = coefs[0, :, 0 : coef_one.shape[1]]
    coef_two[...] = coefs[1, :, 0 : coef_two.shape[1]]
    for copy in copies[2:]:
        copy.start()
    for copy in copies:
        copy.wait()


def local(nx, ny, basis, panel, rate_codes):
    N, R, C = panel.shape
    K = basis.shape[0]
    assert C == LANES and 2 * K == LANES and N == 8
    vmem = pl.BlockSpec(memory_space=pltpu.VMEM)
    hbm = pl.BlockSpec(memory_space=pl.ANY)
    dma = pltpu.SemaphoreType.DMA
    sites = R * LANES
    group = nx * ny if nx * ny <= DIRECT else nx
    Z = K + 2 * N
    first, second, coefs = pl.pallas_call(
        functools.partial(kernel, nx, ny, K, N, R),
        out_shape=(
            pltpu.VMEM((N * (R + PAD), C), F32),
            pltpu.VMEM((N * (R + PAD), C), F32),
            pltpu.VMEM((2, N, C), F32),
        ),
        in_specs=[pl.BlockSpec(memory_space=pltpu.HBM)] * 3,
        out_specs=(vmem, vmem, vmem),
        scratch_shapes=[
            pltpu.VMEM((K, R + PAD, LANES), F32),
            pltpu.VMEM((N, R + PAD, LANES), F32),
            pltpu.VMEM((4 * R, LANES), jnp.int32),
            pltpu.VMEM((5 * (R + 16), LANES), F32),
            pltpu.VMEM((N, (R + 2) * LANES), F32),
            pltpu.VMEM((N, sites + 5 * LANES), F32),
            pltpu.VMEM((2 * N + 2 * Z, sites + 5 * LANES), BF),
            pltpu.VMEM((2 * LANES, 3 * LANES), BF),
            pltpu.VMEM((LANES, LANES), F32),
            pltpu.VMEM((2, LANES, LANES), F32),
            pltpu.VMEM((3, N, LANES), F32),
            pltpu.VMEM((4, N, LANES), F32),
            pltpu.VMEM((3, K, LANES), F32),
            pltpu.VMEM((4, K, LANES), F32),
            pltpu.VMEM((3, N, LANES), F32),
            pltpu.VMEM((4, N, LANES), F32),
            pltpu.VMEM((ny, K // 2 // ny, LANES), F32),
            pltpu.VMEM((2 * ny + nx, K // 2 // ny, LANES), F32),
            pltpu.VMEM((2, ny, N // 2 + 1, LANES), F32),
            pltpu.VMEM((2, group, N // 2 + 1, LANES), F32),
            dma((2 + CHUNKS,)),
            dma((4,)),
            dma((4,)),
            dma((4,)),
            dma((4,)),
            dma((4,)),
            pltpu.SemaphoreType.REGULAR((2,)),
            dma((4,)),
            dma((1 if nx * ny <= DIRECT and nx % BUDDY == 0 else 3,)),
            dma((3,)),
        ],
        compiler_params=pltpu.CompilerParams(
            collective_id=0, has_side_effects=True
        ),
    )(basis, panel, rate_codes.reshape(rate_codes.shape[0] * R, C))
    first, second, coef_one, coef_two = pl.pallas_call(
        functools.partial(deliver, R),
        out_shape=(
            jax.ShapeDtypeStruct((N, R, C), F32),
            jax.ShapeDtypeStruct((N, R, C), F32),
            jax.ShapeDtypeStruct((N, K + N), F32),
            jax.ShapeDtypeStruct((N, K + 2 * N), F32),
        ),
        in_specs=[vmem] * 3,
        out_specs=(hbm, hbm, hbm, hbm),
        scratch_shapes=[
            pltpu.VMEM((N, K + N), F32),
            pltpu.VMEM((N, K + 2 * N), F32),
            dma((4,)),
        ],
        compiler_params=pltpu.CompilerParams(vmem_limit_bytes=4 * 2**20),
    )(first.reshape(N, R + PAD, C), second.reshape(N, R + PAD, C), coefs)
    return first, second, coef_one.T, coef_two.T


def solution(mesh):
    spec = P(None, "gx", "gy")
    return jax.shard_map(
        functools.partial(local, mesh.shape["gx"], mesh.shape["gy"]),
        mesh=mesh,
        in_specs=(spec, spec, spec),
        out_specs=(spec, spec, P(), P()),
        check_vma=False,
    )
```

```python
import functools

import jax
import jax.numpy as jnp
from jax import lax
from jax.experimental import pallas as pl
from jax.experimental.pallas import tpu as pltpu
from jax.sharding import PartitionSpec as P

HIGH = lax.Precision.HIGHEST
MESH = pl.DeviceIdType.MESH
F32 = jnp.float32
BF = jnp.bfloat16
LANES = 128
CHUNKS = 4
DIRECT = 64
BUDDY = 2
PAD = 8


def dot_nn(a, b):
    return jnp.dot(a, b, precision=HIGH, preferred_element_type=F32)


def dot_nt(a, b, precision=HIGH):
    return lax.dot_general(
        a, b, (((1,), (1,)), ((), ())), precision=precision, preferred_element_type=F32
    )


def rows_full(v, at=0):
    parts = [v, jnp.zeros((LANES - at - v.shape[0], LANES), F32)]
    if at:
        parts.insert(0, jnp.zeros((at, LANES), F32))
    return jnp.concatenate(parts, axis=0)


def split(v):
    hi = v.astype(BF).astype(F32)
    return hi, v - hi


def split_rows(v):
    return jnp.concatenate(split(v), axis=0).astype(BF)


def eliminate(a, g0, n):
    sub = lax.broadcasted_iota(jnp.int32, a.shape, 0)
    cols = [jnp.broadcast_to(a[:, g0 + j : g0 + j + 1], a.shape) for j in range(n)]
    pivots = jnp.ones(a.shape, F32)
    for k in range(n):
        pivot = jnp.broadcast_to(cols[k][k : k + 1, :], a.shape)
        pivots = jnp.where(sub == k, pivot, pivots)
        if k == n - 1:
            break
        factor = jnp.where(sub > k, cols[k] * (1.0 / pivot), 0.0)
        for j in range(k + 1, n):
            cols[j] = cols[j] - factor * cols[j][k : k + 1, :]
        a = a - factor * a[k : k + 1, :]
    return a * (1.0 / jnp.sqrt(pivots))


def kernel(
    nx, ny, K, N, R,
    basis_hbm, panel_hbm, rate_hbm,
    first_v, second_v, coefs,
    basis_v, panel_v, rate_v, rates, fext, wf, x_v, m_v, t_v, g_v,
    edge_send, edge_recv, eb_send, eb_recv, ew_send, ew_recv, ms_buf, mm_buf, py_buf, px_buf,
    in_sem, edge_ssem, edge_rsem, eb_ssem, eb_rsem, ew_rsem, ready,
    m_s, py_s, px_s,
):
    ix, iy = lax.axis_index("gx"), lax.axis_index("gy")
    sites = R * LANES
    scale = 1.0 / (sites * nx * ny)
    lane = lax.broadcasted_iota(jnp.int32, (N, LANES), 1)
    sub = lax.broadcasted_iota(jnp.int32, (N, LANES), 0)
    KN = K + N
    Z = K + 2 * N
    HI = 2 * N
    LO = HI + Z
    EXT = sites
    EDGE = sites + LANES
    RP = R + PAD
    T = R + 16

    basis_rows = basis_v.reshape(K * RP, LANES)
    panel_rows = panel_v.reshape(N * RP, LANES)

    axes = (("gx", ix, nx), ("gy", iy, ny))
    everyone = ("all", ix * ny + iy, nx * ny)
    direct = nx * ny <= DIRECT and nx % BUDDY == 0

    def peer_of(axis, me, n, d):
        other = lax.rem(me + d, n)
        if axis == "all":
            return other, {"gx": lax.div(other, ny), "gy": lax.rem(other, ny)}
        return other, {axis: other}

    with jax.named_scope("dma0"):
        step = K // CHUNKS
        panel_in = pltpu.make_async_copy(panel_hbm, panel_v.at[:, pl.ds(0, R)], in_sem.at[0])
        rate_in = pltpu.make_async_copy(rate_hbm, rate_v, in_sem.at[1])
        panel_in.start()
        rate_in.start()

    barrier = pltpu.get_barrier_semaphore()

    def greet(device):
        pl.semaphore_signal(barrier, inc=1, device_id=device, device_id_type=MESH)

    if direct:
        planes = nx // BUDDY
        plane = lax.div(ix, BUDDY)
        home = plane * BUDDY
        group = BUDDY * ny
        seat = (ix - home) * ny + iy
        mates = []
        for d in range(1, group):
            other = lax.rem(seat + d, group)
            mates.append({"gx": home + lax.div(other, ny), "gy": lax.rem(other, ny)})
        outer = [
            ((ix == home) & (ix > 0), ix - 1),
            ((ix == home + BUDDY - 1) & (ix < nx - 1), ix + 1),
        ]
        if planes % 2:
            others = [lax.rem(plane + d, planes) for d in range(1, planes)]
        else:
            others = [lax.rem(planes + c - plane, planes) for c in range(planes - 1, 0, -2)]
            others += [lax.rem(plane + d, planes) for d in range(2, planes, 2)]
        far_first = []
        for other in others:
            for k in range(group):
                to = lax.rem(seat + k + group // 2, group)
                far_first.append(other * group + to)
        far_first += [plane * group + lax.rem(seat + d, group) for d in range(1, group)]
        row_mates = [{"gy": lax.rem(iy + d, ny)} for d in range(1, ny)]
        column_mates = [{"gx": home + lax.rem(ix - home + d, BUDDY)} for d in range(1, BUDDY)]
        greeted = ny - 1 + BUDDY - 1 + BUDDY * plane
        for there, device in outer:
            greeted = greeted + jnp.where(there, 1, 0)

            @pl.when(there)
            def _(device=device):
                greet({"gx": device})

        for device in column_mates + row_mates:
            greet(device)
        for d in range(1, planes):
            @pl.when(plane + d < planes)
            def _(d=d):
                for b in range(BUDDY):
                    greet({"gx": home + d * BUDDY + b})

    else:
        greeted = 0
        for axis, me, n in axes:
            for d in range(1, n):
                greet(peer_of(axis, me, n, d)[1])
                greeted += 1

    basis_in = []
    for c in range(CHUNKS):
        part = pl.ds(c * step, step)
        basis_in.append(
            pltpu.make_async_copy(
                basis_hbm.at[part], basis_v.at[part, pl.ds(0, R)], in_sem.at[2 + c]
            )
        )
        basis_in[-1].start()
    def row_at(r):
        return pl.ds(r * LANES, LANES)

    def rate_row(d, r):
        return rates[pl.ds(d * T + 8 + r, 1), :]

    with jax.named_scope("inwait"):
        panel_in.wait()
        rate_in.wait()
    routes = (
        ("gx", ix - 1, ix > 0, ix < nx - 1),
        ("gx", ix + 1, ix < nx - 1, ix > 0),
        ("gy", iy - 1, iy > 0, iy < ny - 1),
        ("gy", iy + 1, iy < ny - 1, iy > 0),
    )

    def edges(send, recv, ssem, rsem):
        def copy(e):
            return pltpu.make_async_remote_copy(
                src_ref=send.at[min(e, 2)],
                dst_ref=recv.at[e],
                send_sem=ssem.at[e],
                recv_sem=rsem.at[e],
                device_id={routes[e][0]: routes[e][1]},
                device_id_type=MESH,
            )

        def start(which=range(4)):
            for e in which:
                @pl.when(routes[e][2])
                def _(e=e):
                    copy(e).start()

                @pl.when(jnp.logical_not(routes[e][3]))
                def _(e=e):
                    recv[e] = jnp.zeros(recv.shape[1:], F32)

        def wait():
            for e in range(4):
                @pl.when(routes[e][3])
                def _(e=e):
                    copy(e).wait_recv()

        def drain():
            for e in range(4):
                @pl.when(routes[e][2])
                def _(e=e):
                    copy(e).wait_send()

        return start, wait, drain

    def share(buf, send_sem, recv_sem, axis, me, n, source=None):
        def copy(src, dst, device):
            by_mesh = isinstance(device, dict)
            return pltpu.make_async_remote_copy(
                src_ref=src,
                dst_ref=dst,
                send_sem=send_sem,
                recv_sem=recv_sem,
                device_id=device,
                device_id_type=MESH if by_mesh else pl.DeviceIdType.LOGICAL,
            )

        def start(store):
            store(buf.at[me])
            if axis == "all":
                for device in far_first:
                    copy(buf.at[me], buf.at[me], device).start()
                return
            for d in range(1, n):
                other, device = peer_of(axis, me, n, d)
                copy(buf.at[me] if source is None else source.at[other], buf.at[me], device).start()

        def all_of(ref):
            return copy(ref, ref, peer_of(axis, me, n, 1)[1])

        def wait():
            all_of(buf.at[pl.ds(0, n - 1)]).wait_recv()

        def finish():
            wait()
            parts = [buf[k] for k in range(n)]
            while len(parts) > 1:
                parts = [
                    parts[i] + parts[i + 1] if i + 1 < len(parts) else parts[i]
                    for i in range(0, len(parts), 2)
                ]
            return parts[0]

        return start, finish, all_of, wait

    half = N // 2

    def pack(v):
        turned = pltpu.roll(v, K, 1)
        tail = pltpu.roll(v, 0, 1, stride=2 * N, stride_axis=0)
        mine = lax.div(lane, 2 * N) == lax.rem(sub + K // (2 * N), N)
        tail = jnp.sum(jnp.where(mine, tail, 0.0), axis=0, keepdims=True)
        low = lax.broadcasted_iota(jnp.int32, (half, LANES), 1) < K
        return jnp.where(low, v[0:half], turned[half:N]), tail

    def unpack(t):
        body = jnp.concatenate([t[0:half], pltpu.roll(t[0:half], K, 1)], axis=0)
        spread = jnp.broadcast_to(t[half : half + 1], (N, LANES))
        tail = spread
        for j in range(1, N):
            tail = jnp.where(sub == j, pltpu.roll(spread, LANES - 2 * N * j, 1), tail)
        return jnp.where(lane < K, body, jnp.where(lane < Z, tail, 0.0))

    drains = []

    def reduction(s, value):
        xgroup = everyone if direct else axes[0]
        xstart, xfinish, all_of, _ = share(px_buf.at[s], px_s.at[2], px_s.at[s], *xgroup)
        if s:
            both = px_buf.at[:, pl.ds(0, xgroup[2] - 1)]
            drains.append(lambda: all_of(both).wait_send())

        def put(parts):
            def store(ref):
                ref[0:half] = parts[0]
                ref[half : half + 1] = parts[1]

            return store

        parts = pack(value)
        if direct:
            xstart(put(parts))
            return lambda: unpack(xfinish())
        ystart, yfinish, y_all_of, _ = share(py_buf.at[s], py_s.at[2], py_s.at[s], *axes[1])
        if s:
            y_both = py_buf.at[:, pl.ds(0, ny - 1)]
            drains.append(lambda: y_all_of(y_both).wait_send())
        ystart(put(parts))

        def finish():
            t = yfinish()
            xstart(put((t[0:half], t[half : half + 1])))
            return unpack(xfinish())

        return finish

    e0_start, e0_wait, e0_drain = edges(edge_send, edge_recv, edge_ssem, edge_rsem)
    e1_start, e1_wait, e1_drain = edges(eb_send, eb_recv, eb_ssem, eb_rsem)
    e2_start, e2_wait, e2_drain = edges(ew_send, ew_recv, edge_ssem, ew_rsem)
    drains += [e1_drain, e2_drain]

    def slots(shape, r):
        at = lax.broadcasted_iota(jnp.int32, shape, len(shape) - 1)
        return (at == 2 * r) | (at == (2 * r - 1) % LANES)

    def tuck(packed, r, f):
        return jnp.where(slots(f.shape, r), pltpu.roll(f, 2 * r, len(f.shape) - 1), packed)

    def end_row(d, r):
        return panel_rows[pl.ds(r, N, stride=RP), :] * (
            rate_v[d * R + r : d * R + r + 1, :].astype(F32) * 0.125
        )

    edge_send[0] = end_row(0, 0)
    edge_send[1] = end_row(1, R - 1)
    with jax.named_scope("barrier"):
        pl.semaphore_wait(barrier, greeted)
    e0_start((0, 1))
    for d in range(4):
        rates[d * T : d * T + 8, :] = jnp.ones((8, LANES), F32)
        rates[d * T + 8 + R : (d + 1) * T, :] = jnp.ones((8, LANES), F32)
        rates[d * T + 8 : d * T + 8 + R, :] = (
            rate_v[d * R : (d + 1) * R, :].astype(F32) * 0.125
        )
    rates[4 * T + 8 : 4 * T + 8 + R, :] = (
        rates[8 : 8 + R, :]
        + rates[T + 8 : T + 8 + R, :]
        + rates[2 * T + 8 : 2 * T + 8 + R, :]
        + rates[3 * T + 8 : 3 * T + 8 + R, :]
    )

    with jax.named_scope("packp"):
        lane_of = lax.broadcasted_iota(jnp.int32, (R, LANES), 1)
        sides = jnp.where(lane_of == 0, rates[2 * T + 8 : 2 * T + 8 + R, :], rates[3 * T + 8 : 3 * T + 8 + R, :])
        rate_side = jnp.zeros((N, LANES), F32)
        for i in range(R // 8):
            turned = pltpu.roll(sides[i * 8 : i * 8 + 8], 16 * i, 1, stride=2, stride_axis=0)
            mine = (lane == 2 * (sub + 8 * i)) | (lane == lax.rem(2 * (sub + 8 * i) + LANES - 1, LANES))
            rate_side = rate_side + jnp.where(mine, turned, 0.0)
        rate_side = jnp.sum(rate_side, axis=0, keepdims=True)
    packed = jnp.zeros((N, LANES), F32)
    for r in range(R):
        f = panel_rows[pl.ds(r, N, stride=RP), :]
        fext[:, row_at(r + 1)] = f
        packed = tuck(packed, r, f)
    edge_send[2] = packed * rate_side
    e0_start((2, 3))
    if direct:
        for device in row_mates:
            pl.semaphore_signal(ready.at[0], inc=1, device_id=device, device_id_type=MESH)
        for d in range(1, planes):
            @pl.when(plane >= d)
            def _(d=d):
                for b in range(BUDDY):
                    device = {"gx": home - d * BUDDY + b}
                    pl.semaphore_signal(ready.at[1], inc=1, device_id=device, device_id_type=MESH)

    def all_arrived():
        pl.semaphore_wait(ready.at[0], ny - 1)

        @pl.when(plane < planes - 1)
        def _():
            pl.semaphore_wait(ready.at[1], BUDDY * (planes - 1 - plane))

    with jax.named_scope("split"):
        for c in range(CHUNKS):
            basis_in[c].wait()
            mine = slice(c * step, (c + 1) * step)
            above = slice(HI + c * step, HI + (c + 1) * step)
            below = slice(LO + c * step, LO + (c + 1) * step)

            packed = jnp.zeros((step, LANES), F32)
            for r in range(R):
                b = basis_rows[pl.ds(c * step * RP + r, step, stride=RP), :]
                hi = b.astype(BF)
                x_v[above, row_at(r)] = hi
                x_v[below, row_at(r)] = (b - hi.astype(F32)).astype(BF)
                packed = tuck(packed, r, b)
            hi = packed.astype(BF)
            x_v[above, pl.ds(EXT, LANES)] = hi
            x_v[below, pl.ds(EXT, LANES)] = (packed - hi.astype(F32)).astype(BF)
            eb_send[2, mine] = packed * rate_side
            eb_send[0, mine] = basis_rows[pl.ds(c * step * RP, step, stride=RP), :] * rate_row(0, 0)
            eb_send[1, mine] = (
                basis_rows[pl.ds(c * step * RP + R - 1, step, stride=RP), :] * rate_row(1, R - 1)
            )

    e1_start()

    def sides(from_right, from_left):
        side = jnp.where(lax.rem(lane, 2) == 1, from_left, pltpu.roll(from_right, LANES - 2, 1))
        return lambda r: pltpu.roll(side, (LANES + 1 - 2 * r) % LANES, 1)

    def stencil(beside, finish):
        for r in range(R):
            f = fext[:, row_at(r + 1)]
            above = fext[:, row_at(r)] * rate_row(1, r - 1)
            below = fext[:, row_at(r + 2)] * rate_row(0, r + 1)
            west = pltpu.roll(f * rate_row(3, r), 1, 1)
            east = pltpu.roll(f * rate_row(2, r), LANES - 1, 1)
            other = beside(r)
            west = jnp.where(lane == 0, other, west)
            east = jnp.where(lane == LANES - 1, other, east)
            finish(r, f, above + below + west + east - rate_row(4, r) * f)

    def put_pair(at, upper, lower):
        both = jnp.concatenate([upper, lower], axis=0)
        hi = both.astype(BF)
        low = both - hi.astype(F32)
        x_v[HI + K : LO, at] = hi
        x_v[LO + K : LO + Z, at] = low.astype(BF)
        return hi.astype(F32), low

    def put_rhs(at, hi, low):
        x_v[0:HI, at] = jnp.concatenate([hi, low], axis=0).astype(BF)

    def against(at, width):
        return [
            dot_nt(x_v[top : top + Z, at], x_v[0:width, at], lax.Precision.DEFAULT)
            for top in (HI, LO)
        ]

    def halves(width):
        parts = [against(pl.ds(h * (sites // 2), sites // 2), width) for h in range(2)]
        return [parts[0][i] * scale + parts[1][i] * scale for i in range(2)]

    def turned(total):
        t_v[0:Z, 0:HI] = total
        value = t_v[...].T
        return value[0:N] + value[N:HI]

    mid = K // 2
    part = mid // ny
    my_buf, mx_buf, mz_buf = (
        mm_buf.at[pl.ds(at, n)] for at, n in ((0, ny), (ny, nx), (ny + nx, ny))
    )
    m1_start, m1_finish, m_all_of, _ = share(my_buf, m_s.at[3], m_s.at[0], *axes[1], source=ms_buf)
    m2_start, m2_finish, _, _ = share(mx_buf, m_s.at[3], m_s.at[1], *axes[0])
    m3_start, _, _, m3_wait = share(mz_buf, m_s.at[3], m_s.at[2], *axes[1])
    m_sent = mm_buf.at[pl.ds(0, 2 * (ny - 1) + nx - 1)]
    drains.append(lambda: m_all_of(m_sent).wait_send())

    zero = jnp.zeros((N, LANES), F32)
    with jax.named_scope("sten0"):
        t_v[...] = jnp.zeros_like(t_v)
        fext[:, 0:LANES] = zero
        fext[:, (R + 1) * LANES : (R + 2) * LANES] = zero
        columns = [zero]

        def finish_first(r, f, w):
            wf[:, row_at(r)] = w
            hi, low = put_pair(row_at(r), w, zero)
            put_rhs(row_at(r), hi[0:N], low[0:N])

        stencil(lambda r: 0.0, finish_first)
    with jax.named_scope("tuck0"):
        for r in range(R):
            columns[0] = tuck(columns[0], r, wf[:, row_at(r)])
    with jax.named_scope("gram"):
        high, low = halves(HI + K)
        first = (high + low)[:, 0:HI]
        g_v[...] = jnp.zeros_like(g_v)
        g_v[0, 0:K, 0 : HI + K] = (high + low)[0:K]
        g_v[1, 0:K, 0 : HI + K] = low[0:K]
        straight = g_v[0]
        flipped = g_v[1].T[HI : HI + K]
        is_low = lax.broadcasted_iota(jnp.int32, (mid, LANES), 1) < K
        full = jnp.where(
            is_low,
            pltpu.roll(straight[0:mid], LANES - HI, 1) + flipped[0:mid],
            pltpu.roll(straight[mid:K], K - HI, 1) + pltpu.roll(flipped[mid:K], K, 1),
        )
        for p in range(ny):
            ms_buf[p] = full[p * part : (p + 1) * part]

        def put_own(ref):
            ref[...] = ms_buf[iy]

        m1_start(put_own)

    with jax.named_scope("ewait0"):
        e0_wait()
    with jax.named_scope("lat0"):
        from_below, from_above, from_right, from_left = [edge_recv[e] for e in range(4)]
        gain = jnp.where(
            lax.rem(lane, 2) == 0, pltpu.roll(from_left, 1, 1), pltpu.roll(from_right, LANES - 1, 1)
        )
        column = columns[0]
        column = jnp.where(slots(zero.shape, 0), column + from_above, column)
        column = jnp.where(
            slots(zero.shape, R - 1), column + pltpu.roll(from_below, 2 * (R - 1), 1), column
        )
        ends = ((0, from_above), (R - 1, from_below))
        for r, extra in ends:
            w = wf[:, row_at(r)]
            put_pair(row_at(r), zero, w + 0.5 * extra)
            put_rhs(row_at(r), *split(extra))
            wf[:, row_at(r)] = w + extra
        put_pair(pl.ds(EXT, LANES), zero, column + 0.5 * gain)
        put_rhs(pl.ds(EXT, LANES), *split(gain))
        last = against(pl.ds(sites - LANES, 2 * LANES), HI)
        top = against(row_at(0), HI)
        value = turned(first + ((last[0] + last[1]) + (top[0] + top[1])) * scale)
        if direct:
            all_arrived()
        finish0 = reduction(0, value)
    with jax.named_scope("packw"):
        beside = sides(from_right, from_left)
        outer = (lane == 0) | (lane == LANES - 1)
        for r in range(R):
            wf[:, row_at(r)] = wf[:, row_at(r)] + jnp.where(outer, beside(r), 0.0)
        ew_send[0] = wf[:, row_at(0)] * rate_row(0, 0)
        ew_send[1] = wf[:, row_at(R - 1)] * rate_row(1, R - 1)
        ew_send[2] = (column + gain) * rate_side
    e0_drain()
    e2_start()

    with jax.named_scope("ewait1"):
        e1_wait()
    with jax.named_scope("esplit"):
        for e in range(4):
            at = pl.ds(EDGE + e * LANES, LANES)
            b = eb_recv[e]
            hi = b.astype(BF)
            x_v[HI : HI + K, at] = hi
            x_v[LO : LO + K, at] = (b - hi.astype(F32)).astype(BF)

    def forward(ref, value):
        ref[...] = value

    with jax.named_scope("m12"):
        m = m1_finish()
        m2_start(lambda ref: forward(ref, m))
    with jax.named_scope("ewait2"):
        e2_wait()
        for e in range(4):
            wf[:, pl.ds(EDGE + e * LANES, LANES)] = ew_recv[e]
    with jax.named_scope("red0"):
        total = finish0()

    def combine(lhs, at):
        both = jnp.dot(lhs, x_v[HI:LO, at], preferred_element_type=F32) + jnp.dot(
            lhs, x_v[LO : LO + Z, at], preferred_element_type=F32
        )
        return both[0:N] + both[N : 2 * N]

    wide8 = 8 * LANES
    pm = jnp.where(lane < K, total, 0.0)
    def project(lhs, at):
        both = jnp.dot(lhs, x_v[HI : HI + K, at], preferred_element_type=F32) + jnp.dot(
            lhs, x_v[LO : LO + K, at], preferred_element_type=F32
        )
        return both[0:N] + both[N : 2 * N]

    with jax.named_scope("new0"):
        lhs = split_rows(pm)[:, 0:K]
        at = pl.ds(EDGE, 4 * LANES)
        edge = wf[:, at] - project(lhs, at)
        fext[:, 0:LANES] = edge[:, LANES : 2 * LANES]
        fext[:, (R + 1) * LANES : (R + 2) * LANES] = edge[:, 0:LANES]
        for i in range(R // 8):
            at = pl.ds(i * wide8, wide8)
            fext[:, pl.ds(LANES + i * wide8, wide8)] = wf[:, at] - project(lhs, at)
    with jax.named_scope("lat1"):
        def finish_second(r, f, u):
            hi, low = put_pair(row_at(r), f, u)
            put_rhs(row_at(r), hi[N:HI], low[N:HI])

        with jax.named_scope("sten1"):
            stencil(
                sides(edge[:, 2 * LANES : 3 * LANES], edge[:, 3 * LANES : 4 * LANES]), finish_second
            )
        with jax.named_scope("prod1"):
            high, low = halves(HI)
            value = turned(high + low)
        m_own = m2_finish()
        m3_start(lambda ref: forward(ref, m_own))
        finish1 = reduction(1, value)

    with jax.named_scope("mxfin"):
        m3_wait()
        m = jnp.concatenate([mz_buf[p] for p in range(ny)], axis=0)
        gram = rows_full(
            jnp.concatenate(
                [
                    jnp.where(lax.broadcasted_iota(jnp.int32, (mid, LANES), 1) < K, m, 0.0),
                    jnp.where(
                        lax.broadcasted_iota(jnp.int32, (mid, LANES), 1) < K,
                        pltpu.roll(m, LANES - K, 1),
                        0.0,
                    ),
                ],
                axis=0,
            )
        )
    G0 = Z

    def times(parts, stacked):
        pair = jnp.concatenate(parts, axis=0).astype(BF)
        both = jnp.dot(
            jnp.concatenate([pair, pair], axis=1), stacked, preferred_element_type=F32
        )
        return both[0:N] + both[N : 2 * N]

    def gram_of(value, parts):
        both = sum(
            dot_nt(split_rows(value), rows_full(p, G0).astype(BF), lax.Precision.DEFAULT)
            for p in parts
        )
        return both[0:N] + both[N : 2 * N]

    with jax.named_scope("fac0"):
        own = (
            pltpu.roll(total, G0 - K, 1)
            + pltpu.roll(total, G0 - KN, 1)
            + pltpu.roll(rows_full(total).T[KN:Z], G0, 1)
        )
        pm_parts = split(pm)
        rest = 2.0 * pm - times(pm_parts, jnp.concatenate(split(gram), axis=0).astype(BF))
        g = own - gram_of(rest, pm_parts)
        g = jnp.where((lane >= G0) & (lane < G0 + N), g, 0.0)
        a = jnp.where(lane < K, rest - pm, jnp.where(lane == sub + K, 1.0, g))
        a = eliminate(a, G0, N)
        at_t = rows_full(a).T
        inv = pltpu.roll(a, LANES - K, 1)
        inv = jnp.where(lane < N, inv, 0.0)
        low1 = at_t[G0 : G0 + N]
        coefs[0] = pm + jnp.where((lane >= K) & (lane < KN), pltpu.roll(low1, K, 1), 0.0)
        row = lax.broadcasted_iota(jnp.int32, (LANES, LANES), 0)
        col = lax.broadcasted_iota(jnp.int32, (LANES, LANES), 1)
        inner = jnp.where((row < KN), at_t, 0.0)
        flow = dot_nn(inner, rows_full(jnp.where(lane < KN, a, 0.0)))
        in_b = (row < K) & (col < K)
        in_w = (row >= K) & (row < KN) & (col >= K) & (col < KN)
        eye = jnp.where(row == col, 1.0, 0.0)
        kmat = jnp.where(in_b, 2.0 * eye - gram, jnp.where(in_w, flow, -flow))
        dmat = jnp.where(in_b, eye, jnp.where(in_w, flow, 0.0))
        tmat = jnp.where((row >= K) & (row < KN) & (col < N), at_t, 0.0)
        for i, mat in enumerate((kmat, dmat, tmat)):
            hi, low = split(mat)
            m_v[0:LANES, i * LANES : (i + 1) * LANES] = hi.astype(BF)
            m_v[LANES : 2 * LANES, i * LANES : (i + 1) * LANES] = low.astype(BF)
    with jax.named_scope("q1"):
        lhs = split_rows(inv)[:, 0 : 2 * N]
        for i in range(R // 8):
            at = pl.ds(i * wide8, wide8)
            both = jnp.dot(lhs, x_v[HI + K : LO, at], preferred_element_type=F32) + jnp.dot(
                lhs, x_v[LO + K : LO + Z, at], preferred_element_type=F32
            )
            q = both[0:N] + both[N : 2 * N]
            for u in range(8):
                first_v[pl.ds(i * 8 + u, N, stride=RP), :] = q[:, u * LANES : (u + 1) * LANES]

    with jax.named_scope("red1"):
        total = finish1()
    with jax.named_scope("fac1"):
        ep = jnp.where(lane < KN, total, 0.0)
        own = pltpu.roll(total, G0 - KN, 1)
        ep_parts = split(ep)
        both = times(ep_parts, m_v[:, 0 : 2 * LANES])
        ek, ed = both[:, 0:LANES], both[:, LANES : 2 * LANES]
        g = own - gram_of(ek, ep_parts)
        g = jnp.where((lane >= G0) & (lane < G0 + N), g, 0.0)
        a = jnp.where(lane < KN, ed, jnp.where(lane == sub + KN, 1.0, g))
        a = eliminate(a, G0, N)
        lhs = split_rows(jnp.where(lane < KN, -a, a))[:, 0:Z]
    with jax.named_scope("new1"):
        for i in range(R // 8):
            q = combine(lhs, pl.ds(i * wide8, wide8))
            for u in range(8):
                second_v[pl.ds(i * 8 + u, N, stride=RP), :] = q[:, u * LANES : (u + 1) * LANES]
    with jax.named_scope("coef1"):
        low2 = rows_full(a).T[G0 : G0 + N]
        es = times(ep_parts, m_v[:, 2 * LANES : 3 * LANES])
        stack = jnp.where(lane < K, ep, jnp.where(lane < KN, pltpu.roll(es, K, 1), 0.0))
        stack = jnp.where((lane >= KN) & (lane < Z), pltpu.roll(low2, KN, 1), stack)
        coefs[1] = dot_nn(inv, rows_full(stack))
    with jax.named_scope("drain"):
        for drain in drains:
            drain()


def deliver(
    R, first_v, second_v, coefs, first_hbm, second_hbm, one_hbm, two_hbm, coef_one, coef_two, sem
):
    copies = [
        pltpu.make_async_copy(first_v.at[:, pl.ds(0, R)], first_hbm, sem.at[0]),
        pltpu.make_async_copy(second_v.at[:, pl.ds(0, R)], second_hbm, sem.at[1]),
        pltpu.make_async_copy(coef_one, one_hbm, sem.at[2]),
        pltpu.make_async_copy(coef_two, two_hbm, sem.at[3]),
    ]
    for copy in copies[:2]:
        copy.start()
    coef_one[...] = coefs[0, :, 0 : coef_one.shape[1]]
    coef_two[...] = coefs[1, :, 0 : coef_two.shape[1]]
    for copy in copies[2:]:
        copy.start()
    for copy in copies:
        copy.wait()


def local(nx, ny, basis, panel, rate_codes):
    N, R, C = panel.shape
    K = basis.shape[0]
    assert C == LANES and 2 * K == LANES and N == 8
    vmem = pl.BlockSpec(memory_space=pltpu.VMEM)
    hbm = pl.BlockSpec(memory_space=pl.ANY)
    dma = pltpu.SemaphoreType.DMA
    sites = R * LANES
    group = nx * ny if nx * ny <= DIRECT else nx
    Z = K + 2 * N
    first, second, coefs = pl.pallas_call(
        functools.partial(kernel, nx, ny, K, N, R),
        out_shape=(
            pltpu.VMEM((N * (R + PAD), C), F32),
            pltpu.VMEM((N * (R + PAD), C), F32),
            pltpu.VMEM((2, N, C), F32),
        ),
        in_specs=[pl.BlockSpec(memory_space=pltpu.HBM)] * 3,
        out_specs=(vmem, vmem, vmem),
        scratch_shapes=[
            pltpu.VMEM((K, R + PAD, LANES), F32),
            pltpu.VMEM((N, R + PAD, LANES), F32),
            pltpu.VMEM((4 * R, LANES), jnp.int32),
            pltpu.VMEM((5 * (R + 16), LANES), F32),
            pltpu.VMEM((N, (R + 2) * LANES), F32),
            pltpu.VMEM((N, sites + 5 * LANES), F32),
            pltpu.VMEM((2 * N + 2 * Z, sites + 5 * LANES), BF),
            pltpu.VMEM((2 * LANES, 3 * LANES), BF),
            pltpu.VMEM((LANES, LANES), F32),
            pltpu.VMEM((2, LANES, LANES), F32),
            pltpu.VMEM((3, N, LANES), F32),
            pltpu.VMEM((4, N, LANES), F32),
            pltpu.VMEM((3, K, LANES), F32),
            pltpu.VMEM((4, K, LANES), F32),
            pltpu.VMEM((3, N, LANES), F32),
            pltpu.VMEM((4, N, LANES), F32),
            pltpu.VMEM((ny, K // 2 // ny, LANES), F32),
            pltpu.VMEM((2 * ny + nx, K // 2 // ny, LANES), F32),
            pltpu.VMEM((2, ny, N // 2 + 1, LANES), F32),
            pltpu.VMEM((2, group, N // 2 + 1, LANES), F32),
            dma((2 + CHUNKS,)),
            dma((4,)),
            dma((4,)),
            dma((4,)),
            dma((4,)),
            dma((4,)),
            pltpu.SemaphoreType.REGULAR((2,)),
            dma((4,)),
            dma((1 if nx * ny <= DIRECT and nx % BUDDY == 0 else 3,)),
            dma((3,)),
        ],
        compiler_params=pltpu.CompilerParams(
            collective_id=0, has_side_effects=True
        ),
    )(basis, panel, rate_codes.reshape(rate_codes.shape[0] * R, C))
    first, second, coef_one, coef_two = pl.pallas_call(
        functools.partial(deliver, R),
        out_shape=(
            jax.ShapeDtypeStruct((N, R, C), F32),
            jax.ShapeDtypeStruct((N, R, C), F32),
            jax.ShapeDtypeStruct((N, K + N), F32),
            jax.ShapeDtypeStruct((N, K + 2 * N), F32),
        ),
        in_specs=[vmem] * 3,
        out_specs=(hbm, hbm, hbm, hbm),
        scratch_shapes=[
            pltpu.VMEM((N, K + N), F32),
            pltpu.VMEM((N, K + 2 * N), F32),
            dma((4,)),
        ],
        compiler_params=pltpu.CompilerParams(vmem_limit_bytes=4 * 2**20),
    )(first.reshape(N, R + PAD, C), second.reshape(N, R + PAD, C), coefs)
    return first, second, coef_one.T, coef_two.T


def solution(mesh):
    spec = P(None, "gx", "gy")
    return jax.shard_map(
        functools.partial(local, mesh.shape["gx"], mesh.shape["gy"]),
        mesh=mesh,
        in_specs=(spec, spec, spec),
        out_specs=(spec, spec, P(), P()),
        check_vma=False,
    )
```

```python
import functools

import jax
import jax.numpy as jnp
from jax import lax
from jax.experimental import pallas as pl
from jax.experimental.pallas import tpu as pltpu
from jax.sharding import PartitionSpec as P

HIGH = lax.Precision.HIGHEST
MESH = pl.DeviceIdType.MESH
F32 = jnp.float32
BF = jnp.bfloat16
LANES = 128
CHUNKS = 4
DIRECT = 64
BUDDY = 2
PAD = 8


def dot_nn(a, b):
    return jnp.dot(a, b, precision=HIGH, preferred_element_type=F32)


def dot_nt(a, b, precision=HIGH):
    return lax.dot_general(
        a, b, (((1,), (1,)), ((), ())), precision=precision, preferred_element_type=F32
    )


def rows_full(v, at=0):
    parts = [v, jnp.zeros((LANES - at - v.shape[0], LANES), F32)]
    if at:
        parts.insert(0, jnp.zeros((at, LANES), F32))
    return jnp.concatenate(parts, axis=0)


def split(v):
    hi = v.astype(BF).astype(F32)
    return hi, v - hi


def split_rows(v):
    return jnp.concatenate(split(v), axis=0).astype(BF)


def eliminate(a, g0, n):
    sub = lax.broadcasted_iota(jnp.int32, a.shape, 0)
    cols = [jnp.broadcast_to(a[:, g0 + j : g0 + j + 1], a.shape) for j in range(n)]
    pivots = jnp.ones(a.shape, F32)
    for k in range(n):
        pivot = jnp.broadcast_to(cols[k][k : k + 1, :], a.shape)
        pivots = jnp.where(sub == k, pivot, pivots)
        if k == n - 1:
            break
        factor = jnp.where(sub > k, cols[k] * (1.0 / pivot), 0.0)
        for j in range(k + 1, n):
            cols[j] = cols[j] - factor * cols[j][k : k + 1, :]
        a = a - factor * a[k : k + 1, :]
    return a * (1.0 / jnp.sqrt(pivots))


def kernel(
    nx, ny, K, N, R,
    basis_hbm, panel_hbm, rate_hbm,
    first_v, second_v, coefs,
    basis_v, panel_v, rate_v, rates, fext, wf, x_v, m_v, t_v, g_v,
    edge_send, edge_recv, eb_send, eb_recv, ew_send, ew_recv, ms_buf, mm_buf, py_buf, px_buf,
    in_sem, edge_ssem, edge_rsem, eb_ssem, eb_rsem, ew_rsem, ready,
    m_s, py_s, px_s,
):
    ix, iy = lax.axis_index("gx"), lax.axis_index("gy")
    sites = R * LANES
    scale = 1.0 / (sites * nx * ny)
    lane = lax.broadcasted_iota(jnp.int32, (N, LANES), 1)
    sub = lax.broadcasted_iota(jnp.int32, (N, LANES), 0)
    KN = K + N
    Z = K + 2 * N
    HI = 2 * N
    LO = HI + Z
    EXT = sites
    EDGE = sites + LANES
    RP = R + PAD
    T = R + 16

    basis_rows = basis_v.reshape(K * RP, LANES)
    panel_rows = panel_v.reshape(N * RP, LANES)

    axes = (("gx", ix, nx), ("gy", iy, ny))
    everyone = ("all", ix * ny + iy, nx * ny)
    direct = nx * ny <= DIRECT and nx % BUDDY == 0

    def peer_of(axis, me, n, d):
        other = lax.rem(me + d, n)
        if axis == "all":
            return other, {"gx": lax.div(other, ny), "gy": lax.rem(other, ny)}
        return other, {axis: other}

    with jax.named_scope("dma0"):
        step = K // CHUNKS
        panel_in = pltpu.make_async_copy(panel_hbm, panel_v.at[:, pl.ds(0, R)], in_sem.at[0])
        rate_in = pltpu.make_async_copy(rate_hbm, rate_v, in_sem.at[1])
        panel_in.start()
        rate_in.start()

    barrier = pltpu.get_barrier_semaphore()

    def greet(device):
        pl.semaphore_signal(barrier, inc=1, device_id=device, device_id_type=MESH)

    if direct:
        planes = nx // BUDDY
        plane = lax.div(ix, BUDDY)
        home = plane * BUDDY
        group = BUDDY * ny
        seat = (ix - home) * ny + iy
        mates = []
        for d in range(1, group):
            other = lax.rem(seat + d, group)
            mates.append({"gx": home + lax.div(other, ny), "gy": lax.rem(other, ny)})
        outer = [
            ((ix == home) & (ix > 0), ix - 1),
            ((ix == home + BUDDY - 1) & (ix < nx - 1), ix + 1),
        ]
        if planes % 2:
            others = [lax.rem(plane + d, planes) for d in range(1, planes)]
        else:
            others = [lax.rem(planes + c - plane, planes) for c in range(planes - 1, 0, -2)]
            others += [lax.rem(plane + d, planes) for d in range(2, planes, 2)]
        far_first = []
        for other in others:
            for k in range(group):
                to = lax.rem(seat + k + group // 2, group)
                far_first.append(other * group + to)
        far_first += [plane * group + lax.rem(seat + d, group) for d in range(1, group)]
        row_mates = [{"gy": lax.rem(iy + d, ny)} for d in range(1, ny)]
        column_mates = [{"gx": home + lax.rem(ix - home + d, BUDDY)} for d in range(1, BUDDY)]
        greeted = ny - 1 + BUDDY - 1 + BUDDY * plane
        for there, device in outer:
            greeted = greeted + jnp.where(there, 1, 0)

            @pl.when(there)
            def _(device=device):
                greet({"gx": device})

        for device in column_mates + row_mates:
            greet(device)
        for d in range(1, planes):
            @pl.when(plane + d < planes)
            def _(d=d):
                for b in range(BUDDY):
                    greet({"gx": home + d * BUDDY + b})

    else:
        greeted = 0
        for axis, me, n in axes:
            for d in range(1, n):
                greet(peer_of(axis, me, n, d)[1])
                greeted += 1

    basis_in = []
    for c in range(CHUNKS):
        part = pl.ds(c * step, step)
        basis_in.append(
            pltpu.make_async_copy(
                basis_hbm.at[part], basis_v.at[part, pl.ds(0, R)], in_sem.at[2 + c]
            )
        )
        basis_in[-1].start()
    def row_at(r):
        return pl.ds(r * LANES, LANES)

    def rate_row(d, r):
        return rates[pl.ds(d * T + 8 + r, 1), :]

    with jax.named_scope("inwait"):
        panel_in.wait()
        rate_in.wait()
    routes = (
        ("gx", ix - 1, ix > 0, ix < nx - 1),
        ("gx", ix + 1, ix < nx - 1, ix > 0),
        ("gy", iy - 1, iy > 0, iy < ny - 1),
        ("gy", iy + 1, iy < ny - 1, iy > 0),
    )

    def edges(send, recv, ssem, rsem):
        def copy(e):
            return pltpu.make_async_remote_copy(
                src_ref=send.at[min(e, 2)],
                dst_ref=recv.at[e],
                send_sem=ssem.at[e],
                recv_sem=rsem.at[e],
                device_id={routes[e][0]: routes[e][1]},
                device_id_type=MESH,
            )

        def start(which=range(4)):
            for e in which:
                @pl.when(routes[e][2])
                def _(e=e):
                    copy(e).start()

                @pl.when(jnp.logical_not(routes[e][3]))
                def _(e=e):
                    recv[e] = jnp.zeros(recv.shape[1:], F32)

        def wait():
            for e in range(4):
                @pl.when(routes[e][3])
                def _(e=e):
                    copy(e).wait_recv()

        def drain():
            for e in range(4):
                @pl.when(routes[e][2])
                def _(e=e):
                    copy(e).wait_send()

        return start, wait, drain

    def share(buf, send_sem, recv_sem, axis, me, n, source=None):
        def copy(src, dst, device):
            by_mesh = isinstance(device, dict)
            return pltpu.make_async_remote_copy(
                src_ref=src,
                dst_ref=dst,
                send_sem=send_sem,
                recv_sem=recv_sem,
                device_id=device,
                device_id_type=MESH if by_mesh else pl.DeviceIdType.LOGICAL,
            )

        def start(store):
            store(buf.at[me])
            if axis == "all":
                for device in far_first:
                    copy(buf.at[me], buf.at[me], device).start()
                return
            for d in range(1, n):
                other, device = peer_of(axis, me, n, d)
                copy(buf.at[me] if source is None else source.at[other], buf.at[me], device).start()

        def all_of(ref):
            return copy(ref, ref, peer_of(axis, me, n, 1)[1])

        def wait():
            all_of(buf.at[pl.ds(0, n - 1)]).wait_recv()

        def finish():
            wait()
            parts = [buf[k] for k in range(n)]
            while len(parts) > 1:
                parts = [
                    parts[i] + parts[i + 1] if i + 1 < len(parts) else parts[i]
                    for i in range(0, len(parts), 2)
                ]
            return parts[0]

        return start, finish, all_of, wait

    half = N // 2

    def pack(v):
        turned = pltpu.roll(v, K, 1)
        tail = pltpu.roll(v, 0, 1, stride=2 * N, stride_axis=0)
        mine = lax.div(lane, 2 * N) == lax.rem(sub + K // (2 * N), N)
        tail = jnp.sum(jnp.where(mine, tail, 0.0), axis=0, keepdims=True)
        low = lax.broadcasted_iota(jnp.int32, (half, LANES), 1) < K
        return jnp.where(low, v[0:half], turned[half:N]), tail

    def unpack(t):
        body = jnp.concatenate([t[0:half], pltpu.roll(t[0:half], K, 1)], axis=0)
        spread = jnp.broadcast_to(t[half : half + 1], (N, LANES))
        tail = spread
        for j in range(1, N):
            tail = jnp.where(sub == j, pltpu.roll(spread, LANES - 2 * N * j, 1), tail)
        return jnp.where(lane < K, body, jnp.where(lane < Z, tail, 0.0))

    drains = []

    def reduction(s, value):
        xgroup = everyone if direct else axes[0]
        xstart, xfinish, all_of, _ = share(px_buf.at[s], px_s.at[2], px_s.at[s], *xgroup)
        if s:
            both = px_buf.at[:, pl.ds(0, xgroup[2] - 1)]
            drains.append(lambda: all_of(both).wait_send())

        def put(parts):
            def store(ref):
                ref[0:half] = parts[0]
                ref[half : half + 1] = parts[1]

            return store

        parts = pack(value)
        if direct:
            xstart(put(parts))
            return lambda: unpack(xfinish())
        ystart, yfinish, y_all_of, _ = share(py_buf.at[s], py_s.at[2], py_s.at[s], *axes[1])
        if s:
            y_both = py_buf.at[:, pl.ds(0, ny - 1)]
            drains.append(lambda: y_all_of(y_both).wait_send())
        ystart(put(parts))

        def finish():
            t = yfinish()
            xstart(put((t[0:half], t[half : half + 1])))
            return unpack(xfinish())

        return finish

    e0_start, e0_wait, e0_drain = edges(edge_send, edge_recv, edge_ssem, edge_rsem)
    e1_start, e1_wait, e1_drain = edges(eb_send, eb_recv, eb_ssem, eb_rsem)
    e2_start, e2_wait, e2_drain = edges(ew_send, ew_recv, edge_ssem, ew_rsem)
    drains += [e1_drain, e2_drain]

    def slots(shape, r):
        at = lax.broadcasted_iota(jnp.int32, shape, len(shape) - 1)
        return (at == 2 * r) | (at == (2 * r - 1) % LANES)

    def tuck(packed, r, f):
        return jnp.where(slots(f.shape, r), pltpu.roll(f, 2 * r, len(f.shape) - 1), packed)

    def end_row(d, r):
        return panel_rows[pl.ds(r, N, stride=RP), :] * (
            rate_v[d * R + r : d * R + r + 1, :].astype(F32) * 0.125
        )

    edge_send[0] = end_row(0, 0)
    edge_send[1] = end_row(1, R - 1)
    with jax.named_scope("barrier"):
        pl.semaphore_wait(barrier, greeted)
    e0_start((0, 1))
    for d in range(4):
        rates[d * T : d * T + 8, :] = jnp.ones((8, LANES), F32)
        rates[d * T + 8 + R : (d + 1) * T, :] = jnp.ones((8, LANES), F32)
        rates[d * T + 8 : d * T + 8 + R, :] = (
            rate_v[d * R : (d + 1) * R, :].astype(F32) * 0.125
        )
    rates[4 * T + 8 : 4 * T + 8 + R, :] = (
        rates[8 : 8 + R, :]
        + rates[T + 8 : T + 8 + R, :]
        + rates[2 * T + 8 : 2 * T + 8 + R, :]
        + rates[3 * T + 8 : 3 * T + 8 + R, :]
    )

    with jax.named_scope("packp"):
        lane_of = lax.broadcasted_iota(jnp.int32, (R, LANES), 1)
        sides = jnp.where(lane_of == 0, rates[2 * T + 8 : 2 * T + 8 + R, :], rates[3 * T + 8 : 3 * T + 8 + R, :])
        rate_side = jnp.zeros((N, LANES), F32)
        for i in range(R // 8):
            turned = pltpu.roll(sides[i * 8 : i * 8 + 8], 16 * i, 1, stride=2, stride_axis=0)
            mine = (lane == 2 * (sub + 8 * i)) | (lane == lax.rem(2 * (sub + 8 * i) + LANES - 1, LANES))
            rate_side = rate_side + jnp.where(mine, turned, 0.0)
        rate_side = jnp.sum(rate_side, axis=0, keepdims=True)
    packed = jnp.zeros((N, LANES), F32)
    for r in range(R):
        f = panel_rows[pl.ds(r, N, stride=RP), :]
        fext[:, row_at(r + 1)] = f
        packed = tuck(packed, r, f)
    edge_send[2] = packed * rate_side
    e0_start((2, 3))
    if direct:
        for device in row_mates:
            pl.semaphore_signal(ready.at[0], inc=1, device_id=device, device_id_type=MESH)
        for d in range(1, planes):
            @pl.when(plane >= d)
            def _(d=d):
                for b in range(BUDDY):
                    device = {"gx": home - d * BUDDY + b}
                    pl.semaphore_signal(ready.at[1], inc=1, device_id=device, device_id_type=MESH)

    def all_arrived():
        pl.semaphore_wait(ready.at[0], ny - 1)

        @pl.when(plane < planes - 1)
        def _():
            pl.semaphore_wait(ready.at[1], BUDDY * (planes - 1 - plane))

    with jax.named_scope("split"):
        for c in range(CHUNKS):
            basis_in[c].wait()
            mine = slice(c * step, (c + 1) * step)
            above = slice(HI + c * step, HI + (c + 1) * step)
            below = slice(LO + c * step, LO + (c + 1) * step)

            packed = jnp.zeros((step, LANES), F32)
            for r in range(R):
                b = basis_rows[pl.ds(c * step * RP + r, step, stride=RP), :]
                hi = b.astype(BF)
                x_v[above, row_at(r)] = hi
                x_v[below, row_at(r)] = (b - hi.astype(F32)).astype(BF)
                packed = tuck(packed, r, b)
            hi = packed.astype(BF)
            x_v[above, pl.ds(EXT, LANES)] = hi
            x_v[below, pl.ds(EXT, LANES)] = (packed - hi.astype(F32)).astype(BF)
            eb_send[2, mine] = packed * rate_side
            eb_send[0, mine] = basis_rows[pl.ds(c * step * RP, step, stride=RP), :] * rate_row(0, 0)
            eb_send[1, mine] = (
                basis_rows[pl.ds(c * step * RP + R - 1, step, stride=RP), :] * rate_row(1, R - 1)
            )

    e1_start()

    def sides(from_right, from_left):
        side = jnp.where(lax.rem(lane, 2) == 1, from_left, pltpu.roll(from_right, LANES - 2, 1))
        return lambda r: pltpu.roll(side, (LANES + 1 - 2 * r) % LANES, 1)

    def stencil(beside, finish):
        for r in range(R):
            f = fext[:, row_at(r + 1)]
            above = fext[:, row_at(r)] * rate_row(1, r - 1)
            below = fext[:, row_at(r + 2)] * rate_row(0, r + 1)
            west = pltpu.roll(f * rate_row(3, r), 1, 1)
            east = pltpu.roll(f * rate_row(2, r), LANES - 1, 1)
            other = beside(r)
            west = jnp.where(lane == 0, other, west)
            east = jnp.where(lane == LANES - 1, other, east)
            finish(r, f, above + below + west + east - rate_row(4, r) * f)

    def put_pair(at, upper, lower):
        both = jnp.concatenate([upper, lower], axis=0)
        hi = both.astype(BF)
        low = both - hi.astype(F32)
        x_v[HI + K : LO, at] = hi
        x_v[LO + K : LO + Z, at] = low.astype(BF)
        return hi.astype(F32), low

    def put_rhs(at, hi, low):
        x_v[0:HI, at] = jnp.concatenate([hi, low], axis=0).astype(BF)

    def against(at, width):
        return [
            dot_nt(x_v[top : top + Z, at], x_v[0:width, at], lax.Precision.DEFAULT)
            for top in (HI, LO)
        ]

    def halves(width):
        parts = [against(pl.ds(h * (sites // 2), sites // 2), width) for h in range(2)]
        return [parts[0][i] * scale + parts[1][i] * scale for i in range(2)]

    def turned(total):
        t_v[0:Z, 0:HI] = total
        value = t_v[...].T
        return value[0:N] + value[N:HI]

    mid = K // 2
    part = mid // ny
    my_buf, mx_buf, mz_buf = (
        mm_buf.at[pl.ds(at, n)] for at, n in ((0, ny), (ny, nx), (ny + nx, ny))
    )
    m1_start, m1_finish, m_all_of, _ = share(my_buf, m_s.at[3], m_s.at[0], *axes[1], source=ms_buf)
    m2_start, m2_finish, _, _ = share(mx_buf, m_s.at[3], m_s.at[1], *axes[0])
    m3_start, _, _, m3_wait = share(mz_buf, m_s.at[3], m_s.at[2], *axes[1])
    m_sent = mm_buf.at[pl.ds(0, 2 * (ny - 1) + nx - 1)]
    drains.append(lambda: m_all_of(m_sent).wait_send())

    zero = jnp.zeros((N, LANES), F32)
    with jax.named_scope("sten0"):
        t_v[...] = jnp.zeros_like(t_v)
        fext[:, 0:LANES] = zero
        fext[:, (R + 1) * LANES : (R + 2) * LANES] = zero
        columns = [zero]

        def finish_first(r, f, w):
            wf[:, row_at(r)] = w
            hi, low = put_pair(row_at(r), w, zero)
            put_rhs(row_at(r), hi[0:N], low[0:N])

        stencil(lambda r: 0.0, finish_first)
    with jax.named_scope("tuck0"):
        for r in range(R):
            columns[0] = tuck(columns[0], r, wf[:, row_at(r)])
    with jax.named_scope("gram"):
        high, low = halves(HI + K)
        first = (high + low)[:, 0:HI]
        g_v[...] = jnp.zeros_like(g_v)
        g_v[0, 0:K, 0 : HI + K] = (high + low)[0:K]
        g_v[1, 0:K, 0 : HI + K] = low[0:K]
        straight = g_v[0]
        flipped = g_v[1].T[HI : HI + K]
        is_low = lax.broadcasted_iota(jnp.int32, (mid, LANES), 1) < K
        full = jnp.where(
            is_low,
            pltpu.roll(straight[0:mid], LANES - HI, 1) + flipped[0:mid],
            pltpu.roll(straight[mid:K], K - HI, 1) + pltpu.roll(flipped[mid:K], K, 1),
        )
        for p in range(ny):
            ms_buf[p] = full[p * part : (p + 1) * part]

        def put_own(ref):
            ref[...] = ms_buf[iy]

        m1_start(put_own)

    with jax.named_scope("ewait0"):
        e0_wait()
    with jax.named_scope("lat0"):
        from_below, from_above, from_right, from_left = [edge_recv[e] for e in range(4)]
        gain = jnp.where(
            lax.rem(lane, 2) == 0, pltpu.roll(from_left, 1, 1), pltpu.roll(from_right, LANES - 1, 1)
        )
        column = columns[0]
        column = jnp.where(slots(zero.shape, 0), column + from_above, column)
        column = jnp.where(
            slots(zero.shape, R - 1), column + pltpu.roll(from_below, 2 * (R - 1), 1), column
        )
        ends = ((0, from_above), (R - 1, from_below))
        for r, extra in ends:
            w = wf[:, row_at(r)]
            put_pair(row_at(r), zero, w + 0.5 * extra)
            put_rhs(row_at(r), *split(extra))
            wf[:, row_at(r)] = w + extra
        put_pair(pl.ds(EXT, LANES), zero, column + 0.5 * gain)
        put_rhs(pl.ds(EXT, LANES), *split(gain))
        last = against(pl.ds(sites - LANES, 2 * LANES), HI)
        top = against(row_at(0), HI)
        value = turned(first + ((last[0] + last[1]) + (top[0] + top[1])) * scale)
        if direct:
            all_arrived()
        finish0 = reduction(0, value)
    with jax.named_scope("packw"):
        beside = sides(from_right, from_left)
        outer = (lane == 0) | (lane == LANES - 1)
        for r in range(R):
            wf[:, row_at(r)] = wf[:, row_at(r)] + jnp.where(outer, beside(r), 0.0)
        ew_send[0] = wf[:, row_at(0)] * rate_row(0, 0)
        ew_send[1] = wf[:, row_at(R - 1)] * rate_row(1, R - 1)
        ew_send[2] = (column + gain) * rate_side
    e0_drain()
    e2_start()

    with jax.named_scope("ewait1"):
        e1_wait()
    with jax.named_scope("esplit"):
        for e in range(4):
            at = pl.ds(EDGE + e * LANES, LANES)
            b = eb_recv[e]
            hi = b.astype(BF)
            x_v[HI : HI + K, at] = hi
            x_v[LO : LO + K, at] = (b - hi.astype(F32)).astype(BF)

    def forward(ref, value):
        ref[...] = value

    with jax.named_scope("m12"):
        m = m1_finish()
        m2_start(lambda ref: forward(ref, m))
    with jax.named_scope("ewait2"):
        e2_wait()
        for e in range(4):
            wf[:, pl.ds(EDGE + e * LANES, LANES)] = ew_recv[e]
    with jax.named_scope("red0"):
        total = finish0()

    def combine(lhs, at):
        both = jnp.dot(lhs, x_v[HI:LO, at], preferred_element_type=F32) + jnp.dot(
            lhs, x_v[LO : LO + Z, at], preferred_element_type=F32
        )
        return both[0:N] + both[N : 2 * N]

    wide8 = 8 * LANES
    pm = jnp.where(lane < K, total, 0.0)
    def project(lhs, at):
        both = jnp.dot(lhs, x_v[HI : HI + K, at], preferred_element_type=F32) + jnp.dot(
            lhs, x_v[LO : LO + K, at], preferred_element_type=F32
        )
        return both[0:N] + both[N : 2 * N]

    with jax.named_scope("new0"):
        lhs = split_rows(pm)[:, 0:K]
        at = pl.ds(EDGE, 4 * LANES)
        edge = wf[:, at] - project(lhs, at)
        fext[:, 0:LANES] = edge[:, LANES : 2 * LANES]
        fext[:, (R + 1) * LANES : (R + 2) * LANES] = edge[:, 0:LANES]
        for i in range(R // 8):
            at = pl.ds(i * wide8, wide8)
            fext[:, pl.ds(LANES + i * wide8, wide8)] = wf[:, at] - project(lhs, at)
    with jax.named_scope("lat1"):
        def finish_second(r, f, u):
            hi, low = put_pair(row_at(r), f, u)
            put_rhs(row_at(r), hi[N:HI], low[N:HI])

        with jax.named_scope("sten1"):
            stencil(
                sides(edge[:, 2 * LANES : 3 * LANES], edge[:, 3 * LANES : 4 * LANES]), finish_second
            )
        with jax.named_scope("prod1"):
            high, low = halves(HI)
            value = turned(high + low)
        m_own = m2_finish()
        m3_start(lambda ref: forward(ref, m_own))
        finish1 = reduction(1, value)

    with jax.named_scope("mxfin"):
        m3_wait()
        m = jnp.concatenate([mz_buf[p] for p in range(ny)], axis=0)
        gram = rows_full(
            jnp.concatenate(
                [
                    jnp.where(lax.broadcasted_iota(jnp.int32, (mid, LANES), 1) < K, m, 0.0),
                    jnp.where(
                        lax.broadcasted_iota(jnp.int32, (mid, LANES), 1) < K,
                        pltpu.roll(m, LANES - K, 1),
                        0.0,
                    ),
                ],
                axis=0,
            )
        )
    G0 = Z

    def times(parts, stacked):
        pair = jnp.concatenate(parts, axis=0).astype(BF)
        both = jnp.dot(
            jnp.concatenate([pair, pair], axis=1), stacked, preferred_element_type=F32
        )
        return both[0:N] + both[N : 2 * N]

    def gram_of(value, parts):
        both = sum(
            dot_nt(split_rows(value), rows_full(p, G0).astype(BF), lax.Precision.DEFAULT)
            for p in parts
        )
        return both[0:N] + both[N : 2 * N]

    with jax.named_scope("fac0"):
        own = (
            pltpu.roll(total, G0 - K, 1)
            + pltpu.roll(total, G0 - KN, 1)
            + pltpu.roll(rows_full(total).T[KN:Z], G0, 1)
        )
        pm_parts = split(pm)
        rest = 2.0 * pm - times(pm_parts, jnp.concatenate(split(gram), axis=0).astype(BF))
        g = own - gram_of(rest, pm_parts)
        g = jnp.where((lane >= G0) & (lane < G0 + N), g, 0.0)
        a = jnp.where(lane < K, rest - pm, jnp.where(lane == sub + K, 1.0, g))
        a = eliminate(a, G0, N)
        at_t = rows_full(a).T
        inv = pltpu.roll(a, LANES - K, 1)
        inv = jnp.where(lane < N, inv, 0.0)
        low1 = at_t[G0 : G0 + N]
        coefs[0] = pm + jnp.where((lane >= K) & (lane < KN), pltpu.roll(low1, K, 1), 0.0)
        row = lax.broadcasted_iota(jnp.int32, (LANES, LANES), 0)
        col = lax.broadcasted_iota(jnp.int32, (LANES, LANES), 1)
        inner = jnp.where((row < KN), at_t, 0.0)
        flow = dot_nn(inner, rows_full(jnp.where(lane < KN, a, 0.0)))
        in_b = (row < K) & (col < K)
        in_w = (row >= K) & (row < KN) & (col >= K) & (col < KN)
        eye = jnp.where(row == col, 1.0, 0.0)
        kmat = jnp.where(in_b, 2.0 * eye - gram, jnp.where(in_w, flow, -flow))
        dmat = jnp.where(in_b, eye, jnp.where(in_w, flow, 0.0))
        tmat = jnp.where((row >= K) & (row < KN) & (col < N), at_t, 0.0)
        for i, mat in enumerate((kmat, dmat, tmat)):
            hi, low = split(mat)
            m_v[0:LANES, i * LANES : (i + 1) * LANES] = hi.astype(BF)
            m_v[LANES : 2 * LANES, i * LANES : (i + 1) * LANES] = low.astype(BF)
    with jax.named_scope("q1"):
        lhs = split_rows(inv)[:, 0 : 2 * N]
        for i in range(R // 8):
            at = pl.ds(i * wide8, wide8)
            both = jnp.dot(lhs, x_v[HI + K : LO, at], preferred_element_type=F32) + jnp.dot(
                lhs, x_v[LO + K : LO + Z, at], preferred_element_type=F32
            )
            q = both[0:N] + both[N : 2 * N]
            for u in range(8):
                first_v[pl.ds(i * 8 + u, N, stride=RP), :] = q[:, u * LANES : (u + 1) * LANES]

    with jax.named_scope("red1"):
        total = finish1()
    with jax.named_scope("fac1"):
        ep = jnp.where(lane < KN, total, 0.0)
        own = pltpu.roll(total, G0 - KN, 1)
        ep_parts = split(ep)
        both = times(ep_parts, m_v[:, 0 : 2 * LANES])
        ek, ed = both[:, 0:LANES], both[:, LANES : 2 * LANES]
        g = own - gram_of(ek, ep_parts)
        g = jnp.where((lane >= G0) & (lane < G0 + N), g, 0.0)
        a = jnp.where(lane < KN, ed, jnp.where(lane == sub + KN, 1.0, g))
        a = eliminate(a, G0, N)
        lhs = split_rows(jnp.where(lane < KN, -a, a))[:, 0:Z]
    with jax.named_scope("coef1"):
        low2 = rows_full(a).T[G0 : G0 + N]
        es = times(ep_parts, m_v[:, 2 * LANES : 3 * LANES])
        stack = jnp.where(lane < K, ep, jnp.where(lane < KN, pltpu.roll(es, K, 1), 0.0))
        stack = jnp.where((lane >= KN) & (lane < Z), pltpu.roll(low2, KN, 1), stack)
        stacked = jnp.concatenate(split(rows_full(stack)), axis=0).astype(BF)
        coefs[1] = times(split(inv), stacked)
    with jax.named_scope("new1"):
        for i in range(R // 8):
            q = combine(lhs, pl.ds(i * wide8, wide8))
            for u in range(8):
                second_v[pl.ds(i * 8 + u, N, stride=RP), :] = q[:, u * LANES : (u + 1) * LANES]
    with jax.named_scope("drain"):
        for drain in drains:
            drain()


def deliver(
    R, first_v, second_v, coefs, first_hbm, second_hbm, one_hbm, two_hbm, coef_one, coef_two, sem
):
    copies = [
        pltpu.make_async_copy(first_v.at[:, pl.ds(0, R)], first_hbm, sem.at[0]),
        pltpu.make_async_copy(second_v.at[:, pl.ds(0, R)], second_hbm, sem.at[1]),
        pltpu.make_async_copy(coef_one, one_hbm, sem.at[2]),
        pltpu.make_async_copy(coef_two, two_hbm, sem.at[3]),
    ]
    for copy in copies[:2]:
        copy.start()
    coef_one[...] = coefs[0, :, 0 : coef_one.shape[1]]
    coef_two[...] = coefs[1, :, 0 : coef_two.shape[1]]
    for copy in copies[2:]:
        copy.start()
    for copy in copies:
        copy.wait()


def local(nx, ny, basis, panel, rate_codes):
    N, R, C = panel.shape
    K = basis.shape[0]
    assert C == LANES and 2 * K == LANES and N == 8
    vmem = pl.BlockSpec(memory_space=pltpu.VMEM)
    hbm = pl.BlockSpec(memory_space=pl.ANY)
    dma = pltpu.SemaphoreType.DMA
    sites = R * LANES
    group = nx * ny if nx * ny <= DIRECT else nx
    Z = K + 2 * N
    first, second, coefs = pl.pallas_call(
        functools.partial(kernel, nx, ny, K, N, R),
        out_shape=(
            pltpu.VMEM((N * (R + PAD), C), F32),
            pltpu.VMEM((N * (R + PAD), C), F32),
            pltpu.VMEM((2, N, C), F32),
        ),
        in_specs=[pl.BlockSpec(memory_space=pltpu.HBM)] * 3,
        out_specs=(vmem, vmem, vmem),
        scratch_shapes=[
            pltpu.VMEM((K, R + PAD, LANES), F32),
            pltpu.VMEM((N, R + PAD, LANES), F32),
            pltpu.VMEM((4 * R, LANES), jnp.int32),
            pltpu.VMEM((5 * (R + 16), LANES), F32),
            pltpu.VMEM((N, (R + 2) * LANES), F32),
            pltpu.VMEM((N, sites + 5 * LANES), F32),
            pltpu.VMEM((2 * N + 2 * Z, sites + 5 * LANES), BF),
            pltpu.VMEM((2 * LANES, 3 * LANES), BF),
            pltpu.VMEM((LANES, LANES), F32),
            pltpu.VMEM((2, LANES, LANES), F32),
            pltpu.VMEM((3, N, LANES), F32),
            pltpu.VMEM((4, N, LANES), F32),
            pltpu.VMEM((3, K, LANES), F32),
            pltpu.VMEM((4, K, LANES), F32),
            pltpu.VMEM((3, N, LANES), F32),
            pltpu.VMEM((4, N, LANES), F32),
            pltpu.VMEM((ny, K // 2 // ny, LANES), F32),
            pltpu.VMEM((2 * ny + nx, K // 2 // ny, LANES), F32),
            pltpu.VMEM((2, ny, N // 2 + 1, LANES), F32),
            pltpu.VMEM((2, group, N // 2 + 1, LANES), F32),
            dma((2 + CHUNKS,)),
            dma((4,)),
            dma((4,)),
            dma((4,)),
            dma((4,)),
            dma((4,)),
            pltpu.SemaphoreType.REGULAR((2,)),
            dma((4,)),
            dma((1 if nx * ny <= DIRECT and nx % BUDDY == 0 else 3,)),
            dma((3,)),
        ],
        compiler_params=pltpu.CompilerParams(
            collective_id=0, has_side_effects=True
        ),
    )(basis, panel, rate_codes.reshape(rate_codes.shape[0] * R, C))
    first, second, coef_one, coef_two = pl.pallas_call(
        functools.partial(deliver, R),
        out_shape=(
            jax.ShapeDtypeStruct((N, R, C), F32),
            jax.ShapeDtypeStruct((N, R, C), F32),
            jax.ShapeDtypeStruct((N, K + N), F32),
            jax.ShapeDtypeStruct((N, K + 2 * N), F32),
        ),
        in_specs=[vmem] * 3,
        out_specs=(hbm, hbm, hbm, hbm),
        scratch_shapes=[
            pltpu.VMEM((N, K + N), F32),
            pltpu.VMEM((N, K + 2 * N), F32),
            dma((4,)),
        ],
        compiler_params=pltpu.CompilerParams(vmem_limit_bytes=4 * 2**20),
    )(first.reshape(N, R + PAD, C), second.reshape(N, R + PAD, C), coefs)
    return first, second, coef_one.T, coef_two.T


def solution(mesh):
    spec = P(None, "gx", "gy")
    return jax.shard_map(
        functools.partial(local, mesh.shape["gx"], mesh.shape["gy"]),
        mesh=mesh,
        in_specs=(spec, spec, spec),
        out_specs=(spec, spec, P(), P()),
        check_vma=False,
    )
```
